32 devices in a mesh: fsdp: 4 (over x, core), ctx: 8 (over z, y).
Axes of the slice: x: 2, y: 2, z: 4, core: 2. Of those that a mesh axis runs over, the one named last changes fastest.
Arguments:
- inputs: bfloat16 [8, 1024, 1600], P('fsdp', 'ctx'), may hold values from -6 to 6
- cotangent: bfloat16 [8, 1024, 1600], P('fsdp', 'ctx'), may hold values from -6 to 6
- segments: int32 [8, 1024], P('fsdp', 'ctx'), may hold values from 0 to 10, as said below
- stretch_order: int32 [8], replicated, may hold values from 0 to 7, as said below
- prenorm_gain: bfloat16 [1600], P('ctx'), may hold values from 0.5 to 1.5
- prenorm_shift: bfloat16 [1600], P('ctx'), may hold values from -2 to 2
- joint_weight: bfloat16 [1600, 4800], P('fsdp', 'ctx')
- query_bias: bfloat16 [1600], P('ctx'), may hold values from -2 to 2
- value_bias: bfloat16 [1600], P('ctx'), may hold values from -2 to 2
- mixer_weight: bfloat16 [1600, 1600], P('fsdp', 'ctx'), may hold values from -0.75 to 0.75
- mixer_bias: bfloat16 [1600], P('ctx'), may hold values from -2 to 2
- midnorm_gain: bfloat16 [1600], P('ctx'), may hold values from 0.5 to 1.5
- midnorm_shift: bfloat16 [1600], P('ctx'), may hold values from -2 to 2
- expand_weight: bfloat16 [1600, 6400], P('fsdp', 'ctx'), may hold values from -0.15625 to 0.15625
- expand_bias: bfloat16 [6400], P('ctx'), may hold values from -2 to 2
- shrink_weight: bfloat16 [6400, 1600], P('fsdp', 'ctx'), may hold values from -0.078125 to 0.078125
- shrink_bias: bfloat16 [1600], P('ctx'), may hold values from -2 to 2
Outputs:
- block_output: bfloat16 [8, 1024, 1600], P('fsdp', 'ctx')
- input_gradient: float32 [8, 1024, 1600], P('fsdp', 'ctx')
- prenormgain_gradient: float32 [1600], P('ctx')
- prenormshift_gradient: float32 [1600], P('ctx')
- joint_gradient: float32 [1600, 4800], P('fsdp', 'ctx')
- querybias_gradient: float32 [1600], P('ctx')
- valuebias_gradient: float32 [1600], P('ctx')
- mixer_gradient: float32 [1600, 1600], P('fsdp', 'ctx')
- mixerbias_gradient: float32 [1600], P('ctx')
- midnormgain_gradient: float32 [1600], P('ctx')
- midnormshift_gradient: float32 [1600], P('ctx')
- expand_gradient: float32 [1600, 6400], P('fsdp', 'ctx')
- expandbias_gradient: float32 [6400], P('ctx')
- shrink_gradient: float32 [6400, 1600], P('fsdp', 'ctx')
- shrinkbias_gradient: float32 [1600], P('ctx')
The draws below stay inside these ranges and needn't reach their ends.
Inputs may be any that keep to these rules, and one draw needn't show every extreme that they name: A permutation: stored block i of every sequence is its true block stretch_order[i]. `segments`: in true order the numbers start at 0 and rise by one where a document starts; each document but a sequence's last spans 100 to 1000 positions.
All inputs are finite; a program needn't handle non-finite values.
Results may differ from the reference program's by a relative error of at most 0.019.
Values may be sent and summed in bfloat16 or wider, within the bound.
A program may use at most 320 MiB of HBM per device.

```python
import jax
import jax.numpy as jnp
from jax import lax

D = 1600
H = 25
HEAD = 64
FF = 6400
DOC_MIN = 100
DOC_MAX = 1000
STRETCH = 128
SEQ = 1024
SEQS = 8
N_CTX = 8


def stretch_permutation(key):
    return jax.random.permutation(jax.random.fold_in(key, 11), N_CTX).astype(jnp.int32)


def draw_stretch_order(key, part):
    return stretch_permutation(key)


def draw_segments(key, part):
    order_table = stretch_permutation(key)
    doc_count = SEQ // DOC_MIN + 1
    densest = jax.random.randint(jax.random.fold_in(key, 29), (), 0, SEQS).astype(jnp.int32)

    def one_sequence(seq_index):
        seq_key = jax.random.fold_in(jax.random.fold_in(key, 23), seq_index)
        drawn_lengths = jax.random.randint(seq_key, (doc_count,), DOC_MIN, DOC_MAX + 1).astype(jnp.int32)
        doc_lengths = jnp.where(seq_index == densest, jnp.int32(DOC_MIN), drawn_lengths).astype(jnp.int32)
        doc_ends = jnp.cumsum(doc_lengths)
        true_place = jnp.arange(SEQ, dtype=jnp.int32)
        true_ids = jnp.sum((doc_ends[None, :] <= true_place[:, None]).astype(jnp.int32), axis=1)
        id_table = true_ids.reshape(N_CTX, STRETCH)
        return jnp.take(id_table, order_table, axis=0).reshape(SEQ).astype(jnp.int32)
    return jax.vmap(one_sequence)(jnp.arange(SEQS, dtype=jnp.int32))


def draw_joint_weight(key, part):
    base_draw = jax.random.normal(jax.random.fold_in(key, 3), (D, 3 * D), jnp.float32) * D ** (-0.5)
    return base_draw.astype(jnp.bfloat16)


def block_scale(own_key, extent, pieces, low, largest):
    factor_of = 1.0
    for position, shards_of in pieces:
        draws = jax.random.uniform(jax.random.fold_in(jax.random.fold_in(own_key, 6), position), (shards_of,), jnp.float32, low / len(pieces), largest / len(pieces))
        factor_of = factor_of * jnp.repeat(jnp.exp(draws), extent[position] // shards_of).reshape((-1,) + (1,) * (len(extent) - 1 - position))
    return factor_of


def noise(key, dims, scale, reach, shards=(), kind=jnp.bfloat16):
    factor_of = block_scale(key, dims, shards, -0.22, 0.18) if shards else 1.0
    values = jax.random.normal(key, dims, jnp.float32) * scale * factor_of
    return jnp.minimum(jnp.maximum(values, -reach), reach).astype(kind)


def setup_inputs(seed: int = 0) -> dict:
    splits = jax.random.split(jax.random.key(seed), 18)
    inputs = noise(splits[0], (SEQS, SEQ, D), 1.0, 6.0, ((0, 4), (1, 8)))
    cotangent = noise(splits[1], (SEQS, SEQ, D), 1.0, 6.0, ((0, 4), (1, 8)))
    segments = draw_segments(jax.random.fold_in(splits[17], 71), 0)
    stretch_order = draw_stretch_order(jax.random.fold_in(splits[17], 71), 0)
    prenorm_gain = jnp.clip(1.0 + 0.1 * jax.random.normal(splits[4], (D,), jnp.float32), 0.5, 1.5).astype(jnp.bfloat16)
    prenorm_shift = noise(splits[5], (D,), 0.3, 2.0, ((0, 8),))
    joint_weight = draw_joint_weight(jax.random.fold_in(splits[17], 71), 0)
    query_bias = noise(splits[7], (D,), 0.3, 2.0, ((0, 8),))
    value_bias = noise(splits[8], (D,), 0.3, 2.0, ((0, 8),))
    mixer_weight = noise(splits[9], (D, D), 64 ** -0.5, 0.75, ((0, 4), (1, 8)))
    mixer_bias = noise(splits[10], (D,), 0.3, 2.0, ((0, 8),))
    midnorm_gain = jnp.clip(1.0 + 0.1 * jax.random.normal(splits[11], (D,), jnp.float32), 0.5, 1.5).astype(jnp.bfloat16)
    midnorm_shift = noise(splits[12], (D,), 0.3, 2.0, ((0, 8),))
    expand_weight = noise(splits[13], (D, FF), D ** -0.5, 0.15625, ((0, 4), (1, 8)))
    expand_bias = noise(splits[14], (FF,), 0.3, 2.0, ((0, 8),))
    shrink_weight = noise(splits[15], (FF, D), FF ** -0.5, 0.078125, ((0, 4), (1, 8)))
    shrink_bias = noise(splits[16], (D,), 0.3, 2.0, ((0, 8),))
    return {"inputs": inputs, "cotangent": cotangent, "segments": segments, "stretch_order": stretch_order, "prenorm_gain": prenorm_gain, "prenorm_shift": prenorm_shift, "joint_weight": joint_weight, "query_bias": query_bias, "value_bias": value_bias, "mixer_weight": mixer_weight, "mixer_bias": mixer_bias, "midnorm_gain": midnorm_gain, "midnorm_shift": midnorm_shift, "expand_weight": expand_weight, "expand_bias": expand_bias, "shrink_weight": shrink_weight, "shrink_bias": shrink_bias}


@jax.custom_vjp
def low(v):
    return lax.optimization_barrier(v.astype(jnp.bfloat16)).astype(jnp.float32)

@jax.custom_vjp
def low_back(v):
    return v

def low_keep(v):
    return (low(v), None)

def low_pass(kept, grad):
    return (grad,)

def back_keep(v):
    return (v, None)

def back_low(kept, grad):
    return (low(grad),)
low.defvjp(low_keep, low_pass)
low_back.defvjp(back_keep, back_low)
epsilon = 1e-05
highest = lax.Precision.HIGHEST

def layer_norm(values, gain, shift):
    center = values - lax.optimization_barrier(jnp.mean(values, axis=-1, keepdims=True))
    spread = lax.optimization_barrier(jnp.mean(center * center, axis=-1, keepdims=True))
    return center * lax.rsqrt(spread + epsilon) * gain + shift

def attend_rows(query_rows, query_pos, query_seg, key_rows, value_rows, key_pos, key_seg):
    scores = jnp.einsum('qhd,khd->hqk', query_rows, key_rows, precision=highest) * HEAD ** (-0.5)
    allowed = (query_seg[:, None] == key_seg[None, :]) & (key_pos[None, :] <= query_pos[:, None])
    scores = low_back(jnp.where(allowed[None], scores, -1e+30))
    weights = low(jax.nn.softmax(scores, axis=-1))
    return jnp.einsum('hqk,khd->qhd', weights, value_rows, precision=highest)

def block_forward(tokens, seg_row, positions, params):
    prenorm_gain, prenorm_shift, joint_weight, query_bias, value_bias, mixer_weight, mixer_bias, midnorm_gain, midnorm_shift, expand_weight, expand_bias, shrink_weight, shrink_bias = params
    model_width = tokens.shape[1]
    token_count = tokens.shape[0]
    normed = low(layer_norm(tokens, prenorm_gain, prenorm_shift))
    joint_bias = jnp.concatenate([query_bias, jnp.zeros_like(query_bias), value_bias])
    joint_rows = low_back(low(jnp.dot(normed, joint_weight, precision=highest) + joint_bias))
    queries = joint_rows[:, :model_width].reshape(token_count, H, HEAD)
    key_rows = joint_rows[:, model_width:2 * model_width].reshape(token_count, H, HEAD)
    value_rows = joint_rows[:, 2 * model_width:].reshape(token_count, H, HEAD)
    row_count = min(token_count, 512)
    block_count = token_count // row_count

    def one_block(block_item):
        query_rows, query_pos, query_seg = block_item
        return attend_rows(query_rows, query_pos, query_seg, key_rows, value_rows, positions, seg_row)
    mixed_rows = lax.map(jax.checkpoint(one_block), (queries.reshape(block_count, row_count, H, HEAD), positions.reshape(block_count, row_count), seg_row.reshape(block_count, row_count)))
    mixed_rows = low_back(low(mixed_rows.reshape(token_count, model_width)))
    branch = low_back(jnp.dot(mixed_rows, mixer_weight, precision=highest) + mixer_bias)
    middle = tokens + branch
    second = low(layer_norm(middle, midnorm_gain, midnorm_shift))
    expanded = low_back(jnp.dot(second, expand_weight, precision=highest) + expand_bias)
    active = low(jax.nn.gelu(expanded, approximate=True))
    return middle + jnp.dot(active, shrink_weight, precision=highest) + shrink_bias

def reference(inputs, cotangent, segments, stretch_order, prenorm_gain, prenorm_shift, joint_weight, query_bias, value_bias, mixer_weight, mixer_bias, midnorm_gain, midnorm_shift, expand_weight, expand_bias, shrink_weight, shrink_bias):
    params = tuple((tensor.astype(jnp.float32) for tensor in (prenorm_gain, prenorm_shift, joint_weight, query_bias, value_bias, mixer_weight, mixer_bias, midnorm_gain, midnorm_shift, expand_weight, expand_bias, shrink_weight, shrink_bias)))
    positions = (stretch_order[:, None] * STRETCH + jnp.arange(STRETCH, dtype=jnp.int32)[None, :]).reshape(SEQ).astype(jnp.int32)

    def per_sequence(totals, sequence):
        tokens, tangent, seg_row = sequence
        result, pullback = jax.vjp(lambda values_in, param_in: block_forward(values_in, seg_row, positions, param_in), tokens.astype(jnp.float32), params)
        token_grad, param_grad = pullback(tangent.astype(jnp.float32))
        totals = jax.tree.map(jnp.add, totals, param_grad)
        return (totals, (result.astype(jnp.bfloat16), token_grad))
    zeros_start = jax.tree.map(jnp.zeros_like, params)
    totals, (block_output, input_gradient) = lax.scan(per_sequence, zeros_start, (inputs, cotangent, segments))
    return (block_output, input_gradient, totals[0], totals[1], totals[2], totals[3], totals[4], totals[5], totals[6], totals[7], totals[8], totals[9], totals[10], totals[11], totals[12])
```

```python
import functools

import jax
import jax.numpy as jnp
from jax import lax
from jax.experimental import pallas as pl
from jax.experimental.pallas import tpu as pltpu
from jax.sharding import PartitionSpec as P

HEAD = 64
MICRO = 2
LANES = 128
STRETCH = 128
TILE = 256


epsilon = 1e-05
masked_score = -1e30


def layer_norm(values, gain, shift):
    center = values - jnp.mean(values, axis=-1, keepdims=True)
    spread = jnp.mean(center * center, axis=-1, keepdims=True)
    return center * lax.rsqrt(spread + epsilon) * gain + shift


def piece_size(count):
    size_now = min(count, 512)
    while count % size_now:
        size_now -= 1
    return size_now


def true_positions(stretch_order, first_index, count, stretch_len):
    stored = first_index + jnp.arange(count, dtype=jnp.int32)
    holder = stored // stretch_len
    picked = holder[:, None] == jnp.arange(stretch_order.shape[0], dtype=jnp.int32)[None, :]
    return (
        jnp.sum(jnp.where(picked, stretch_order[None, :], 0), axis=1) * stretch_len
        + stored % stretch_len
    )


def times_transposed(left, right):
    return lax.dot_general(
        left, right, (((1,), (1,)), ((), ())), preferred_element_type=jnp.float32
    )


def outer_sum(left, right):
    return lax.dot_general(
        left, right, (((0,), (0,)), ((), ())), preferred_element_type=jnp.float32
    )


def fetch_weights(local_parts):
    (
        joint_weight,
        mixer_weight,
        expand_weight,
        shrink_weight,
        prenorm_gain,
        prenorm_shift,
        query_bias,
        value_bias,
        mixer_bias,
        midnorm_gain,
        midnorm_shift,
        expand_bias,
        shrink_bias,
    ) = local_parts
    spread_out = (
        lax.all_gather(joint_weight, "ctx", axis=1, tiled=True),
        lax.all_gather(mixer_weight, "ctx", axis=1, tiled=True),
        lax.all_gather(expand_weight, "ctx", axis=1, tiled=True),
        lax.all_gather(shrink_weight, "ctx", axis=1, tiled=True),
        lax.all_gather(prenorm_gain, "ctx", axis=0, tiled=True),
        lax.all_gather(prenorm_shift, "ctx", axis=0, tiled=True),
        lax.all_gather(query_bias, "ctx", axis=0, tiled=True),
        lax.all_gather(value_bias, "ctx", axis=0, tiled=True),
        lax.all_gather(mixer_bias, "ctx", axis=0, tiled=True),
        lax.all_gather(midnorm_gain, "ctx", axis=0, tiled=True),
        lax.all_gather(midnorm_shift, "ctx", axis=0, tiled=True),
        lax.all_gather(expand_bias, "ctx", axis=0, tiled=True),
        lax.all_gather(shrink_bias, "ctx", axis=0, tiled=True),
    )
    whole_rows = (
        lax.all_gather(spread_out[0], "fsdp", axis=0, tiled=True),
        lax.all_gather(spread_out[1], "fsdp", axis=0, tiled=True),
        lax.all_gather(spread_out[2], "fsdp", axis=0, tiled=True),
        lax.all_gather(spread_out[3], "fsdp", axis=0, tiled=True),
    )
    return tuple(whole_rows) + tuple(spread_out[4:])


def reduce_gradients(matrices, smalls):
    small_sums = (
        lax.psum(smalls[0].astype(jnp.bfloat16), "fsdp").astype(jnp.float32),
        lax.psum(smalls[1].astype(jnp.bfloat16), "fsdp").astype(jnp.float32),
        lax.psum(smalls[2].astype(jnp.bfloat16), "fsdp").astype(jnp.float32),
        lax.psum(smalls[3].astype(jnp.bfloat16), "fsdp").astype(jnp.float32),
        lax.psum(smalls[4].astype(jnp.bfloat16), "fsdp").astype(jnp.float32),
        lax.psum(smalls[5].astype(jnp.bfloat16), "fsdp").astype(jnp.float32),
        lax.psum(smalls[6].astype(jnp.bfloat16), "fsdp").astype(jnp.float32),
        lax.psum(smalls[7].astype(jnp.bfloat16), "fsdp").astype(jnp.float32),
        lax.psum(smalls[8].astype(jnp.bfloat16), "fsdp").astype(jnp.float32),
    )
    column_part = (
        lax.psum_scatter(
            matrices[0].astype(jnp.bfloat16), "ctx", scatter_dimension=1, tiled=True
        ).astype(jnp.float32),
        lax.psum_scatter(
            matrices[1].astype(jnp.bfloat16), "ctx", scatter_dimension=1, tiled=True
        ).astype(jnp.float32),
        lax.psum_scatter(
            matrices[2].astype(jnp.bfloat16), "ctx", scatter_dimension=1, tiled=True
        ).astype(jnp.float32),
        lax.psum_scatter(
            matrices[3].astype(jnp.bfloat16), "ctx", scatter_dimension=1, tiled=True
        ).astype(jnp.float32),
        lax.psum_scatter(
            small_sums[0].astype(jnp.bfloat16), "ctx", scatter_dimension=0, tiled=True
        ).astype(jnp.float32),
        lax.psum_scatter(
            small_sums[1].astype(jnp.bfloat16), "ctx", scatter_dimension=0, tiled=True
        ).astype(jnp.float32),
        lax.psum_scatter(
            small_sums[2].astype(jnp.bfloat16), "ctx", scatter_dimension=0, tiled=True
        ).astype(jnp.float32),
        lax.psum_scatter(
            small_sums[3].astype(jnp.bfloat16), "ctx", scatter_dimension=0, tiled=True
        ).astype(jnp.float32),
        lax.psum_scatter(
            small_sums[4].astype(jnp.bfloat16), "ctx", scatter_dimension=0, tiled=True
        ).astype(jnp.float32),
        lax.psum_scatter(
            small_sums[5].astype(jnp.bfloat16), "ctx", scatter_dimension=0, tiled=True
        ).astype(jnp.float32),
        lax.psum_scatter(
            small_sums[6].astype(jnp.bfloat16), "ctx", scatter_dimension=0, tiled=True
        ).astype(jnp.float32),
        lax.psum_scatter(
            small_sums[7].astype(jnp.bfloat16), "ctx", scatter_dimension=0, tiled=True
        ).astype(jnp.float32),
        lax.psum_scatter(
            small_sums[8].astype(jnp.bfloat16), "ctx", scatter_dimension=0, tiled=True
        ).astype(jnp.float32),
    )
    row_part = (
        lax.psum_scatter(
            column_part[0].astype(jnp.bfloat16), "fsdp", scatter_dimension=0, tiled=True
        ).astype(jnp.float32),
        lax.psum_scatter(
            column_part[1].astype(jnp.bfloat16), "fsdp", scatter_dimension=0, tiled=True
        ).astype(jnp.float32),
        lax.psum_scatter(
            column_part[2].astype(jnp.bfloat16), "fsdp", scatter_dimension=0, tiled=True
        ).astype(jnp.float32),
        lax.psum_scatter(
            column_part[3].astype(jnp.bfloat16), "fsdp", scatter_dimension=0, tiled=True
        ).astype(jnp.float32),
    )
    return tuple(row_part) + tuple(column_part[4:])


def local(
    inputs,
    cotangent,
    segments,
    stretch_order,
    prenorm_gain,
    prenorm_shift,
    joint_weight,
    query_bias,
    value_bias,
    mixer_weight,
    mixer_bias,
    midnorm_gain,
    midnorm_shift,
    expand_weight,
    expand_bias,
    shrink_weight,
    shrink_bias,
):
    local_parts = (
        joint_weight,
        mixer_weight,
        expand_weight,
        shrink_weight,
        prenorm_gain,
        prenorm_shift,
        query_bias,
        value_bias,
        mixer_bias,
        midnorm_gain,
        midnorm_shift,
        expand_bias,
        shrink_bias,
    )
    seq_local, stretch_len, model_width = inputs.shape
    head_count = model_width // HEAD
    group_size = seq_local // MICRO
    row_count = group_size * stretch_len
    score_scale = HEAD ** (-0.5)
    ctx_place = lax.axis_index("ctx")
    own_stretch = jnp.sum(
        jnp.where(
            jnp.arange(stretch_order.shape[0], dtype=jnp.int32) == ctx_place, stretch_order, 0
        )
    )
    own_pos = own_stretch * stretch_len + jnp.arange(stretch_len, dtype=jnp.int32)
    all_segments = lax.all_gather(segments, "ctx", axis=1, tiled=True)

    def backward_micro(weights, kept_values, micro_index):
        (
            joint_full,
            mixer_full,
            expand_full,
            shrink_full,
            gain_one,
            shift_one,
            qbias_full,
            vbias_full,
            mbias_full,
            gain_two,
            shift_two,
            ebias_full,
            sbias_full,
        ) = weights
        (
            tokens,
            seg_local,
            seg_whole,
            normed,
            queries,
            keys_local,
            values_local,
            mixed_rows,
            attended,
            log_total,
            middle,
            second,
            expanded,
            active,
        ) = kept_values
        lower = micro_index * group_size
        tangent_rows = cotangent[lower : lower + group_size].reshape(row_count, model_width)
        active_grad = times_transposed(tangent_rows, shrink_full)
        gelu_pull = jax.vjp(lambda value_in: jax.nn.gelu(value_in, approximate=True), expanded)[1]
        expand_delta = gelu_pull(active_grad)[0].astype(jnp.bfloat16)
        second_grad = times_transposed(expand_delta, expand_full)
        mid_pull = jax.vjp(
            layer_norm, middle, gain_two.astype(jnp.float32), shift_two.astype(jnp.float32)
        )[1]
        middle_grad, gain_two_grad, shift_two_grad = mid_pull(second_grad)
        middle_grad = middle_grad + tangent_rows.astype(jnp.float32)
        branch_delta = middle_grad.astype(jnp.bfloat16)
        attended_delta = times_transposed(branch_delta, mixer_full).astype(jnp.bfloat16)
        grad_heads = attended_delta.reshape(group_size, stretch_len, head_count, HEAD)
        delta_heads = jnp.sum(
            grad_heads.transpose(0, 2, 1, 3).astype(jnp.float32) * attended, axis=-1
        )
        delta_rows = delta_heads.transpose(0, 2, 1)
        log_rows = log_total.transpose(0, 2, 1)
        lse_whole, delta_whole = (
            lax.all_gather(log_rows, "ctx", axis=1, tiled=True),
            lax.all_gather(delta_rows, "ctx", axis=1, tiled=True),
        )
        query_heads = queries.reshape(group_size, stretch_len, head_count, HEAD)
        key_heads = keys_local.reshape(group_size, stretch_len, head_count, HEAD)
        value_heads = values_local.reshape(group_size, stretch_len, head_count, HEAD)
        head_zeros = jnp.zeros((group_size, head_count, stretch_len, HEAD), jnp.float32)
        query_key_piece = lax.all_gather(keys_local, "ctx", axis=1, tiled=True)
        value_piece = lax.all_gather(values_local, "ctx", axis=1, tiled=True)
        count = query_key_piece.shape[1]
        step_len = piece_size(count)

        def query_block_step(turn_index, running):
            offset = turn_index * step_len
            key_block = lax.dynamic_slice_in_dim(query_key_piece, offset, step_len, 1).reshape(
                group_size, step_len, head_count, HEAD
            )
            value_block = lax.dynamic_slice_in_dim(value_piece, offset, step_len, 1).reshape(
                group_size, step_len, head_count, HEAD
            )
            key_pos = true_positions(stretch_order, offset, step_len, stretch_len)
            key_seg = lax.dynamic_slice_in_dim(seg_whole, offset, step_len, 1)
            allowed = (
                (seg_local[:, :, None] == key_seg[:, None, :])
                & (key_pos[None, None, :] <= own_pos[None, :, None])
            )[:, None]
            scores = (
                jnp.einsum(
                    "gqhd,gkhd->ghqk", query_heads, key_block, preferred_element_type=jnp.float32
                )
                * score_scale
            )
            probs = jnp.where(allowed, jnp.exp(scores - log_total[..., None]), 0.0)
            dots = jnp.einsum(
                "gqhd,gkhd->ghqk", grad_heads, value_block, preferred_element_type=jnp.float32
            )
            score_delta = (probs * (dots - delta_heads[..., None])).astype(jnp.bfloat16)
            return running + jnp.einsum(
                "ghqk,gkhd->ghqd", score_delta, key_block, preferred_element_type=jnp.float32
            )

        query_acc = lax.fori_loop(0, count // step_len, query_block_step, head_zeros)
        grad_rows3 = attended_delta.reshape(group_size, stretch_len, model_width)
        query_piece_rows = lax.all_gather(queries, "ctx", axis=1, tiled=True)
        grad_piece = lax.all_gather(grad_rows3, "ctx", axis=1, tiled=True)
        count = query_piece_rows.shape[1]
        key_step_len = piece_size(count)

        def key_block_step(turn_index, running):
            key_acc, value_acc = running
            offset = turn_index * key_step_len
            query_block = lax.dynamic_slice_in_dim(
                query_piece_rows, offset, key_step_len, 1
            ).reshape(group_size, key_step_len, head_count, HEAD)
            grad_block = lax.dynamic_slice_in_dim(grad_piece, offset, key_step_len, 1).reshape(
                group_size, key_step_len, head_count, HEAD
            )
            query_pos = true_positions(stretch_order, offset, key_step_len, stretch_len)
            query_seg = lax.dynamic_slice_in_dim(seg_whole, offset, key_step_len, 1)
            lse_block = lax.dynamic_slice_in_dim(lse_whole, offset, key_step_len, 1).transpose(
                0, 2, 1
            )
            delta_block = lax.dynamic_slice_in_dim(delta_whole, offset, key_step_len, 1).transpose(
                0, 2, 1
            )
            allowed = (
                (query_seg[:, :, None] == seg_local[:, None, :])
                & (own_pos[None, None, :] <= query_pos[None, :, None])
            )[:, None]
            scores = (
                jnp.einsum(
                    "gqhd,gkhd->ghqk", query_block, key_heads, preferred_element_type=jnp.float32
                )
                * score_scale
            )
            probs = jnp.where(allowed, jnp.exp(scores - lse_block[..., None]), 0.0)
            value_acc = value_acc + jnp.einsum(
                "ghqk,gqhd->ghkd",
                probs.astype(jnp.bfloat16),
                grad_block,
                preferred_element_type=jnp.float32,
            )
            dots = jnp.einsum(
                "gqhd,gkhd->ghqk", grad_block, value_heads, preferred_element_type=jnp.float32
            )
            score_delta = (probs * (dots - delta_block[..., None])).astype(jnp.bfloat16)
            key_acc = key_acc + jnp.einsum(
                "ghqk,gqhd->ghkd", score_delta, query_block, preferred_element_type=jnp.float32
            )
            return (key_acc, value_acc)

        key_acc, value_acc = lax.fori_loop(
            0, count // key_step_len, key_block_step, (head_zeros, head_zeros)
        )
        query_delta = (
            (query_acc * score_scale)
            .transpose(0, 2, 1, 3)
            .reshape(row_count, model_width)
            .astype(jnp.bfloat16)
        )
        key_delta = (
            (key_acc * score_scale)
            .transpose(0, 2, 1, 3)
            .reshape(row_count, model_width)
            .astype(jnp.bfloat16)
        )
        value_delta = (
            value_acc.transpose(0, 2, 1, 3).reshape(row_count, model_width).astype(jnp.bfloat16)
        )
        joint_delta = jnp.concatenate([query_delta, key_delta, value_delta], axis=1)
        normed_grad = times_transposed(joint_delta, joint_full)
        first_pull = jax.vjp(
            layer_norm,
            tokens.reshape(row_count, model_width),
            gain_one.astype(jnp.float32),
            shift_one.astype(jnp.float32),
        )[1]
        token_grad, gain_one_grad, shift_one_grad = first_pull(normed_grad)
        input_grad = (middle_grad + token_grad).reshape(group_size, stretch_len, model_width)
        small_terms = (
            gain_one_grad,
            shift_one_grad,
            jnp.sum(query_delta.astype(jnp.float32), axis=0),
            jnp.sum(value_delta.astype(jnp.float32), axis=0),
            jnp.sum(branch_delta.astype(jnp.float32), axis=0),
            gain_two_grad,
            shift_two_grad,
            jnp.sum(expand_delta.astype(jnp.float32), axis=0),
            jnp.sum(tangent_rows.astype(jnp.float32), axis=0),
        )
        factor_pairs = (
            normed.reshape(row_count, model_width),
            joint_delta,
            mixed_rows,
            branch_delta,
            second,
            expand_delta,
            active,
            tangent_rows,
        )
        return (input_grad, small_terms, factor_pairs)

    output_list = []
    input_list = []
    factor_list = []
    small_totals = None
    for micro_index in range(MICRO):
        forward_weights = fetch_weights(local_parts)
        (
            forward_joint_full,
            forward_mixer_full,
            forward_expand_full,
            forward_shrink_full,
            forward_gain_one,
            forward_shift_one,
            forward_qbias_full,
            forward_vbias_full,
            forward_mbias_full,
            forward_gain_two,
            forward_shift_two,
            forward_ebias_full,
            forward_sbias_full,
        ) = forward_weights
        forward_lower = micro_index * group_size
        forward_tokens = inputs[forward_lower : forward_lower + group_size].astype(jnp.float32)
        forward_seg_local = segments[forward_lower : forward_lower + group_size]
        forward_seg_whole = all_segments[forward_lower : forward_lower + group_size]
        forward_normed = layer_norm(
            forward_tokens,
            forward_gain_one.astype(jnp.float32),
            forward_shift_one.astype(jnp.float32),
        ).astype(jnp.bfloat16)
        joint_bias = jnp.concatenate(
            [forward_qbias_full, jnp.zeros_like(forward_qbias_full), forward_vbias_full]
        ).astype(jnp.float32)
        joint_rows = (
            jnp.dot(
                forward_normed.reshape(row_count, model_width),
                forward_joint_full,
                preferred_element_type=jnp.float32,
            )
            + joint_bias
        )
        joint_rows = joint_rows.astype(jnp.bfloat16).reshape(
            group_size, stretch_len, 3 * model_width
        )
        forward_queries = joint_rows[..., :model_width]
        forward_keys_local = joint_rows[..., model_width : 2 * model_width]
        forward_values_local = joint_rows[..., 2 * model_width :]
        forward_query_heads = forward_queries.reshape(group_size, stretch_len, head_count, HEAD)
        start_state = (
            jnp.full((group_size, head_count, stretch_len), masked_score, jnp.float32),
            jnp.zeros((group_size, head_count, stretch_len), jnp.float32),
            jnp.zeros((group_size, head_count, stretch_len, HEAD), jnp.float32),
        )
        forward_key_piece = lax.all_gather(forward_keys_local, "ctx", axis=1, tiled=True)
        forward_value_piece = lax.all_gather(forward_values_local, "ctx", axis=1, tiled=True)
        forward_count = forward_key_piece.shape[1]
        forward_step_len = piece_size(forward_count)

        def forward_block_step(turn_index, state):
            top_score, row_total, accumulated = state
            offset = turn_index * forward_step_len
            key_block = lax.dynamic_slice_in_dim(
                forward_key_piece, offset, forward_step_len, 1
            ).reshape(group_size, forward_step_len, head_count, HEAD)
            value_block = lax.dynamic_slice_in_dim(
                forward_value_piece, offset, forward_step_len, 1
            ).reshape(group_size, forward_step_len, head_count, HEAD)
            key_pos = true_positions(stretch_order, offset, forward_step_len, stretch_len)
            key_seg = lax.dynamic_slice_in_dim(forward_seg_whole, offset, forward_step_len, 1)
            allowed = (
                (forward_seg_local[:, :, None] == key_seg[:, None, :])
                & (key_pos[None, None, :] <= own_pos[None, :, None])
            )[:, None]
            scores = (
                jnp.einsum(
                    "gqhd,gkhd->ghqk",
                    forward_query_heads,
                    key_block,
                    preferred_element_type=jnp.float32,
                )
                * score_scale
            )
            scores = jnp.where(allowed, scores, masked_score)
            new_top = jnp.maximum(top_score, jnp.max(scores, axis=-1))
            weights_now = jnp.where(allowed, jnp.exp(scores - new_top[..., None]), 0.0)
            fade_factor = jnp.exp(top_score - new_top)
            row_total = row_total * fade_factor + jnp.sum(weights_now, axis=-1)
            accumulated = accumulated * fade_factor[..., None] + jnp.einsum(
                "ghqk,gkhd->ghqd",
                weights_now.astype(jnp.bfloat16),
                value_block,
                preferred_element_type=jnp.float32,
            )
            return (new_top, row_total, accumulated)

        top_score, row_total, accumulated = lax.fori_loop(
            0, forward_count // forward_step_len, forward_block_step, start_state
        )
        forward_attended = accumulated / row_total[..., None]
        forward_log_total = top_score + jnp.log(row_total)
        forward_mixed_rows = (
            forward_attended.transpose(0, 2, 1, 3)
            .reshape(row_count, model_width)
            .astype(jnp.bfloat16)
        )
        branch = jnp.dot(
            forward_mixed_rows, forward_mixer_full, preferred_element_type=jnp.float32
        ) + forward_mbias_full.astype(jnp.float32)
        forward_middle = forward_tokens.reshape(row_count, model_width) + branch
        forward_second = layer_norm(
            forward_middle,
            forward_gain_two.astype(jnp.float32),
            forward_shift_two.astype(jnp.float32),
        ).astype(jnp.bfloat16)
        forward_expanded = jnp.dot(
            forward_second, forward_expand_full, preferred_element_type=jnp.float32
        ) + forward_ebias_full.astype(jnp.float32)
        forward_active = jax.nn.gelu(forward_expanded, approximate=True).astype(jnp.bfloat16)
        output = (
            forward_middle
            + jnp.dot(forward_active, forward_shrink_full, preferred_element_type=jnp.float32)
            + forward_sbias_full.astype(jnp.float32)
        )
        forward_kept_values = (
            forward_tokens,
            forward_seg_local,
            forward_seg_whole,
            forward_normed,
            forward_queries,
            forward_keys_local,
            forward_values_local,
            forward_mixed_rows,
            forward_attended,
            forward_log_total,
            forward_middle,
            forward_second,
            forward_expanded,
            forward_active,
        )
        output_now = output.reshape(group_size, stretch_len, model_width).astype(jnp.bfloat16)
        kept_values = forward_kept_values
        backward_weights = fetch_weights(local_parts)
        input_now, small_terms, factor_pairs = backward_micro(
            backward_weights, kept_values, micro_index
        )
        output_list.append(output_now)
        input_list.append(input_now)
        factor_list.append(factor_pairs)
        if small_totals is None:
            small_totals = small_terms
        else:
            small_totals = tuple(
                (total_now + term_now for total_now, term_now in zip(small_totals, small_terms))
            )

    def joined(position):
        return jnp.concatenate([pairs_now[position] for pairs_now in factor_list], axis=0)

    matrices = (
        outer_sum(joined(0), joined(1)),
        outer_sum(joined(2), joined(3)),
        outer_sum(joined(4), joined(5)),
        outer_sum(joined(6), joined(7)),
    )
    reduced = reduce_gradients(matrices, small_totals)
    block_output = jnp.concatenate(output_list, axis=0)
    input_gradient = jnp.concatenate(input_list, axis=0)
    return (
        block_output,
        input_gradient,
        reduced[4],
        reduced[5],
        reduced[0],
        reduced[6],
        reduced[7],
        reduced[1],
        reduced[8],
        reduced[9],
        reduced[10],
        reduced[2],
        reduced[11],
        reduced[3],
        reduced[12],
    )


def joint_split(rows, parts, heads_each):
    count, three, width = rows.shape
    span = heads_each * HEAD
    slots = slot_width(heads_each)
    rows = jnp.pad(rows, ((0, 0), (0, 0), (0, parts * span - width)))
    rows = rows.reshape(count, three, parts, span)
    rows = jnp.pad(rows, ((0, 0), (0, 0), (0, 0), (0, slots - span)))
    return rows.transpose(2, 0, 1, 3).reshape(parts, count, three * slots)


def joint_join(pieces, heads_each, width):
    parts, count, wide = pieces.shape
    span = heads_each * HEAD
    rows = pieces.reshape(parts, count, 3, wide // 3)[..., :span]
    rows = rows.transpose(1, 2, 0, 3).reshape(count, 3, parts * span)
    return rows[..., :width].reshape(count, 3 * width)


def slot_width(heads_each):
    return -(-heads_each * HEAD // LANES) * LANES


def attend_prepare(inv_ref, seg_row_ref, seg_col_ref, seg_row, seg_col):
    for place in range(inv_ref.shape[0]):
        stored = inv_ref[place]
        here = pl.ds(place * STRETCH, STRETCH)
        seg_row[:, here] = seg_row_ref[pl.ds(stored, 1), :]
        seg_col[here, :] = seg_col_ref[pl.ds(pl.multiple_of(stored * STRETCH, STRETCH), STRETCH), :]


def true_rows(inv_ref, source, column):
    pieces = []
    for place in range(inv_ref.shape[0]):
        at_row = pl.multiple_of(inv_ref[place] * STRETCH, STRETCH)
        pieces.append(source[pl.ds(at_row, STRETCH), pl.ds(column, LANES)])
    return jnp.concatenate(pieces, axis=0)


def store_true(inv_ref, target, first_place, column, rows):
    for step in range(rows.shape[0] // STRETCH):
        at_row = pl.multiple_of(inv_ref[first_place + step] * STRETCH, STRETCH)
        target[pl.ds(at_row, STRETCH), pl.ds(column, LANES)] = rows[
            step * STRETCH : (step + 1) * STRETCH
        ]


def attend_forward_kernel(
    inv_ref, seg_row_ref, seg_col_ref, qkv_ref, out_ref, turned_ref, lse_ref,
    seg_row, seg_col, q_low, q_high, keys, values_turned, acc, tops, sums,
):
    pair = pl.program_id(0)
    slots = out_ref.shape[1]
    scale = HEAD ** (-0.5)

    @pl.when(pair == 0)
    def _():
        attend_prepare(inv_ref, seg_row_ref, seg_col_ref, seg_row, seg_col)

    column = pl.multiple_of(pair * LANES, LANES)
    queries = true_rows(inv_ref, qkv_ref, column) * jnp.bfloat16(scale)
    low_half = lax.broadcasted_iota(jnp.int32, queries.shape, 1) < HEAD
    q_low[...] = jnp.where(low_half, queries, jnp.zeros_like(queries))
    q_high[...] = jnp.where(low_half, jnp.zeros_like(queries), queries)
    keys[...] = true_rows(inv_ref, qkv_ref, slots + column)
    values = true_rows(inv_ref, qkv_ref, 2 * slots + column)
    values_turned[...] = values.astype(jnp.float32).T.astype(jnp.bfloat16)
    halves = (q_low, q_high)

    def one_block(q_block, k_block, first):
        q_at = pl.ds(pl.multiple_of(q_block * TILE, TILE), TILE)
        k_at = pl.ds(pl.multiple_of(k_block * TILE, TILE), TILE)
        same = seg_col[k_at, :] == seg_row[:, q_at]
        if first:
            same = same & (
                lax.broadcasted_iota(jnp.int32, (TILE, TILE), 0)
                <= lax.broadcasted_iota(jnp.int32, (TILE, TILE), 1)
            )
        for half in range(2):
            dims = pl.ds(half * HEAD, HEAD)
            scores = times_transposed(keys[k_at, :], halves[half][q_at, :])
            scores = jnp.where(same, scores, masked_score)
            top = jnp.max(scores, axis=0, keepdims=True)
            if not first:
                old_top = tops[half]
                top = jnp.maximum(old_top, top)
            weights = jnp.exp(scores - top)
            total = jnp.sum(weights, axis=0, keepdims=True)
            part = jnp.dot(
                values_turned[dims, k_at],
                weights.astype(jnp.bfloat16),
                preferred_element_type=jnp.float32,
            )
            if not first:
                fade = jnp.exp(old_top - top)
                total = total + sums[half] * fade
                part = part + acc[dims, :] * fade
            tops[half] = top
            sums[half] = total
            acc[dims, :] = part

    @pl.loop(0, qkv_ref.shape[0] // TILE)
    def _(q_block):
        one_block(q_block, q_block, True)

        @pl.loop(0, q_block)
        def _(k_block):
            one_block(q_block, k_block, False)

        q_at = pl.ds(pl.multiple_of(q_block * TILE, TILE), TILE)
        for half in range(2):
            dims = pl.ds(half * HEAD, HEAD)
            acc[dims, :] = acc[dims, :] / sums[half]
            lse_ref[0, pl.ds(half, 1), q_at] = tops[half] + jnp.log(sums[half])
        turned_ref[0, :, q_at] = acc[...]
        store_true(
            inv_ref, out_ref, q_block * (TILE // STRETCH), column, acc[...].T.astype(jnp.bfloat16)
        )


def attend_backward_kernel(
    inv_ref, seg_row_ref, seg_col_ref, qkv_ref, grad_ref, turned_ref, lse_ref, out_ref,
    seg_row, seg_col, q_low, q_high, keys, keys_turned, values, g_low, g_high,
    query_acc, key_acc, value_acc, corrections,
):
    pair = pl.program_id(0)
    slots = grad_ref.shape[1]
    scale = HEAD ** (-0.5)

    @pl.when(pair == 0)
    def _():
        attend_prepare(inv_ref, seg_row_ref, seg_col_ref, seg_row, seg_col)

    column = pl.multiple_of(pair * LANES, LANES)
    queries = true_rows(inv_ref, qkv_ref, column) * jnp.bfloat16(scale)
    low_half = lax.broadcasted_iota(jnp.int32, queries.shape, 1) < HEAD
    zeros = jnp.zeros_like(queries)
    q_low[...] = jnp.where(low_half, queries, zeros)
    q_high[...] = jnp.where(low_half, zeros, queries)
    grads = true_rows(inv_ref, grad_ref, column)
    g_low[...] = jnp.where(low_half, grads, zeros)
    g_high[...] = jnp.where(low_half, zeros, grads)
    product = grads.astype(jnp.float32).T * turned_ref[0]
    corrections[0] = jnp.sum(product[:HEAD], axis=0, keepdims=True)
    corrections[1] = jnp.sum(product[HEAD:], axis=0, keepdims=True)
    keys_now = true_rows(inv_ref, qkv_ref, slots + column)
    keys[...] = keys_now
    keys_turned[...] = keys_now.astype(jnp.float32).T.astype(jnp.bfloat16)
    values[...] = true_rows(inv_ref, qkv_ref, 2 * slots + column)
    key_acc[...] = jnp.zeros_like(key_acc)
    value_acc[...] = jnp.zeros_like(value_acc)
    q_halves = (q_low, q_high)
    g_halves = (g_low, g_high)

    def one_block(q_block, k_block, first):
        q_at = pl.ds(pl.multiple_of(q_block * TILE, TILE), TILE)
        k_at = pl.ds(pl.multiple_of(k_block * TILE, TILE), TILE)
        same = seg_col[k_at, :] == seg_row[:, q_at]
        if first:
            same = same & (
                lax.broadcasted_iota(jnp.int32, (TILE, TILE), 0)
                <= lax.broadcasted_iota(jnp.int32, (TILE, TILE), 1)
            )
        value_sum = value_acc[k_at, :]
        key_sum = key_acc[k_at, :]
        for half in range(2):
            dims = pl.ds(half * HEAD, HEAD)
            query_rows = q_halves[half][q_at, :]
            grad_rows = g_halves[half][q_at, :]
            scores = times_transposed(keys[k_at, :], query_rows)
            lse = lse_ref[0, pl.ds(half, 1), q_at]
            probs = jnp.exp(jnp.where(same, scores - lse, masked_score))
            dots = times_transposed(values[k_at, :], grad_rows)
            delta = (probs * (dots - corrections[half, :, q_at])).astype(jnp.bfloat16)
            value_sum = value_sum + jnp.dot(
                probs.astype(jnp.bfloat16), grad_rows, preferred_element_type=jnp.float32
            )
            key_sum = key_sum + jnp.dot(delta, query_rows, preferred_element_type=jnp.float32)
            part = jnp.dot(keys_turned[dims, k_at], delta, preferred_element_type=jnp.float32)
            if first:
                query_acc[dims, :] = part
            else:
                query_acc[dims, :] += part
        value_acc[k_at, :] = value_sum
        key_acc[k_at, :] = key_sum

    @pl.loop(0, qkv_ref.shape[0] // TILE)
    def _(q_block):
        one_block(q_block, q_block, True)

        @pl.loop(0, q_block)
        def _(k_block):
            one_block(q_block, k_block, False)

        store_true(
            inv_ref,
            out_ref,
            q_block * (TILE // STRETCH),
            column,
            (query_acc[...].T * scale).astype(jnp.bfloat16),
        )

    store_true(inv_ref, out_ref, 0, slots + column, key_acc[...].astype(jnp.bfloat16))
    store_true(inv_ref, out_ref, 0, 2 * slots + column, value_acc[...].astype(jnp.bfloat16))


def whole_block(array):
    return pl.BlockSpec(array.shape, lambda *_, n=array.ndim: (0,) * n)


def attend_forward(inverse, seg_blocks, qkv):
    rows, wide = qkv.shape
    slots = wide // 3
    pairs = slots // LANES
    seg_col = seg_blocks.reshape(rows, 1)
    outs = (
        jax.ShapeDtypeStruct((rows, slots), jnp.bfloat16),
        jax.ShapeDtypeStruct((pairs, LANES, rows), jnp.float32),
        jax.ShapeDtypeStruct((pairs, 2, rows), jnp.float32),
    )
    low = jnp.bfloat16
    return pl.pallas_call(
        attend_forward_kernel,
        grid_spec=pltpu.PrefetchScalarGridSpec(
            num_scalar_prefetch=1,
            grid=(pairs,),
            in_specs=[whole_block(seg_blocks), whole_block(seg_col), whole_block(qkv)],
            out_specs=[
                whole_block(outs[0]),
                pl.BlockSpec((1, LANES, rows), lambda p, *_: (p, 0, 0)),
                pl.BlockSpec((1, 2, rows), lambda p, *_: (p, 0, 0)),
            ],
            scratch_shapes=[
                pltpu.VMEM((1, rows), jnp.int32),
                pltpu.VMEM((rows, 1), jnp.int32),
                pltpu.VMEM((rows, LANES), low),
                pltpu.VMEM((rows, LANES), low),
                pltpu.VMEM((rows, LANES), low),
                pltpu.VMEM((LANES, rows), low),
                pltpu.VMEM((LANES, TILE), jnp.float32),
                pltpu.VMEM((2, 1, TILE), jnp.float32),
                pltpu.VMEM((2, 1, TILE), jnp.float32),
            ],
        ),
        out_shape=outs,
        name="attend_forward",
    )(inverse, seg_blocks, seg_col, qkv)


def attend_backward(inverse, seg_blocks, qkv, grads, turned, lse):
    rows, wide = qkv.shape
    slots = wide // 3
    pairs = slots // LANES
    seg_col = seg_blocks.reshape(rows, 1)
    out = jax.ShapeDtypeStruct((rows, wide), jnp.bfloat16)
    low = jnp.bfloat16
    return pl.pallas_call(
        attend_backward_kernel,
        grid_spec=pltpu.PrefetchScalarGridSpec(
            num_scalar_prefetch=1,
            grid=(pairs,),
            in_specs=[
                whole_block(seg_blocks),
                whole_block(seg_col),
                whole_block(qkv),
                whole_block(grads),
                pl.BlockSpec((1, LANES, rows), lambda p, *_: (p, 0, 0)),
                pl.BlockSpec((1, 2, rows), lambda p, *_: (p, 0, 0)),
            ],
            out_specs=whole_block(out),
            scratch_shapes=[
                pltpu.VMEM((1, rows), jnp.int32),
                pltpu.VMEM((rows, 1), jnp.int32),
                pltpu.VMEM((rows, LANES), low),
                pltpu.VMEM((rows, LANES), low),
                pltpu.VMEM((rows, LANES), low),
                pltpu.VMEM((LANES, rows), low),
                pltpu.VMEM((rows, LANES), low),
                pltpu.VMEM((rows, LANES), low),
                pltpu.VMEM((rows, LANES), low),
                pltpu.VMEM((LANES, TILE), jnp.float32),
                pltpu.VMEM((rows, LANES), jnp.float32),
                pltpu.VMEM((rows, LANES), jnp.float32),
                pltpu.VMEM((2, 1, rows), jnp.float32),
            ],
        ),
        out_shape=out,
        name="attend_backward",
    )(inverse, seg_blocks, seg_col, qkv, grads, turned, lse)


def normalize(rows):
    center = rows - jnp.mean(rows, axis=-1, keepdims=True)
    spread = jnp.mean(center * center, axis=-1, keepdims=True)
    inverse = lax.rsqrt(spread + epsilon)
    return center * inverse, inverse


def normalize_back(grads, gain, unit, inverse):
    pulled = grads * gain
    return inverse * (
        pulled
        - jnp.mean(pulled, axis=-1, keepdims=True)
        - unit * jnp.mean(pulled * unit, axis=-1, keepdims=True)
    )


def gelu_parts(value):
    root = 0.7978845608028654
    inner = root * (value + 0.044715 * value * value * value)
    bend = jnp.tanh(inner)
    slope = 0.5 * (1.0 + bend) + 0.5 * value * (1.0 - bend * bend) * root * (
        1.0 + 3 * 0.044715 * value * value
    )
    return 0.5 * value * (1.0 + bend), slope


def mesh_copy(source, target, send, receive, device):
    return pltpu.make_async_remote_copy(
        src_ref=source,
        dst_ref=target,
        send_sem=send,
        recv_sem=receive,
        device_id=device,
        device_id_type=pl.DeviceIdType.MESH,
    )


def greet(devices):
    barrier = pltpu.get_barrier_semaphore()
    for device in devices:
        pl.semaphore_signal(
            barrier, inc=1, device_id=device, device_id_type=pl.DeviceIdType.MESH
        )
    pl.semaphore_wait(barrier, len(devices))


def fsdp_places():
    shard = lax.axis_index("fsdp")
    partner = shard + 1 - 2 * (shard % 2)
    return shard, partner, (shard + 2) % 4, (partner + 2) % 4


def ring_places(nc):
    place = lax.axis_index("ctx")
    z, y = place // 2, place % 2
    spot = z * (1 - y) + (nc - 1 - z) * y

    def holder(at):
        at = (at + nc) % nc
        side = at // (nc // 2)
        return (1 - side) * 2 * at + side * (2 * (nc - 1 - at) + 1)

    return spot, holder


def chunks_of(rows, count):
    step = -(-rows // count // 16) * 16
    return [(at, min(step, rows - at)) for at in range(0, rows, step)]


class FsdpGather:
    SEMS = 7

    def __init__(self, own, out, sems, parts=4):
        self.own, self.out, self.sems = own, out, sems
        self.shard, self.partner, self.cross, self.corner = fsdp_places()
        self.place = lax.axis_index("ctx")
        self.chunks = chunks_of(own.shape[0], parts)

    def peers(self):
        return [(self.partner, self.place), (self.cross, self.place)]

    def copy(self, kind, k):
        at, size = self.chunks[k]
        rows = pl.ds(at, size)
        if kind == "own":
            return pltpu.make_async_copy(
                self.own.at[rows], self.out.at[self.shard, rows], self.sems.at[6, k]
            )
        if kind == "across":
            source, slot, device, sem = self.own.at[rows], self.shard, self.cross, 0
        elif kind == "beside":
            source, slot, device, sem = self.own.at[rows], self.shard, self.partner, 2
        else:
            slot, device, sem = self.cross, self.partner, 4
            source = self.out.at[slot, rows]
        return mesh_copy(
            source,
            self.out.at[slot, rows],
            self.sems.at[sem, k],
            self.sems.at[sem + 1, k],
            (device, self.place),
        )

    def begin(self):
        for kind in ("across", "beside", "own"):
            for k in range(len(self.chunks)):
                self.copy(kind, k).start()

    def pass_on(self):
        for k in range(len(self.chunks)):
            self.copy("across", k).wait_recv()
            self.copy("on", k).start()

    def finish(self):
        for k in range(len(self.chunks)):
            self.copy("across", k).wait_send()
            self.copy("beside", k).wait()
            self.copy("on", k).wait()
            self.copy("own", k).wait()


class RingGather:
    def __init__(self, nc, own, out, sems):
        self.nc, self.own, self.out, self.sems = nc, own, out, sems
        self.spot, self.holder = ring_places(nc)
        self.shard = lax.axis_index("fsdp")
        rows = own.shape[0]
        self.half = rows // 2 // 8 * 8
        self.rows = rows

    def peers(self):
        return [(self.shard, self.holder(self.spot + way)) for way in (1, -1)]

    def copy(self, way, step):
        origin = self.holder(self.spot - way * (step - 1))
        rows = pl.ds(0, self.rows)
        if step == self.nc // 2:
            rows = pl.ds(0, self.half) if way == 1 else pl.ds(self.half, self.rows - self.half)
        source = self.own.at[rows] if step == 1 else self.out.at[origin, rows]
        side = 0 if way == 1 else 2
        return mesh_copy(
            source,
            self.out.at[origin, rows],
            self.sems.at[side, step - 1],
            self.sems.at[side + 1, step - 1],
            (self.shard, self.holder(self.spot + way)),
        )

    def keep(self):
        return pltpu.make_async_copy(
            self.own, self.out.at[lax.axis_index("ctx")], self.sems.at[4, 0]
        )

    def begin(self):
        for way in (1, -1):
            self.copy(way, 1).start()
        self.keep().start()

    def advance(self, step):
        for way in (1, -1):
            self.copy(way, step - 1).wait_recv()
            self.copy(way, step).start()

    def finish(self):
        last = self.nc // 2
        for way in (1, -1):
            for step in range(1, last + 1):
                self.copy(way, step).wait_send()
            self.copy(way, last).wait_recv()
        self.keep().wait()


def startup_kernel(nc, ring_count, row_count, *refs):
    total = ring_count + row_count
    ins, outs, sems = refs[:total], refs[total : 2 * total], refs[2 * total :]
    rings = [RingGather(nc, ins[k], outs[k], sems[k]) for k in range(ring_count)]
    sides = [FsdpGather(ins[k], outs[k], sems[k]) for k in range(ring_count, total)]
    greet(rings[0].peers() + (sides[0].peers() if sides else []))
    for ring in rings:
        ring.begin()
    for side in sides:
        side.begin()
    for step in range(2, nc // 2 + 1):
        if step - 2 < len(sides):
            sides[step - 2].pass_on()
        for ring in rings:
            ring.advance(step)
    for side in sides:
        side.finish()
    for ring in rings:
        ring.finish()


def gather_fsdp_kernel(own_ref, out_ref, sems):
    side = FsdpGather(own_ref, out_ref, sems)
    greet(side.peers())
    side.begin()
    side.pass_on()
    side.finish()


def add_rows(target, source, rows):
    first, size = rows
    step = 16 if size % 16 == 0 else 8

    @pl.loop(0, size // step)
    def _(turn):
        at = pl.ds(pl.multiple_of(first + turn * step, 8), step)
        target[at] = (target[at].astype(jnp.float32) + source[at].astype(jnp.float32)).astype(
            target.dtype
        )


def set_rows(target, source, rows):
    first, size = rows
    step = 16 if size % 16 == 0 else 8

    @pl.loop(0, size // step)
    def _(turn):
        at = pl.ds(pl.multiple_of(first + turn * step, 8), step)
        target[at] = source[at]


def scatter_fsdp_kernel(part_ref, out_ref, first_in, own_in, chip_sum, across_in, sems):
    shard, partner, cross, corner = fsdp_places()
    place = lax.axis_index("ctx")
    greet([(partner, place), (cross, place)])
    chunks = chunks_of(out_ref.shape[0], 4)

    def copy(kind, k):
        at, size = chunks[k]
        rows = pl.ds(at, size)
        if kind == 0:
            source, target, device = part_ref.at[corner, rows], first_in, partner
        elif kind == 1:
            source, target, device = part_ref.at[partner, rows], own_in, partner
        else:
            source, target, device = chip_sum.at[rows], across_in, cross
        return mesh_copy(
            source,
            target.at[rows],
            sems.at[2 * kind, k],
            sems.at[2 * kind + 1, k],
            (device, place),
        )

    for kind in range(2):
        for k in range(len(chunks)):
            copy(kind, k).start()
    for k, (at, size) in enumerate(chunks):
        copy(0, k).wait_recv()

        @pl.loop(0, size // 16)
        def _(turn):
            rows = pl.ds(pl.multiple_of(at + turn * 16, 16), 16)
            chip_sum[rows] = (
                part_ref[cross, rows].astype(jnp.float32) + first_in[rows].astype(jnp.float32)
            ).astype(chip_sum.dtype)

        copy(2, k).start()
    for k, (at, size) in enumerate(chunks):
        copy(1, k).wait_recv()
        copy(2, k).wait_recv()

        @pl.loop(0, size // 16)
        def _(turn):
            rows = pl.ds(pl.multiple_of(at + turn * 16, 16), 16)
            out_ref[rows] = (
                part_ref[shard, rows].astype(jnp.float32)
                + own_in[rows].astype(jnp.float32)
                + across_in[rows].astype(jnp.float32)
            )

    for kind in range(3):
        for k in range(len(chunks)):
            copy(kind, k).wait_send()


class RingScatter:
    def __init__(self, nc, mine, out, right, left, sems):
        self.nc, self.mine, self.out, self.sems = nc, mine, out, sems
        self.inbox = {1: right, -1: left}
        self.spot, self.holder = ring_places(nc)
        self.shard = lax.axis_index("fsdp")
        self.rows = out.shape[0]
        self.half = self.rows // 2 // 8 * 8

    def peers(self):
        return [(self.shard, self.holder(self.spot + way)) for way in (1, -1)]

    def copy(self, way, step):
        inbox = self.inbox[way]
        rows = pl.ds(0, self.rows)
        if step == 1:
            rows = pl.ds(0, self.half) if way == 1 else pl.ds(self.half, self.rows - self.half)
            source = self.mine.at[self.holder(self.spot + self.nc // 2), rows]
        else:
            source = inbox.at[step - 2, rows]
        side = 0 if way == 1 else 2
        return mesh_copy(
            source,
            inbox.at[step - 1, rows],
            self.sems.at[side, step - 1],
            self.sems.at[side + 1, step - 1],
            (self.shard, self.holder(self.spot + way)),
        )

    def begin(self):
        for way in (1, -1):
            self.copy(way, 1).start()

    def advance(self, step):
        for way in (1, -1):
            self.copy(way, step - 1).wait_recv()
            box = self.inbox[way].at[step - 2]
            mine = self.mine.at[self.holder(self.spot + way * (self.nc // 2 + 1 - step))]
            if step == 2:
                low, high = (0, self.half), (self.half, self.rows - self.half)
                got, rest = (low, high) if way == 1 else (high, low)
                add_rows(box, mine, got)
                set_rows(box, mine, rest)
            else:
                add_rows(box, mine, (0, self.rows))
            self.copy(way, step).start()

    def finish(self):
        last = self.nc // 2
        for way in (1, -1):
            self.copy(way, last).wait_recv()
        right, left = self.inbox[1].at[last - 1], self.inbox[-1].at[last - 1]
        mine = self.mine.at[lax.axis_index("ctx")]
        step = 16 if self.rows % 16 == 0 else 8

        @pl.loop(0, self.rows // step)
        def _(turn):
            at = pl.ds(pl.multiple_of(turn * step, 8), step)
            self.out[at] = (
                mine[at].astype(jnp.float32)
                + right[at].astype(jnp.float32)
                + left[at].astype(jnp.float32)
            ).astype(self.out.dtype)

        for way in (1, -1):
            for step in range(1, last + 1):
                self.copy(way, step).wait_send()


def scatter_ctx_kernel(nc, count, *refs):
    ins, outs, rest = refs[:count], refs[count : 2 * count], refs[2 * count :]
    rings = [
        RingScatter(nc, ins[k], outs[k], rest[3 * k], rest[3 * k + 1], rest[3 * k + 2])
        for k in range(count)
    ]
    greet(rings[0].peers())
    for ring in rings:
        ring.begin()
    for step in range(2, nc // 2 + 1):
        for ring in rings:
            ring.advance(step)
    for ring in rings:
        ring.finish()


def trade_kernel(axes, sizes, *refs):
    count = len(axes)
    ins, outs, sems = refs[:count], refs[count : 2 * count], refs[2 * count :]
    place = {"fsdp": lax.axis_index("fsdp"), "ctx": lax.axis_index("ctx")}

    def device(axis, at):
        return (at, place["ctx"]) if axis == "fsdp" else (place["fsdp"], at)

    peers = []
    for axis in sorted(set(axes)):
        for k in range(1, sizes[axis]):
            peers.append(device(axis, (place[axis] + k) % sizes[axis]))
    greet(peers)
    copies, stays = [], []
    for j in range(count):
        axis = axes[j]
        me = place[axis]
        stay = pltpu.make_async_copy(ins[j].at[me], outs[j].at[me], sems[j].at[2, 0])
        stay.start()
        stays.append(stay)
        for k in range(1, sizes[axis]):
            other = (me + k) % sizes[axis]
            copy = mesh_copy(
                ins[j].at[other],
                outs[j].at[me],
                sems[j].at[0, k],
                sems[j].at[1, k],
                device(axis, other),
            )
            copy.start()
            copies.append(copy)
    for copy in copies:
        copy.wait()
    for stay in stays:
        stay.wait()


def in_vmem():
    return pl.BlockSpec(memory_space=pltpu.VMEM)


def in_place():
    return pl.BlockSpec(memory_space=pl.ANY)


def widen(pieces):
    return jnp.pad(pieces, ((0, 0),) * (pieces.ndim - 1) + ((0, -pieces.shape[-1] % LANES),))


class Net:
    def __init__(self, nf, nc):
        self.nf, self.nc = nf, nc
        self.each = nc // nf
        self.ids = {}

    def call(self, kernel, key, outs, ins, in_specs, out_specs, scratch, name):
        ident = self.ids.setdefault(key, len(self.ids))
        return pl.pallas_call(
            kernel,
            out_shape=outs,
            in_specs=in_specs,
            out_specs=out_specs,
            scratch_shapes=scratch,
            compiler_params=pltpu.CompilerParams(
                collective_id=ident, has_side_effects=True, vmem_limit_bytes=60 << 20
            ),
            name=name,
        )(*ins)

    def to_column(self, f, c, i):
        return 2 * (c // 2 % 2) + c // 4, 2 * (2 * (f % 2) + i) + f // 2, c % 2

    def to_origin(self, f, c, j):
        return 2 * (c % 2) + c // 4, 2 * (2 * (f % 2) + f // 2) + j, c // 2 % 2

    def blocks_in_order(self):
        return [self.to_origin(k // 2, 0, k % 2)[1] for k in range(self.nc)]

    def sequence_of(self, place):
        return self.each * (2 * (place % 2) + place // 4) + place // 2 % 2

    def swap_blocks(self, blocks, move):
        place = lax.axis_index("ctx")
        out_slot = move(0, place, 0)[2]
        got = []
        for turn in range(self.each):
            slot = (out_slot + turn) % self.each
            piece = lax.dynamic_index_in_dim(blocks, slot, 0, keepdims=False)
            pairs = []
            for f in range(self.nf):
                for c in range(self.nc):
                    there = move(f, c, (move(f, c, 0)[2] + turn) % self.each)
                    pairs.append((f * self.nc + c, there[0] * self.nc + there[1]))
            got.append(lax.ppermute(piece, ("fsdp", "ctx"), pairs))
        back = self.to_origin if move == self.to_column else self.to_column
        own_slot = back(0, place, 0)[2]
        order = (own_slot - jnp.arange(self.each)) % self.each
        return jnp.take(jnp.stack(got), order, axis=0)

    def trade(self, arrays, axes):
        sizes = {"fsdp": self.nf, "ctx": self.nc}
        extents = [a.shape[-1] for a in arrays]
        arrays = [widen(a) for a in arrays]
        key = ("trade",) + tuple((a.shape, x) for a, x in zip(arrays, axes))
        outs = tuple(jax.ShapeDtypeStruct(a.shape, a.dtype) for a in arrays)
        count = len(arrays)
        got = self.call(
            functools.partial(trade_kernel, tuple(axes), sizes),
            key, outs, arrays, [in_vmem()] * count, [in_place()] * count,
            [pltpu.SemaphoreType.DMA((3, sizes[x])) for x in axes],
            "trade",
        )
        return [whole[..., :extent] for whole, extent in zip(got, extents)]

    def trade_fsdp(self, pieces):
        return self.trade([pieces], ["fsdp"])[0]

    def trade_ctx(self, pieces):
        return self.trade([pieces], ["ctx"])[0]

    def startup(self, blocks, rows):
        arrays = list(blocks) + list(rows)
        outs = [jax.ShapeDtypeStruct((self.nc,) + a.shape, a.dtype) for a in blocks]
        outs += [jax.ShapeDtypeStruct((self.nf,) + a.shape, a.dtype) for a in rows]
        sems = [pltpu.SemaphoreType.DMA((5, self.nc // 2)) for _ in blocks]
        sems += [pltpu.SemaphoreType.DMA((FsdpGather.SEMS, 8)) for _ in rows]
        count = len(arrays)
        key = ("startup",) + tuple(a.shape for a in arrays)
        return self.call(
            functools.partial(startup_kernel, self.nc, len(blocks), len(rows)),
            key, tuple(outs), arrays, [in_vmem()] * count, [in_place()] * count, sems, "startup",
        )

    def gather_ctx(self, block):
        return lax.all_gather(block, "ctx", axis=0)

    def scatter_ctx(self, blocks):
        return lax.psum_scatter(blocks, "ctx", scatter_dimension=0)

    def ring_scatter(self, arrays):
        outs, scratch = [], []
        for a in arrays:
            outs.append(jax.ShapeDtypeStruct(a.shape[1:], a.dtype))
            box = pltpu.VMEM((self.nc // 2,) + a.shape[1:], a.dtype)
            scratch += [box, box, pltpu.SemaphoreType.DMA((4, self.nc // 2))]
        count = len(arrays)
        key = ("ring",) + tuple(a.shape for a in arrays)
        return self.call(
            functools.partial(scatter_ctx_kernel, self.nc, count),
            key, tuple(outs), arrays, [in_vmem()] * count, [in_vmem()] * count, scratch,
            "ring_scatter",
        )

    def gather_fsdp(self, rows):
        out = self.call(
            gather_fsdp_kernel,
            ("gather", rows.shape),
            jax.ShapeDtypeStruct((self.nf,) + rows.shape, rows.dtype),
            [rows], [in_vmem()], in_place(),
            [pltpu.SemaphoreType.DMA((FsdpGather.SEMS, 8))],
            "gather_fsdp",
        )
        return out.reshape((-1,) + rows.shape[1:])

    def scatter_fsdp(self, rows):
        count = rows.shape[0] // self.nf
        block = (count,) + rows.shape[1:]
        box = pltpu.VMEM(block, rows.dtype)
        return self.call(
            scatter_fsdp_kernel,
            ("scatter", rows.shape),
            jax.ShapeDtypeStruct(block, jnp.float32),
            [rows.reshape((self.nf,) + block)], [in_vmem()], in_vmem(),
            [box, box, box, box, pltpu.SemaphoreType.DMA((6, 8))],
            "scatter_fsdp",
        )


def local_fast(
    net,
    inputs,
    cotangent,
    segments,
    stretch_order,
    prenorm_gain,
    prenorm_shift,
    joint_weight,
    query_bias,
    value_bias,
    mixer_weight,
    mixer_bias,
    midnorm_gain,
    midnorm_shift,
    expand_weight,
    expand_bias,
    shrink_weight,
    shrink_bias,
):
    nf, nc, each = net.nf, net.nc, net.each
    low, wide = jnp.bfloat16, jnp.float32
    _, stretch_len, width = inputs.shape
    heads_each = -(-(width // HEAD) // nf)
    span = heads_each * HEAD
    slots = slot_width(heads_each)
    rows_all = nc * stretch_len
    rows_own = each * stretch_len
    shard = lax.axis_index("fsdp")
    place = lax.axis_index("ctx")
    in_order = net.blocks_in_order()
    inverse = jnp.sum(
        jnp.where(
            jnp.stack([stretch_order[k] for k in in_order])[None, :] == jnp.arange(nc, dtype=jnp.int32)[:, None],
            jnp.arange(nc, dtype=jnp.int32)[None, :],
            0,
        ),
        axis=1,
    ).astype(jnp.int32)

    narrow = prenorm_gain.shape[0]
    unit_each = expand_bias.shape[0] // nf

    own_tokens = net.swap_blocks(inputs, net.to_column).reshape(rows_own, width)
    own_tangent = net.swap_blocks(cotangent, net.to_column).reshape(rows_own, width)

    depth = joint_weight.shape[0]
    thin = -(-depth // (8 * nc)) * 8
    out_each = shrink_weight.shape[1]
    seg_own = jnp.pad(segments.astype(low), ((0, 16 - each), (0, 0)))
    joint_tall = jnp.pad(joint_weight, ((0, nc * thin - depth), (0, 0)))
    joint_pieces, expand_pieces, shrink_pieces, seg_pieces = net.trade(
        [
            joint_tall.reshape(nc, thin, joint_weight.shape[1]),
            expand_weight.T.reshape(nf, unit_each, depth),
            shrink_weight.reshape(each, nf, unit_each, out_each)
            .transpose(1, 0, 2, 3)
            .reshape(nf, each * unit_each, out_each),
            jnp.broadcast_to(seg_own[None], (nf,) + seg_own.shape),
        ],
        ["ctx", "fsdp", "fsdp", "fsdp"],
    )
    small_parts = (
        prenorm_gain, prenorm_shift, query_bias, value_bias, mixer_bias,
        midnorm_gain, midnorm_shift, shrink_bias, expand_bias,
    )
    small_own = jnp.concatenate(small_parts)
    small_count = small_own.shape[0]
    small_rows = -(-small_count // (16 * LANES)) * 16
    small_own = jnp.pad(small_own, (0, small_rows * LANES - small_count))
    small_own = jnp.concatenate(
        [small_own.reshape(small_rows, LANES), seg_pieces[:, :each].reshape(nf * each, LANES)]
    )
    small_own = jnp.pad(small_own, ((0, -small_own.shape[0] % 16), (0, 0)))
    joint_pieces = joint_pieces.transpose(1, 0, 2).reshape(thin, 3, width)
    joint_pieces = net.trade_fsdp(joint_split(joint_pieces, nf, heads_each))
    expand_pieces = expand_pieces.transpose(1, 0, 2).reshape(unit_each, width)
    shrink_pieces = shrink_pieces.reshape(nc * unit_each, out_each).T

    step = span - mixer_weight.shape[0]
    most = step * (nf - 1)
    above = lax.ppermute(
        mixer_weight[:most], "fsdp", [(f, (f - 1) % nf) for f in range(nf)]
    )
    tall = jnp.concatenate([mixer_weight, above, jnp.zeros_like(above)])
    mixer_rows = lax.dynamic_slice_in_dim(tall, step * shard, span, 0)
    kept = shard * span + jnp.arange(span, dtype=jnp.int32) < width
    mixer_rows = jnp.where(kept[:, None], mixer_rows, jnp.zeros_like(mixer_rows))
    mixer_pieces = jnp.pad(mixer_rows.T, ((0, 0), (0, slots - span)))

    joint, mixer, expand, shrink, small_all, tokens, tangent = net.startup(
        [
            joint_pieces.reshape(nf * thin, 3 * slots),
            mixer_pieces,
            expand_pieces,
            shrink_pieces,
            small_own,
        ],
        [own_tokens, own_tangent],
    )
    expand = expand.reshape(nc * unit_each, width)
    joint = joint.reshape(nc, nf, thin, 3 * slots).transpose(1, 0, 2, 3)
    joint = joint.reshape(nf, nc * thin, 3 * slots)[:, :depth].reshape(width, 3 * slots)
    mixer = mixer.reshape(width, slots)
    shrink = shrink.reshape(width, nc * unit_each)
    tokens = tokens.reshape(rows_all, width)
    tangent = tangent.reshape(rows_all, width)
    seg_blocks = lax.dynamic_index_in_dim(
        small_all[:, small_rows : small_rows + nf * each],
        net.sequence_of(place),
        1,
        keepdims=False,
    ).astype(jnp.int32)
    seg_blocks = jnp.stack([seg_blocks[k] for k in in_order])
    small_all = small_all[:, :small_rows].reshape(nc, small_rows * LANES)[:, :small_count]
    smalls = [
        small_all[:, k * narrow : (k + 1) * narrow].reshape(width).astype(wide) for k in range(8)
    ]
    gain_one, shift_one, qbias, vbias, mbias, gain_two, shift_two, sbias = smalls
    ebias = lax.dynamic_index_in_dim(
        small_all[:, 8 * narrow :].reshape(nc, nf, unit_each), shard, 1, keepdims=False
    ).reshape(nc * unit_each).astype(wide)
    joint_bias = lax.dynamic_index_in_dim(
        joint_split(
            jnp.stack([qbias, jnp.zeros_like(qbias), vbias])[None], nf, heads_each
        ),
        shard, 0, keepdims=False,
    )

    token_values = tokens.astype(wide)
    unit_one, _ = normalize(token_values)
    normed = (unit_one * gain_one + shift_one).astype(low)
    qkv = (
        jnp.dot(normed, joint, preferred_element_type=wide) + joint_bias
    ).astype(low)
    attended, turned, lse = attend_forward(inverse, seg_blocks, qkv)
    branch = net.scatter_fsdp(times_transposed(attended, mixer).astype(low))
    middle = own_tokens.astype(wide) + branch + mbias
    unit_two, inverse_two = normalize(middle)
    second_own = (unit_two * gain_two + shift_two).astype(low)
    second = net.gather_fsdp(second_own)
    expanded = times_transposed(second, expand) + ebias
    active, slope = gelu_parts(expanded)
    active = active.astype(low)
    lifted = net.scatter_fsdp(times_transposed(active, shrink).astype(low))
    out_rows = (middle + lifted + sbias).astype(low)
    block_output = net.swap_blocks(out_rows.reshape(each, stretch_len, width), net.to_origin)

    shrink_grad = net.scatter_ctx(
        outer_sum(tangent, active).astype(low).reshape(nc, out_each, nc * unit_each)
    )
    active_grad = jnp.dot(tangent, shrink, preferred_element_type=wide)
    expand_delta = (active_grad * slope).astype(low)
    expand_grad = net.scatter_ctx(
        outer_sum(expand_delta, second).astype(low).reshape(nc, unit_each, width)
    )
    second_grad = net.scatter_fsdp(
        jnp.dot(expand_delta, expand, preferred_element_type=wide).astype(low)
    )
    middle_delta = own_tangent.astype(wide) + normalize_back(
        second_grad, gain_two, unit_two, inverse_two
    )
    branch_own = middle_delta.astype(low)
    branch_delta = net.gather_fsdp(branch_own)
    attended_delta = jnp.dot(branch_delta, mixer, preferred_element_type=wide).astype(low)
    mixer_rows = outer_sum(branch_delta, attended).astype(low).reshape(nc, out_each, slots)
    joint_delta = attend_backward(inverse, seg_blocks, qkv, attended_delta, turned, lse)
    normed_grad = net.scatter_fsdp(times_transposed(joint_delta, joint).astype(low))
    unit_own, inverse_own = normalize(own_tokens.astype(wide))
    input_rows = middle_delta + normalize_back(normed_grad, gain_one, unit_own, inverse_own)
    input_gradient = net.swap_blocks(
        input_rows.astype(low).reshape(each, stretch_len, width), net.to_origin
    ).astype(wide)

    mine = jnp.arange(nf, dtype=jnp.int32) == shard
    sums = jnp.sum(joint_delta.astype(wide), axis=0).reshape(3, slots)[:, :span]
    spread = jnp.where(mine[None, :, None], sums[:, None, :], 0.0).reshape(3, nf * span)
    unit_sums = jnp.sum(expand_delta.astype(wide), axis=0).reshape(nc, 1, unit_each)
    unit_sums = jnp.where(mine[None, :, None], unit_sums, 0.0).reshape(nc, nf * unit_each)
    vectors = (
        jnp.sum(normed_grad * unit_own, axis=0),
        jnp.sum(normed_grad, axis=0),
        spread[0, :width],
        spread[2, :width],
        jnp.sum(branch_own.astype(wide), axis=0),
        jnp.sum(second_grad * unit_two, axis=0),
        jnp.sum(second_grad, axis=0),
        jnp.sum(own_tangent.astype(wide), axis=0),
    )
    stacked = jnp.concatenate([v.reshape(nc, narrow) for v in vectors] + [unit_sums], axis=1)
    stacked = jnp.pad(stacked, ((0, 0), (0, small_rows * LANES - small_count)))
    small_blocks = stacked.astype(low).reshape(nc, small_rows, LANES)

    joint_rows = outer_sum(normed, joint_delta).astype(low)
    joint_rows = jnp.pad(
        joint_rows.reshape(nf, depth, 3 * slots), ((0, 0), (0, nc * thin - depth), (0, 0))
    )
    joint_rows = joint_rows.reshape(nf, nc, thin, 3 * slots).transpose(1, 0, 2, 3)
    joint_grad, mixer_grad, small_grad = net.ring_scatter(
        [joint_rows.reshape(nc, nf * thin, 3 * slots), mixer_rows, small_blocks]
    )
    joint_pieces, expand_pieces, shrink_pieces, small_pieces = net.trade(
        [
            joint_grad.reshape(nf, thin, 3 * slots),
            expand_grad.reshape(unit_each, nf, depth).transpose(1, 0, 2),
            shrink_grad.T.reshape(nf, each * unit_each, out_each),
            jnp.broadcast_to(small_grad[None], (nf,) + small_grad.shape),
        ],
        ["fsdp"] * 4,
    )
    joint_pieces = joint_join(joint_pieces, heads_each, width)
    joint_pieces = joint_pieces.reshape(thin, nc, joint_weight.shape[1]).transpose(1, 0, 2)
    joint_gradient = (
        net.trade_ctx(joint_pieces)
        .reshape(nc * thin, joint_weight.shape[1])[:depth]
        .astype(wide)
    )
    expand_gradient = expand_pieces.reshape(nf * unit_each, depth).T.astype(wide)
    shrink_pieces = shrink_pieces.reshape(nf, each, unit_each, out_each).transpose(1, 0, 2, 3)
    shrink_gradient = shrink_pieces.reshape(shrink_weight.shape).astype(wide)

    own_rows = mixer_grad[:, :span].T
    below = lax.dynamic_slice_in_dim(
        jnp.pad(own_rows, ((0, most), (0, 0))), mixer_weight.shape[0] - step * shard, most, 0
    )
    below = lax.ppermute(below, "fsdp", [(f, (f + 1) % nf) for f in range(nf)])
    moved = lax.dynamic_slice_in_dim(
        jnp.pad(own_rows, ((most, 0), (0, 0))), most - step * shard, mixer_weight.shape[0], 0
    )
    first_rows = jnp.arange(mixer_weight.shape[0], dtype=jnp.int32)[:, None] < step * shard
    below = jnp.pad(below, ((0, mixer_weight.shape[0] - most), (0, 0)))
    mixer_gradient = jnp.where(first_rows, below, moved).astype(wide)

    small_sum = jnp.sum(small_pieces.astype(wide), axis=0).reshape(small_rows * LANES)
    outs = [small_sum[k * narrow : (k + 1) * narrow] for k in range(8)]
    return (
        block_output,
        input_gradient,
        outs[0],
        outs[1],
        joint_gradient,
        outs[2],
        outs[3],
        mixer_gradient,
        outs[4],
        outs[5],
        outs[6],
        expand_gradient,
        small_sum[8 * narrow : small_count],
        shrink_gradient,
        outs[7],
    )


def solution(mesh):
    in_specs = (
        P("fsdp", "ctx", None),
        P("fsdp", "ctx", None),
        P("fsdp", "ctx"),
        P(),
        P("ctx"),
        P("ctx"),
        P("fsdp", "ctx"),
        P("ctx"),
        P("ctx"),
        P("fsdp", "ctx"),
        P("ctx"),
        P("ctx"),
        P("ctx"),
        P("fsdp", "ctx"),
        P("ctx"),
        P("fsdp", "ctx"),
        P("ctx"),
    )
    out_specs = (
        P("fsdp", "ctx", None),
        P("fsdp", "ctx", None),
        P("ctx"),
        P("ctx"),
        P("fsdp", "ctx"),
        P("ctx"),
        P("ctx"),
        P("fsdp", "ctx"),
        P("ctx"),
        P("ctx"),
        P("ctx"),
        P("fsdp", "ctx"),
        P("ctx"),
        P("fsdp", "ctx"),
        P("ctx"),
    )

    def run(*arrays):
        nf, nc = mesh.shape["fsdp"], mesh.shape["ctx"]
        whole_each = arrays[0].shape[0] == nc and (nf, nc) == (4, 8)
        if whole_each and arrays[0].shape[1] == nc * STRETCH:
            body = functools.partial(local_fast, Net(nf, nc))
        else:
            body = local
        return jax.shard_map(
            body, mesh=mesh, in_specs=in_specs, out_specs=out_specs, check_vma=False
        )(*arrays)

    return run
```

```python
import functools

import jax
import jax.numpy as jnp
from jax import lax
from jax.experimental import pallas as pl
from jax.experimental.pallas import tpu as pltpu
from jax.sharding import PartitionSpec as P


HEAD = 64
MICRO = 2
LANES = 128
STRETCH = 128
TILE = 256


epsilon = 1e-05
masked_score = -1e30


def layer_norm(values, gain, shift):
    center = values - jnp.mean(values, axis=-1, keepdims=True)
    spread = jnp.mean(center * center, axis=-1, keepdims=True)
    return center * lax.rsqrt(spread + epsilon) * gain + shift


def piece_size(count):
    size_now = min(count, 512)
    while count % size_now:
        size_now -= 1
    return size_now


def true_positions(stretch_order, first_index, count, stretch_len):
    stored = first_index + jnp.arange(count, dtype=jnp.int32)
    holder = stored // stretch_len
    picked = holder[:, None] == jnp.arange(stretch_order.shape[0], dtype=jnp.int32)[None, :]
    return (
        jnp.sum(jnp.where(picked, stretch_order[None, :], 0), axis=1) * stretch_len
        + stored % stretch_len
    )


def times_transposed(left, right):
    return lax.dot_general(
        left, right, (((1,), (1,)), ((), ())), preferred_element_type=jnp.float32
    )


def outer_sum(left, right):
    return lax.dot_general(
        left, right, (((0,), (0,)), ((), ())), preferred_element_type=jnp.float32
    )


def fetch_weights(local_parts):
    (
        joint_weight,
        mixer_weight,
        expand_weight,
        shrink_weight,
        prenorm_gain,
        prenorm_shift,
        query_bias,
        value_bias,
        mixer_bias,
        midnorm_gain,
        midnorm_shift,
        expand_bias,
        shrink_bias,
    ) = local_parts
    spread_out = (
        lax.all_gather(joint_weight, "ctx", axis=1, tiled=True),
        lax.all_gather(mixer_weight, "ctx", axis=1, tiled=True),
        lax.all_gather(expand_weight, "ctx", axis=1, tiled=True),
        lax.all_gather(shrink_weight, "ctx", axis=1, tiled=True),
        lax.all_gather(prenorm_gain, "ctx", axis=0, tiled=True),
        lax.all_gather(prenorm_shift, "ctx", axis=0, tiled=True),
        lax.all_gather(query_bias, "ctx", axis=0, tiled=True),
        lax.all_gather(value_bias, "ctx", axis=0, tiled=True),
        lax.all_gather(mixer_bias, "ctx", axis=0, tiled=True),
        lax.all_gather(midnorm_gain, "ctx", axis=0, tiled=True),
        lax.all_gather(midnorm_shift, "ctx", axis=0, tiled=True),
        lax.all_gather(expand_bias, "ctx", axis=0, tiled=True),
        lax.all_gather(shrink_bias, "ctx", axis=0, tiled=True),
    )
    whole_rows = (
        lax.all_gather(spread_out[0], "fsdp", axis=0, tiled=True),
        lax.all_gather(spread_out[1], "fsdp", axis=0, tiled=True),
        lax.all_gather(spread_out[2], "fsdp", axis=0, tiled=True),
        lax.all_gather(spread_out[3], "fsdp", axis=0, tiled=True),
    )
    return tuple(whole_rows) + tuple(spread_out[4:])


def reduce_gradients(matrices, smalls):
    small_sums = (
        lax.psum(smalls[0].astype(jnp.bfloat16), "fsdp").astype(jnp.float32),
        lax.psum(smalls[1].astype(jnp.bfloat16), "fsdp").astype(jnp.float32),
        lax.psum(smalls[2].astype(jnp.bfloat16), "fsdp").astype(jnp.float32),
        lax.psum(smalls[3].astype(jnp.bfloat16), "fsdp").astype(jnp.float32),
        lax.psum(smalls[4].astype(jnp.bfloat16), "fsdp").astype(jnp.float32),
        lax.psum(smalls[5].astype(jnp.bfloat16), "fsdp").astype(jnp.float32),
        lax.psum(smalls[6].astype(jnp.bfloat16), "fsdp").astype(jnp.float32),
        lax.psum(smalls[7].astype(jnp.bfloat16), "fsdp").astype(jnp.float32),
        lax.psum(smalls[8].astype(jnp.bfloat16), "fsdp").astype(jnp.float32),
    )
    column_part = (
        lax.psum_scatter(
            matrices[0].astype(jnp.bfloat16), "ctx", scatter_dimension=1, tiled=True
        ).astype(jnp.float32),
        lax.psum_scatter(
            matrices[1].astype(jnp.bfloat16), "ctx", scatter_dimension=1, tiled=True
        ).astype(jnp.float32),
        lax.psum_scatter(
            matrices[2].astype(jnp.bfloat16), "ctx", scatter_dimension=1, tiled=True
        ).astype(jnp.float32),
        lax.psum_scatter(
            matrices[3].astype(jnp.bfloat16), "ctx", scatter_dimension=1, tiled=True
        ).astype(jnp.float32),
        lax.psum_scatter(
            small_sums[0].astype(jnp.bfloat16), "ctx", scatter_dimension=0, tiled=True
        ).astype(jnp.float32),
        lax.psum_scatter(
            small_sums[1].astype(jnp.bfloat16), "ctx", scatter_dimension=0, tiled=True
        ).astype(jnp.float32),
        lax.psum_scatter(
            small_sums[2].astype(jnp.bfloat16), "ctx", scatter_dimension=0, tiled=True
        ).astype(jnp.float32),
        lax.psum_scatter(
            small_sums[3].astype(jnp.bfloat16), "ctx", scatter_dimension=0, tiled=True
        ).astype(jnp.float32),
        lax.psum_scatter(
            small_sums[4].astype(jnp.bfloat16), "ctx", scatter_dimension=0, tiled=True
        ).astype(jnp.float32),
        lax.psum_scatter(
            small_sums[5].astype(jnp.bfloat16), "ctx", scatter_dimension=0, tiled=True
        ).astype(jnp.float32),
        lax.psum_scatter(
            small_sums[6].astype(jnp.bfloat16), "ctx", scatter_dimension=0, tiled=True
        ).astype(jnp.float32),
        lax.psum_scatter(
            small_sums[7].astype(jnp.bfloat16), "ctx", scatter_dimension=0, tiled=True
        ).astype(jnp.float32),
        lax.psum_scatter(
            small_sums[8].astype(jnp.bfloat16), "ctx", scatter_dimension=0, tiled=True
        ).astype(jnp.float32),
    )
    row_part = (
        lax.psum_scatter(
            column_part[0].astype(jnp.bfloat16), "fsdp", scatter_dimension=0, tiled=True
        ).astype(jnp.float32),
        lax.psum_scatter(
            column_part[1].astype(jnp.bfloat16), "fsdp", scatter_dimension=0, tiled=True
        ).astype(jnp.float32),
        lax.psum_scatter(
            column_part[2].astype(jnp.bfloat16), "fsdp", scatter_dimension=0, tiled=True
        ).astype(jnp.float32),
        lax.psum_scatter(
            column_part[3].astype(jnp.bfloat16), "fsdp", scatter_dimension=0, tiled=True
        ).astype(jnp.float32),
    )
    return tuple(row_part) + tuple(column_part[4:])


def local(
    inputs,
    cotangent,
    segments,
    stretch_order,
    prenorm_gain,
    prenorm_shift,
    joint_weight,
    query_bias,
    value_bias,
    mixer_weight,
    mixer_bias,
    midnorm_gain,
    midnorm_shift,
    expand_weight,
    expand_bias,
    shrink_weight,
    shrink_bias,
):
    local_parts = (
        joint_weight,
        mixer_weight,
        expand_weight,
        shrink_weight,
        prenorm_gain,
        prenorm_shift,
        query_bias,
        value_bias,
        mixer_bias,
        midnorm_gain,
        midnorm_shift,
        expand_bias,
        shrink_bias,
    )
    seq_local, stretch_len, model_width = inputs.shape
    head_count = model_width // HEAD
    group_size = seq_local // MICRO
    row_count = group_size * stretch_len
    score_scale = HEAD ** (-0.5)
    ctx_place = lax.axis_index("ctx")
    own_stretch = jnp.sum(
        jnp.where(
            jnp.arange(stretch_order.shape[0], dtype=jnp.int32) == ctx_place, stretch_order, 0
        )
    )
    own_pos = own_stretch * stretch_len + jnp.arange(stretch_len, dtype=jnp.int32)
    all_segments = lax.all_gather(segments, "ctx", axis=1, tiled=True)

    def backward_micro(weights, kept_values, micro_index):
        (
            joint_full,
            mixer_full,
            expand_full,
            shrink_full,
            gain_one,
            shift_one,
            _,
            _,
            _,
            gain_two,
            shift_two,
            _,
            _,
        ) = weights
        (
            tokens,
            seg_local,
            seg_whole,
            normed,
            queries,
            keys_local,
            values_local,
            mixed_rows,
            attended,
            log_total,
            middle,
            second,
            expanded,
            active,
        ) = kept_values
        lower = micro_index * group_size
        tangent_rows = cotangent[lower : lower + group_size].reshape(row_count, model_width)
        active_grad = times_transposed(tangent_rows, shrink_full)
        gelu_pull = jax.vjp(lambda value_in: jax.nn.gelu(value_in, approximate=True), expanded)[1]
        expand_delta = gelu_pull(active_grad)[0].astype(jnp.bfloat16)
        second_grad = times_transposed(expand_delta, expand_full)
        mid_pull = jax.vjp(
            layer_norm, middle, gain_two.astype(jnp.float32), shift_two.astype(jnp.float32)
        )[1]
        middle_grad, gain_two_grad, shift_two_grad = mid_pull(second_grad)
        middle_grad = middle_grad + tangent_rows.astype(jnp.float32)
        branch_delta = middle_grad.astype(jnp.bfloat16)
        attended_delta = times_transposed(branch_delta, mixer_full).astype(jnp.bfloat16)
        grad_heads = attended_delta.reshape(group_size, stretch_len, head_count, HEAD)
        delta_heads = jnp.sum(
            grad_heads.transpose(0, 2, 1, 3).astype(jnp.float32) * attended, axis=-1
        )
        delta_rows = delta_heads.transpose(0, 2, 1)
        log_rows = log_total.transpose(0, 2, 1)
        lse_whole, delta_whole = (
            lax.all_gather(log_rows, "ctx", axis=1, tiled=True),
            lax.all_gather(delta_rows, "ctx", axis=1, tiled=True),
        )
        query_heads = queries.reshape(group_size, stretch_len, head_count, HEAD)
        key_heads = keys_local.reshape(group_size, stretch_len, head_count, HEAD)
        value_heads = values_local.reshape(group_size, stretch_len, head_count, HEAD)
        head_zeros = jnp.zeros((group_size, head_count, stretch_len, HEAD), jnp.float32)
        query_key_piece = lax.all_gather(keys_local, "ctx", axis=1, tiled=True)
        value_piece = lax.all_gather(values_local, "ctx", axis=1, tiled=True)
        count = query_key_piece.shape[1]
        step_len = piece_size(count)

        def query_block_step(turn_index, running):
            offset = turn_index * step_len
            key_block = lax.dynamic_slice_in_dim(query_key_piece, offset, step_len, 1).reshape(
                group_size, step_len, head_count, HEAD
            )
            value_block = lax.dynamic_slice_in_dim(value_piece, offset, step_len, 1).reshape(
                group_size, step_len, head_count, HEAD
            )
            key_pos = true_positions(stretch_order, offset, step_len, stretch_len)
            key_seg = lax.dynamic_slice_in_dim(seg_whole, offset, step_len, 1)
            allowed = (
                (seg_local[:, :, None] == key_seg[:, None, :])
                & (key_pos[None, None, :] <= own_pos[None, :, None])
            )[:, None]
            scores = (
                jnp.einsum(
                    "gqhd,gkhd->ghqk", query_heads, key_block, preferred_element_type=jnp.float32
                )
                * score_scale
            )
            probs = jnp.where(allowed, jnp.exp(scores - log_total[..., None]), 0.0)
            dots = jnp.einsum(
                "gqhd,gkhd->ghqk", grad_heads, value_block, preferred_element_type=jnp.float32
            )
            score_delta = (probs * (dots - delta_heads[..., None])).astype(jnp.bfloat16)
            return running + jnp.einsum(
                "ghqk,gkhd->ghqd", score_delta, key_block, preferred_element_type=jnp.float32
            )

        query_acc = lax.fori_loop(0, count // step_len, query_block_step, head_zeros)
        grad_rows3 = attended_delta.reshape(group_size, stretch_len, model_width)
        query_piece_rows = lax.all_gather(queries, "ctx", axis=1, tiled=True)
        grad_piece = lax.all_gather(grad_rows3, "ctx", axis=1, tiled=True)
        count = query_piece_rows.shape[1]
        key_step_len = piece_size(count)

        def key_block_step(turn_index, running):
            key_acc, value_acc = running
            offset = turn_index * key_step_len
            query_block = lax.dynamic_slice_in_dim(
                query_piece_rows, offset, key_step_len, 1
            ).reshape(group_size, key_step_len, head_count, HEAD)
            grad_block = lax.dynamic_slice_in_dim(grad_piece, offset, key_step_len, 1).reshape(
                group_size, key_step_len, head_count, HEAD
            )
            query_pos = true_positions(stretch_order, offset, key_step_len, stretch_len)
            query_seg = lax.dynamic_slice_in_dim(seg_whole, offset, key_step_len, 1)
            lse_block = lax.dynamic_slice_in_dim(lse_whole, offset, key_step_len, 1).transpose(
                0, 2, 1
            )
            delta_block = lax.dynamic_slice_in_dim(delta_whole, offset, key_step_len, 1).transpose(
                0, 2, 1
            )
            allowed = (
                (query_seg[:, :, None] == seg_local[:, None, :])
                & (own_pos[None, None, :] <= query_pos[None, :, None])
            )[:, None]
            scores = (
                jnp.einsum(
                    "gqhd,gkhd->ghqk", query_block, key_heads, preferred_element_type=jnp.float32
                )
                * score_scale
            )
            probs = jnp.where(allowed, jnp.exp(scores - lse_block[..., None]), 0.0)
            value_acc = value_acc + jnp.einsum(
                "ghqk,gqhd->ghkd",
                probs.astype(jnp.bfloat16),
                grad_block,
                preferred_element_type=jnp.float32,
            )
            dots = jnp.einsum(
                "gqhd,gkhd->ghqk", grad_block, value_heads, preferred_element_type=jnp.float32
            )
            score_delta = (probs * (dots - delta_block[..., None])).astype(jnp.bfloat16)
            key_acc = key_acc + jnp.einsum(
                "ghqk,gqhd->ghkd", score_delta, query_block, preferred_element_type=jnp.float32
            )
            return (key_acc, value_acc)

        key_acc, value_acc = lax.fori_loop(
            0, count // key_step_len, key_block_step, (head_zeros, head_zeros)
        )
        query_delta = (
            (query_acc * score_scale)
            .transpose(0, 2, 1, 3)
            .reshape(row_count, model_width)
            .astype(jnp.bfloat16)
        )
        key_delta = (
            (key_acc * score_scale)
            .transpose(0, 2, 1, 3)
            .reshape(row_count, model_width)
            .astype(jnp.bfloat16)
        )
        value_delta = (
            value_acc.transpose(0, 2, 1, 3).reshape(row_count, model_width).astype(jnp.bfloat16)
        )
        joint_delta = jnp.concatenate([query_delta, key_delta, value_delta], axis=1)
        normed_grad = times_transposed(joint_delta, joint_full)
        first_pull = jax.vjp(
            layer_norm,
            tokens.reshape(row_count, model_width),
            gain_one.astype(jnp.float32),
            shift_one.astype(jnp.float32),
        )[1]
        token_grad, gain_one_grad, shift_one_grad = first_pull(normed_grad)
        input_grad = (middle_grad + token_grad).reshape(group_size, stretch_len, model_width)
        small_terms = (
            gain_one_grad,
            shift_one_grad,
            jnp.sum(query_delta.astype(jnp.float32), axis=0),
            jnp.sum(value_delta.astype(jnp.float32), axis=0),
            jnp.sum(branch_delta.astype(jnp.float32), axis=0),
            gain_two_grad,
            shift_two_grad,
            jnp.sum(expand_delta.astype(jnp.float32), axis=0),
            jnp.sum(tangent_rows.astype(jnp.float32), axis=0),
        )
        factor_pairs = (
            normed.reshape(row_count, model_width),
            joint_delta,
            mixed_rows,
            branch_delta,
            second,
            expand_delta,
            active,
            tangent_rows,
        )
        return (input_grad, small_terms, factor_pairs)

    output_list = []
    input_list = []
    factor_list = []
    small_totals = None
    for micro_index in range(MICRO):
        forward_weights = fetch_weights(local_parts)
        (
            forward_joint_full,
            forward_mixer_full,
            forward_expand_full,
            forward_shrink_full,
            forward_gain_one,
            forward_shift_one,
            forward_qbias_full,
            forward_vbias_full,
            forward_mbias_full,
            forward_gain_two,
            forward_shift_two,
            forward_ebias_full,
            forward_sbias_full,
        ) = forward_weights
        forward_lower = micro_index * group_size
        forward_tokens = inputs[forward_lower : forward_lower + group_size].astype(jnp.float32)
        forward_seg_local = segments[forward_lower : forward_lower + group_size]
        forward_seg_whole = all_segments[forward_lower : forward_lower + group_size]
        forward_normed = layer_norm(
            forward_tokens,
            forward_gain_one.astype(jnp.float32),
            forward_shift_one.astype(jnp.float32),
        ).astype(jnp.bfloat16)
        joint_bias = jnp.concatenate(
            [forward_qbias_full, jnp.zeros_like(forward_qbias_full), forward_vbias_full]
        ).astype(jnp.float32)
        joint_rows = (
            jnp.dot(
                forward_normed.reshape(row_count, model_width),
                forward_joint_full,
                preferred_element_type=jnp.float32,
            )
            + joint_bias
        )
        joint_rows = joint_rows.astype(jnp.bfloat16).reshape(
            group_size, stretch_len, 3 * model_width
        )
        forward_queries = joint_rows[..., :model_width]
        forward_keys_local = joint_rows[..., model_width : 2 * model_width]
        forward_values_local = joint_rows[..., 2 * model_width :]
        forward_query_heads = forward_queries.reshape(group_size, stretch_len, head_count, HEAD)
        start_state = (
            jnp.full((group_size, head_count, stretch_len), masked_score, jnp.float32),
            jnp.zeros((group_size, head_count, stretch_len), jnp.float32),
            jnp.zeros((group_size, head_count, stretch_len, HEAD), jnp.float32),
        )
        forward_key_piece = lax.all_gather(forward_keys_local, "ctx", axis=1, tiled=True)
        forward_value_piece = lax.all_gather(forward_values_local, "ctx", axis=1, tiled=True)
        forward_count = forward_key_piece.shape[1]
        forward_step_len = piece_size(forward_count)

        def forward_block_step(turn_index, state):
            top_score, row_total, accumulated = state
            offset = turn_index * forward_step_len
            key_block = lax.dynamic_slice_in_dim(
                forward_key_piece, offset, forward_step_len, 1
            ).reshape(group_size, forward_step_len, head_count, HEAD)
            value_block = lax.dynamic_slice_in_dim(
                forward_value_piece, offset, forward_step_len, 1
            ).reshape(group_size, forward_step_len, head_count, HEAD)
            key_pos = true_positions(stretch_order, offset, forward_step_len, stretch_len)
            key_seg = lax.dynamic_slice_in_dim(forward_seg_whole, offset, forward_step_len, 1)
            allowed = (
                (forward_seg_local[:, :, None] == key_seg[:, None, :])
                & (key_pos[None, None, :] <= own_pos[None, :, None])
            )[:, None]
            scores = (
                jnp.einsum(
                    "gqhd,gkhd->ghqk",
                    forward_query_heads,
                    key_block,
                    preferred_element_type=jnp.float32,
                )
                * score_scale
            )
            scores = jnp.where(allowed, scores, masked_score)
            new_top = jnp.maximum(top_score, jnp.max(scores, axis=-1))
            weights_now = jnp.where(allowed, jnp.exp(scores - new_top[..., None]), 0.0)
            fade_factor = jnp.exp(top_score - new_top)
            row_total = row_total * fade_factor + jnp.sum(weights_now, axis=-1)
            accumulated = accumulated * fade_factor[..., None] + jnp.einsum(
                "ghqk,gkhd->ghqd",
                weights_now.astype(jnp.bfloat16),
                value_block,
                preferred_element_type=jnp.float32,
            )
            return (new_top, row_total, accumulated)

        top_score, row_total, accumulated = lax.fori_loop(
            0, forward_count // forward_step_len, forward_block_step, start_state
        )
        forward_attended = accumulated / row_total[..., None]
        forward_log_total = top_score + jnp.log(row_total)
        forward_mixed_rows = (
            forward_attended.transpose(0, 2, 1, 3)
            .reshape(row_count, model_width)
            .astype(jnp.bfloat16)
        )
        branch = jnp.dot(
            forward_mixed_rows, forward_mixer_full, preferred_element_type=jnp.float32
        ) + forward_mbias_full.astype(jnp.float32)
        forward_middle = forward_tokens.reshape(row_count, model_width) + branch
        forward_second = layer_norm(
            forward_middle,
            forward_gain_two.astype(jnp.float32),
            forward_shift_two.astype(jnp.float32),
        ).astype(jnp.bfloat16)
        forward_expanded = jnp.dot(
            forward_second, forward_expand_full, preferred_element_type=jnp.float32
        ) + forward_ebias_full.astype(jnp.float32)
        forward_active = jax.nn.gelu(forward_expanded, approximate=True).astype(jnp.bfloat16)
        output = (
            forward_middle
            + jnp.dot(forward_active, forward_shrink_full, preferred_element_type=jnp.float32)
            + forward_sbias_full.astype(jnp.float32)
        )
        forward_kept_values = (
            forward_tokens,
            forward_seg_local,
            forward_seg_whole,
            forward_normed,
            forward_queries,
            forward_keys_local,
            forward_values_local,
            forward_mixed_rows,
            forward_attended,
            forward_log_total,
            forward_middle,
            forward_second,
            forward_expanded,
            forward_active,
        )
        output_now = output.reshape(group_size, stretch_len, model_width).astype(jnp.bfloat16)
        kept_values = forward_kept_values
        backward_weights = fetch_weights(local_parts)
        input_now, small_terms, factor_pairs = backward_micro(
            backward_weights, kept_values, micro_index
        )
        output_list.append(output_now)
        input_list.append(input_now)
        factor_list.append(factor_pairs)
        if small_totals is None:
            small_totals = small_terms
        else:
            small_totals = tuple(
                (total_now + term_now for total_now, term_now in zip(small_totals, small_terms))
            )

    def joined(position):
        return jnp.concatenate([pairs_now[position] for pairs_now in factor_list], axis=0)

    matrices = (
        outer_sum(joined(0), joined(1)),
        outer_sum(joined(2), joined(3)),
        outer_sum(joined(4), joined(5)),
        outer_sum(joined(6), joined(7)),
    )
    reduced = reduce_gradients(matrices, small_totals)
    block_output = jnp.concatenate(output_list, axis=0)
    input_gradient = jnp.concatenate(input_list, axis=0)
    return (
        block_output,
        input_gradient,
        reduced[4],
        reduced[5],
        reduced[0],
        reduced[6],
        reduced[7],
        reduced[1],
        reduced[8],
        reduced[9],
        reduced[10],
        reduced[2],
        reduced[11],
        reduced[3],
        reduced[12],
    )


def joint_split(rows, parts, heads_each):
    count, three, width = rows.shape
    span = heads_each * HEAD
    slots = slot_width(heads_each)
    rows = jnp.pad(rows, ((0, 0), (0, 0), (0, parts * span - width)))
    rows = rows.reshape(count, three, parts, span)
    rows = jnp.pad(rows, ((0, 0), (0, 0), (0, 0), (0, slots - span)))
    return rows.transpose(2, 0, 1, 3).reshape(parts, count, three * slots)


def joint_join(pieces, heads_each, width):
    parts, count, wide = pieces.shape
    span = heads_each * HEAD
    rows = pieces.reshape(parts, count, 3, wide // 3)[..., :span]
    rows = rows.transpose(1, 2, 0, 3).reshape(count, 3, parts * span)
    return rows[..., :width].reshape(count, 3 * width)


def slot_width(heads_each):
    return -(-heads_each * HEAD // LANES) * LANES


def causal(k_block_is_diagonal, same):
    if k_block_is_diagonal:
        same = same & (
            lax.broadcasted_iota(jnp.int32, (TILE, TILE), 0)
            <= lax.broadcasted_iota(jnp.int32, (TILE, TILE), 1)
        )
    return same


def attend_forward_kernel(nf, nc, guests, *refs):
    n_in = sum(g[2] for g in guests)
    n_out = sum(g[3] for g in guests)
    own, ins, results, outs, own_scratch, scratch = split_refs(
        refs, (3, n_in, 3, n_out, 7, len(refs) - n_in - n_out - 13)
    )
    seg_row, seg_col, qkv_ref = own
    out_ref, turned_ref, lse_ref = results
    q_low, q_high, keys, values_turned, acc, tops, sums = own_scratch
    made = hosted(nf, nc, guests, ins, outs, scratch)
    greet_all(nc, {needs_of(g) for g in guests})
    begin_guests(made)
    send_guests(made)
    slots = out_ref.shape[1]
    scale = HEAD ** (-0.5)
    halves = (q_low, q_high)

    def one_block(q_block, k_block, first):
        q_at = pl.ds(pl.multiple_of(q_block * TILE, TILE), TILE)
        k_at = pl.ds(pl.multiple_of(k_block * TILE, TILE), TILE)
        same = causal(first, seg_col[k_at, :] == seg_row[:, q_at])
        for half in range(2):
            dims = pl.ds(half * HEAD, HEAD)
            scores = times_transposed(keys[k_at, :], halves[half][q_at, :])
            scores = jnp.where(same, scores, masked_score)
            top = jnp.max(scores, axis=0, keepdims=True)
            if not first:
                old_top = tops[half]
                top = jnp.maximum(old_top, top)
            weights = jnp.exp(scores - top)
            total = jnp.sum(weights, axis=0, keepdims=True)
            part = jnp.dot(
                values_turned[dims, k_at],
                weights.astype(jnp.bfloat16),
                preferred_element_type=jnp.float32,
            )
            if not first:
                fade = jnp.exp(old_top - top)
                total = total + sums[half] * fade
                part = part + acc[dims, :] * fade
            tops[half] = top
            sums[half] = total
            acc[dims, :] = part

    @pl.loop(0, slots // LANES)
    def _(pair):
        column = pl.multiple_of(pair * LANES, LANES)
        queries = qkv_ref[:, pl.ds(column, LANES)] * jnp.bfloat16(scale)
        low_half = lax.broadcasted_iota(jnp.int32, queries.shape, 1) < HEAD
        q_low[...] = jnp.where(low_half, queries, jnp.zeros_like(queries))
        q_high[...] = jnp.where(low_half, jnp.zeros_like(queries), queries)
        keys[...] = qkv_ref[:, pl.ds(slots + column, LANES)]
        values = qkv_ref[:, pl.ds(2 * slots + column, LANES)]
        values_turned[...] = values.astype(jnp.float32).T.astype(jnp.bfloat16)

        @pl.loop(0, qkv_ref.shape[0] // TILE)
        def _(q_block):
            one_block(q_block, q_block, True)

            @pl.loop(0, q_block)
            def _(k_block):
                one_block(q_block, k_block, False)

            q_at = pl.ds(pl.multiple_of(q_block * TILE, TILE), TILE)
            for half in range(2):
                dims = pl.ds(half * HEAD, HEAD)
                acc[dims, :] = acc[dims, :] / sums[half]
                lse_ref[pair, pl.ds(half, 1), q_at] = tops[half] + jnp.log(sums[half])
            turned_ref[pair, :, q_at] = acc[...]
            out_ref[q_at, pl.ds(column, LANES)] = acc[...].T.astype(jnp.bfloat16)

        @pl.when(pair == 2)
        def _():
            pass_on_guests(made)

    run_guests(made)


def attend_backward_kernel(nf, nc, guests, *refs):
    n_in = sum(g[2] for g in guests)
    n_out = sum(g[3] for g in guests)
    own, ins, results, outs, own_scratch, scratch = split_refs(
        refs, (6, n_in, 1, n_out, 11, len(refs) - n_in - n_out - 18)
    )
    seg_row, seg_col, qkv_ref, grad_ref, turned_ref, lse_ref = own
    out_ref = results[0]
    (
        q_low, q_high, keys, keys_turned, values, g_low, g_high,
        query_acc, key_acc, value_acc, corrections,
    ) = own_scratch
    made = hosted(nf, nc, guests, ins, outs, scratch)
    greet_all(nc, {needs_of(g) for g in guests})
    begin_guests(made)
    slots = grad_ref.shape[1]
    scale = HEAD ** (-0.5)
    q_halves = (q_low, q_high)
    g_halves = (g_low, g_high)

    def one_block(pair, q_block, k_block, first):
        q_at = pl.ds(pl.multiple_of(q_block * TILE, TILE), TILE)
        k_at = pl.ds(pl.multiple_of(k_block * TILE, TILE), TILE)
        same = causal(first, seg_col[k_at, :] == seg_row[:, q_at])
        value_sum = value_acc[k_at, :]
        key_sum = key_acc[k_at, :]
        for half in range(2):
            dims = pl.ds(half * HEAD, HEAD)
            query_rows = q_halves[half][q_at, :]
            grad_rows = g_halves[half][q_at, :]
            scores = times_transposed(keys[k_at, :], query_rows)
            lse = lse_ref[pair, pl.ds(half, 1), q_at]
            probs = jnp.exp(jnp.where(same, scores - lse, masked_score))
            dots = times_transposed(values[k_at, :], grad_rows)
            delta = (probs * (dots - corrections[half, :, q_at])).astype(jnp.bfloat16)
            value_sum = value_sum + jnp.dot(
                probs.astype(jnp.bfloat16), grad_rows, preferred_element_type=jnp.float32
            )
            key_sum = key_sum + jnp.dot(delta, query_rows, preferred_element_type=jnp.float32)
            part = jnp.dot(keys_turned[dims, k_at], delta, preferred_element_type=jnp.float32)
            if first:
                query_acc[dims, :] = part
            else:
                query_acc[dims, :] += part
        value_acc[k_at, :] = value_sum
        key_acc[k_at, :] = key_sum

    @pl.loop(0, slots // LANES)
    def _(pair):
        column = pl.multiple_of(pair * LANES, LANES)
        queries = qkv_ref[:, pl.ds(column, LANES)] * jnp.bfloat16(scale)
        low_half = lax.broadcasted_iota(jnp.int32, queries.shape, 1) < HEAD
        zeros = jnp.zeros_like(queries)
        q_low[...] = jnp.where(low_half, queries, zeros)
        q_high[...] = jnp.where(low_half, zeros, queries)
        grads = grad_ref[:, pl.ds(column, LANES)]
        g_low[...] = jnp.where(low_half, grads, zeros)
        g_high[...] = jnp.where(low_half, zeros, grads)
        product = grads.astype(jnp.float32).T * turned_ref[pair]
        corrections[0] = jnp.sum(product[:HEAD], axis=0, keepdims=True)
        corrections[1] = jnp.sum(product[HEAD:], axis=0, keepdims=True)
        keys_now = qkv_ref[:, pl.ds(slots + column, LANES)]
        keys[...] = keys_now
        keys_turned[...] = keys_now.astype(jnp.float32).T.astype(jnp.bfloat16)
        values[...] = qkv_ref[:, pl.ds(2 * slots + column, LANES)]
        key_acc[...] = jnp.zeros_like(key_acc)
        value_acc[...] = jnp.zeros_like(value_acc)

        @pl.loop(0, qkv_ref.shape[0] // TILE)
        def _(q_block):
            one_block(pair, q_block, q_block, True)

            @pl.loop(0, q_block)
            def _(k_block):
                one_block(pair, q_block, k_block, False)

            q_at = pl.ds(pl.multiple_of(q_block * TILE, TILE), TILE)
            out_ref[q_at, pl.ds(column, LANES)] = (query_acc[...].T * scale).astype(jnp.bfloat16)

        out_ref[:, pl.ds(slots + column, LANES)] = key_acc[...].astype(jnp.bfloat16)
        out_ref[:, pl.ds(2 * slots + column, LANES)] = value_acc[...].astype(jnp.bfloat16)

        @pl.when(pair == 0)
        def _():
            send_guests(made)

    run_guests(made)


def pick(blocks, order):
    return blocks.at[order].get(mode="promise_in_bounds", unique_indices=True)


def all_units(vector, nc, nf, unit_each, shard):
    vector = vector.transpose(1, 0, 2).reshape(nc, nf, unit_each)
    return lax.dynamic_index_in_dim(vector, shard, 1, keepdims=False).reshape(nc * unit_each)


def rows_of(vectors, count):
    row = jnp.arange(count, dtype=jnp.int32)[:, None]
    total = jnp.where(row == 0, vectors[0][None], jnp.zeros_like(vectors[0][None]))
    for k, vector in enumerate(vectors[1:], 1):
        total = jnp.where(row == k, vector[None], total)
    return total


def normalize(rows):
    center = rows - jnp.mean(rows, axis=-1, keepdims=True)
    spread = jnp.mean(center * center, axis=-1, keepdims=True)
    inverse = lax.rsqrt(spread + epsilon)
    return center * inverse, inverse


def normalize_back(grads, gain, unit, inverse):
    pulled = grads * gain
    return inverse * (
        pulled
        - jnp.mean(pulled, axis=-1, keepdims=True)
        - unit * jnp.mean(pulled * unit, axis=-1, keepdims=True)
    )


def gelu_parts(value):
    root = 0.7978845608028654
    inner = root * (value + 0.044715 * value * value * value)
    bend = jnp.tanh(inner)
    slope = 0.5 * (1.0 + bend) + 0.5 * value * (1.0 - bend * bend) * root * (
        1.0 + 3 * 0.044715 * value * value
    )
    return 0.5 * value * (1.0 + bend), slope


def mesh_copy(source, target, send, receive, device):
    return pltpu.make_async_remote_copy(
        src_ref=source,
        dst_ref=target,
        send_sem=send,
        recv_sem=receive,
        device_id=device,
        device_id_type=pl.DeviceIdType.MESH,
    )


def greet(devices, swaps=()):
    barrier = pltpu.get_barrier_semaphore()
    for device in devices:
        pl.semaphore_signal(
            barrier, inc=1, device_id=device, device_id_type=pl.DeviceIdType.MESH
        )
    for device in swaps:

        @pl.when(elsewhere(device))
        def _():
            pl.semaphore_signal(
                barrier, inc=1, device_id=device, device_id_type=pl.DeviceIdType.MESH
            )

    count = len(devices)
    for device in swaps:
        count = count + jnp.where(elsewhere(device), 1, 0)
    pl.semaphore_wait(barrier, count)


def elsewhere(device):
    apart = (device[0] - lax.axis_index("fsdp")) * 64 + device[1] - lax.axis_index("ctx")
    return apart != 0


def to_column(f, c, i):
    return 2 * (c // 2 % 2) + c % 2, 2 * (2 * i + f % 2) + (f // 2 + f % 2) % 2, c // 4


def to_origin(f, c, j):
    core = c // 2 % 2
    return 2 * ((c % 2 + core) % 2) + core, 2 * (2 * j + f // 2) + f % 2, c // 4


def swap_peers(move, back):
    f, c = lax.axis_index("fsdp"), lax.axis_index("ctx")
    return [way(f, c, k)[:2] for way in (move, back) for k in range(2)]


def ctx_peers(nc):
    f, c = lax.axis_index("fsdp"), lax.axis_index("ctx")
    return [(f, (c + k) % nc) for k in range(1, nc)]


def greet_all(nc, needs):
    devices, swaps = [], []
    if "fsdp" in needs:
        devices += fsdp_peers(3)
    elif "near" in needs:
        devices += fsdp_peers(2)
    if "ctx" in needs:
        devices += ctx_peers(nc)
    elif "ring" in needs:
        devices += ring_peers(nc)
    if "column" in needs:
        swaps += swap_peers(to_column, to_origin)
    if "origin" in needs:
        swaps += swap_peers(to_origin, to_column)
    greet(devices, swaps)


def fsdp_places():
    shard = lax.axis_index("fsdp")
    partner = shard + 1 - 2 * (shard % 2)
    return shard, partner, (shard + 2) % 4, (partner + 2) % 4


def ring_places(nc):
    place = lax.axis_index("ctx")
    z, y = place // 2, place % 2
    spot = z * (1 - y) + (nc - 1 - z) * y

    def holder(at):
        at = (at + nc) % nc
        side = at // (nc // 2)
        return (1 - side) * 2 * at + side * (2 * (nc - 1 - at) + 1)

    return spot, holder


def ring_peers(nc):
    spot, holder = ring_places(nc)
    shard = lax.axis_index("fsdp")
    return [(shard, holder(spot + way)) for way in (1, -1)]


def fsdp_peers(count):
    place = lax.axis_index("ctx")
    return [(at, place) for at in fsdp_places()[1 : 1 + count]]


def chunks_of(rows, count):
    step = -(-rows // count // 16) * 16
    return [(at, min(step, rows - at)) for at in range(0, rows, step)]


def row_step(size):
    return next(step for step in (56, 40, 32, 16, 8) if size % step == 0)


class FsdpGather:
    SEMS = (7, 4)

    def __init__(self, own, out, sems):
        self.own, self.out, self.sems = own, out, sems
        self.shard, self.partner, self.cross, self.corner = fsdp_places()
        self.place = lax.axis_index("ctx")
        self.chunks = chunks_of(own.shape[0], 4)

    def copy(self, kind, k):
        at, size = self.chunks[k]
        rows = pl.ds(at, size)
        if kind == "own":
            return pltpu.make_async_copy(
                self.own.at[rows], self.out.at[self.shard, rows], self.sems.at[6, k]
            )
        if kind == "across":
            source, slot, device, sem = self.own.at[rows], self.shard, self.cross, 0
        elif kind == "beside":
            source, slot, device, sem = self.own.at[rows], self.shard, self.partner, 2
        else:
            slot, device, sem = self.cross, self.partner, 4
            source = self.out.at[slot, rows]
        return mesh_copy(
            source,
            self.out.at[slot, rows],
            self.sems.at[sem, k],
            self.sems.at[sem + 1, k],
            (device, self.place),
        )

    def begin(self):
        for kind in ("across", "beside", "own"):
            for k in range(len(self.chunks)):
                self.copy(kind, k).start()

    def pass_on(self):
        for k in range(len(self.chunks)):
            self.copy("across", k).wait_recv()
            self.copy("on", k).start()

    def finish(self):
        for k in range(len(self.chunks)):
            self.copy("across", k).wait_send()
            self.copy("beside", k).wait()
            self.copy("on", k).wait()
            self.copy("own", k).wait()


def joint_parts(nf, nc, rows, depth, place):
    thin = depth // nf // (8 * nc) * 8
    rest, each = rows - nf * thin, nc // nf
    parts = []
    for f in range(nf):
        parts.append((f * thin, pl.multiple_of(f * (depth // nf) + place * thin, 8), thin))
    last = (place // each) * (depth // nf) + nc * thin + (place % each) * rest
    parts.append((nf * thin, pl.multiple_of(last, 8), rest))
    return parts


def half_of(parts, way):
    middle = (len(parts) - 1) // 2
    return parts[:middle] if way == 1 else parts[middle:]


class RingGather:
    def __init__(self, nc, own, out, sems, parts=None):
        self.nc, self.own, self.out, self.sems = nc, own, out, sems
        self.spot, self.holder = ring_places(nc)
        self.shard = lax.axis_index("fsdp")
        self.parts = parts
        if parts is None:
            self.rows = out.shape[1]
            self.half = self.rows // 2 // 8 * 8

    def pieces(self, origin, way, step):
        if self.parts is not None:
            parts = self.parts(origin)
            if step == self.nc // 2:
                parts = half_of(parts, way)
            return [(pl.ds(at, size), self.out.at[pl.ds(there, size)]) for at, there, size in parts]
        rows = pl.ds(0, self.rows)
        if step == self.nc // 2:
            rows = pl.ds(0, self.half) if way == 1 else pl.ds(self.half, self.rows - self.half)
        return [(rows, self.out.at[origin, rows])]

    def copies(self, way, step):
        origin = self.holder(self.spot - way * (step - 1))
        side = 0 if way == 1 else 2
        made = []
        for k, (rows, whole) in enumerate(self.pieces(origin, way, step)):
            made.append(
                mesh_copy(
                    self.own.at[rows] if step == 1 else whole,
                    whole,
                    self.sems.at[side, step - 1, k],
                    self.sems.at[side + 1, step - 1, k],
                    (self.shard, self.holder(self.spot + way)),
                )
            )
        return made

    def keeps(self):
        return [
            pltpu.make_async_copy(self.own.at[rows], whole, self.sems.at[4, 0, k])
            for k, (rows, whole) in enumerate(self.pieces(lax.axis_index("ctx"), 1, 1))
        ]

    def start(self, step):
        for way in (1, -1):
            for copy in self.copies(way, step):
                copy.start()
        if step == 1:
            for copy in self.keeps():
                copy.start()

    def arrived(self, way, step):
        for copy in self.copies(way, step):
            copy.wait_recv()

    def advance(self, step):
        for way in (1, -1):
            self.arrived(way, step - 1)
            for copy in self.copies(way, step):
                copy.start()

    def finish(self, first, last):
        for way in (1, -1):
            for step in range(first, last + 1):
                for copy in self.copies(way, step):
                    copy.wait_send()
            self.arrived(way, last)
        if first == 1:
            for copy in self.keeps():
                copy.wait()


class RingScatter:
    def __init__(self, nc, mine, out, right, left, sems, parts=None):
        self.nc, self.mine, self.out, self.sems = nc, mine, out, sems
        self.inbox = {1: right, -1: left}
        self.spot, self.holder = ring_places(nc)
        self.shard = lax.axis_index("fsdp")
        self.rows = out.shape[0]
        self.half = self.rows // 2 // 8 * 8
        self.parts = parts

    def copies(self, way, step):
        inbox = self.inbox[way]
        if step > 1:
            sources = [(pl.ds(0, self.rows), inbox.at[step - 2])]
        else:
            place = self.holder(self.spot + self.nc // 2)
            if self.parts is not None:
                sources = [
                    (pl.ds(at, size), self.mine.at[pl.ds(there, size)])
                    for at, there, size in half_of(self.parts(place), way)
                ]
            else:
                low, high = pl.ds(0, self.half), pl.ds(self.half, self.rows - self.half)
                rows = low if way == 1 else high
                sources = [(rows, self.mine.at[place, rows])]
        side = 0 if way == 1 else 2
        return [
            mesh_copy(
                source,
                inbox.at[step - 1, rows],
                self.sems.at[side, step - 1, k],
                self.sems.at[side + 1, step - 1, k],
                (self.shard, self.holder(self.spot + way)),
            )
            for k, (rows, source) in enumerate(sources)
        ]

    def begin(self):
        for way in (1, -1):
            for copy in self.copies(way, 1):
                copy.start()

    def advance(self, step):
        for way in (1, -1):
            for copy in self.copies(way, step - 1):
                copy.wait_recv()
            box = self.inbox[way].at[step - 2]
            place = self.holder(self.spot + way * (self.nc // 2 + 1 - step))
            if self.parts is not None:
                parts = self.parts(place)
                came = half_of(parts, way) if step == 2 else parts
                for part in parts:
                    at, there, size = part
                    target, source = box.at[pl.ds(at, size)], self.mine.at[pl.ds(there, size)]
                    if any(part is other for other in came):
                        add_rows(target, source, (0, size))
                    else:
                        set_rows(target, source, (0, size))
            else:
                join_rows(box, self.mine.at[place], step, way, self.rows, self.half)
            for copy in self.copies(way, step):
                copy.start()

    def finish(self):
        last = self.nc // 2
        for way in (1, -1):
            for copy in self.copies(way, last):
                copy.wait_recv()
        right, left = self.inbox[1].at[last - 1], self.inbox[-1].at[last - 1]
        place = lax.axis_index("ctx")
        if self.parts is not None:
            for at, there, size in self.parts(place):
                rows = pl.ds(at, size)
                sum_rows(
                    self.out.at[rows], self.mine.at[pl.ds(there, size)], right.at[rows], left.at[rows]
                )
        else:
            sum_rows(self.out, self.mine.at[place], right, left)
        for way in (1, -1):
            for step in range(1, last + 1):
                for copy in self.copies(way, step):
                    copy.wait_send()


def join_rows(box, mine, step, way, rows, half):
    low, high = (0, half), (half, rows - half)
    if step == 2:
        got, rest = (low, high) if way == 1 else (high, low)
        set_rows(box, mine, rest)
    else:
        got = (0, rows)
    add_rows(box, mine, got)


def add_rows(target, source, rows):
    first, size = rows
    step = row_step(size)

    @pl.loop(0, size // step)
    def _(turn):
        at = pl.ds(pl.multiple_of(first + turn * step, 8), step)
        target[at] = (target[at].astype(jnp.float32) + source[at].astype(jnp.float32)).astype(
            target.dtype
        )


def set_rows(target, source, rows):
    first, size = rows
    step = row_step(size)

    @pl.loop(0, size // step)
    def _(turn):
        at = pl.ds(pl.multiple_of(first + turn * step, 8), step)
        target[at] = source[at]


def sum_rows(out, mine, right, left):
    step = row_step(out.shape[0])

    @pl.loop(0, out.shape[0] // step)
    def _(turn):
        at = pl.ds(pl.multiple_of(turn * step, 8), step)
        out[at] = (
            mine[at].astype(jnp.float32)
            + right[at].astype(jnp.float32)
            + left[at].astype(jnp.float32)
        ).astype(out.dtype)


class GatherStep:
    NEEDS = "ring"
    VMEM_IN = 0

    def __init__(self, nf, nc, step, ins, outs, scratch):
        self.step = step
        self.ring = RingGather(nc, None, outs[0], scratch[0])

    @staticmethod
    def shapes(nf, nc, step, arrays):
        (whole,) = arrays
        return (
            [jax.ShapeDtypeStruct(whole.shape, whole.dtype)],
            [pltpu.SemaphoreType.DMA((5, nc // 2, 1))],
            True,
        )

    def begin(self):
        self.ring.start(self.step)

    def send(self):
        pass

    def finish(self):
        self.ring.finish(self.step, self.step)


class SideGather:
    NEEDS = "near"
    VMEM_IN = 1

    def __init__(self, nf, nc, step, ins, outs, scratch):
        self.side = FsdpGather(ins[0], outs[0], scratch[0])

    @staticmethod
    def shapes(nf, nc, step, arrays):
        (array,) = arrays
        return (
            [jax.ShapeDtypeStruct((nf,) + array.shape, array.dtype)],
            [pltpu.SemaphoreType.DMA(FsdpGather.SEMS)],
            False,
        )

    def begin(self):
        pass

    def send(self):
        self.side.begin()

    def finish(self):
        self.side.finish()


class ScatterRing:
    NEEDS = "ring"
    VMEM_IN = 1

    def __init__(self, nf, nc, step, ins, outs, scratch):
        right, left, total, self.put_sem, sems = scratch
        self.out, self.total = outs[0], total
        parts = None
        if step:
            parts = functools.partial(joint_parts, nf, nc, step, ins[0].shape[0])
        self.ring = RingScatter(nc, ins[0], total, right, left, sems, parts)

    @staticmethod
    def shapes(nf, nc, step, arrays):
        mine = arrays[0]
        shape = (step,) + mine.shape[1:] if step else mine.shape[1:]
        box = pltpu.VMEM((nc // 2,) + shape, mine.dtype)
        return (
            [jax.ShapeDtypeStruct(shape, mine.dtype)],
            [
                box,
                box,
                pltpu.VMEM(shape, mine.dtype),
                pltpu.SemaphoreType.DMA((1,)),
                pltpu.SemaphoreType.DMA((4, nc // 2, nf + 1)),
            ],
            False,
        )

    def begin(self):
        self.ring.begin()

    def send(self):
        self.ring.advance(2)

    def more(self, step):
        self.ring.advance(step)

    def finish(self):
        self.ring.finish()
        put = pltpu.make_async_copy(self.total, self.out, self.put_sem.at[0])
        put.start()
        put.wait()


class ScatterStep:
    NEEDS = "ring"
    VMEM_IN = 0

    def __init__(self, nf, nc, step, ins, outs, scratch):
        self.nc, self.step = nc, step
        self.mine, self.before, self.outs = ins[0], ins[1:], outs
        self.sems = scratch[-1]
        self.boxes = scratch[:-1]
        self.spot, self.holder = ring_places(nc)
        self.shard = lax.axis_index("fsdp")
        self.rows = outs[0].shape[0]
        self.half = self.rows // 2 // 8 * 8

    @staticmethod
    def shapes(nf, nc, step, arrays):
        mine = arrays[0]
        block = jax.ShapeDtypeStruct(mine.shape[1:], mine.dtype)
        outs = [block, block]
        scratch = []
        if step > 1:
            scratch += [pltpu.VMEM(mine.shape[1:], mine.dtype)] * 4
        return outs, scratch + [pltpu.SemaphoreType.DMA((4, 4))], False

    def copy(self, k):
        way = (1, -1)[k]
        rows = pl.ds(0, self.rows)
        if self.step == 1:
            rows = pl.ds(0, self.half) if way == 1 else pl.ds(self.half, self.rows - self.half)
            source = self.mine.at[self.holder(self.spot + self.nc // 2), rows]
        else:
            source = self.boxes[k]
        return mesh_copy(
            source,
            self.outs[k].at[rows],
            self.sems.at[0, k],
            self.sems.at[1, k],
            (self.shard, self.holder(self.spot + way)),
        )

    def loads(self, k):
        way = (1, -1)[k]
        rows = pl.ds(0, self.rows)
        if self.step == 2:
            rows = pl.ds(0, self.half) if way == 1 else pl.ds(self.half, self.rows - self.half)
        place = self.holder(self.spot + way * (self.nc // 2 + 1 - self.step))
        return [
            pltpu.make_async_copy(
                self.before[k].at[rows], self.boxes[k].at[rows], self.sems.at[2, k]
            ),
            pltpu.make_async_copy(self.mine.at[place], self.boxes[2 + k], self.sems.at[3, k]),
        ]

    def begin(self):
        for k in range(2):
            if self.step == 1:
                self.copy(k).start()
            else:
                for load in self.loads(k):
                    load.start()

    def send(self):
        if self.step > 1:
            for k in range(2):
                for load in self.loads(k):
                    load.wait()
                way = (1, -1)[k]
                join_rows(self.boxes[k], self.boxes[2 + k], self.step, way, self.rows, self.half)
                self.copy(k).start()

    def finish(self):
        for k in range(2):
            self.copy(k).wait()


class Trade:
    def __init__(self, axis, size, source, target, sems, hops=None):
        self.axis, self.size = axis, size
        self.hops = hops or tuple(range(1, size))
        self.source, self.target, self.sems = source, target, sems
        self.me = lax.axis_index(axis)

    def copies(self):
        made = []
        for k in self.hops:
            other = (self.me + k) % self.size
            device = (
                (other, lax.axis_index("ctx"))
                if self.axis == "fsdp"
                else (lax.axis_index("fsdp"), other)
            )
            made.append(
                mesh_copy(
                    self.source(other),
                    self.target(self.me),
                    self.sems.at[0, k],
                    self.sems.at[1, k],
                    device,
                )
            )
        made.append(
            pltpu.make_async_copy(
                self.source(self.me), self.target(self.me), self.sems.at[2, 0]
            )
        )
        return made

    def begin(self):
        for copy in self.copies():
            copy.start()

    def finish(self):
        for copy in self.copies():
            copy.wait()


class TradeGuest:
    VMEM_IN = 1

    def __init__(self, nf, nc, step, ins, outs, scratch):
        axis, hops = step
        size = nf if axis == "fsdp" else nc
        whole = len(ins[0].shape) < len(outs[0].shape)
        self.trade = Trade(
            axis,
            size,
            (lambda k: ins[0]) if whole else (lambda k: ins[0].at[k]),
            lambda k: outs[0].at[k],
            scratch[0],
            hops,
        )

    @staticmethod
    def shapes(nf, nc, step, arrays):
        (array,) = arrays
        size = nf if step[0] == "fsdp" else nc
        shape = array.shape if array.ndim == 3 else (size,) + array.shape
        return (
            [jax.ShapeDtypeStruct(shape, array.dtype)],
            [pltpu.SemaphoreType.DMA((3, size))],
            False,
        )

    def begin(self):
        pass

    def send(self):
        self.trade.begin()

    def finish(self):
        self.trade.finish()


class SwapGuest:
    VMEM_IN = 1

    def __init__(self, nf, nc, step, ins, outs, scratch):
        self.blocks, self.out, self.sems = ins[0], outs[0], scratch[0]
        self.move, self.back = (
            (to_column, to_origin) if step == "column" else (to_origin, to_column)
        )

    @staticmethod
    def shapes(nf, nc, step, arrays):
        (array,) = arrays
        return (
            [jax.ShapeDtypeStruct(array.shape, array.dtype)],
            [pltpu.SemaphoreType.DMA((3, 2))],
            False,
        )

    def copies(self, k):
        f, c = lax.axis_index("fsdp"), lax.axis_index("ctx")
        there = self.move(f, c, k)
        source, target = self.blocks.at[k], self.out.at[there[2]]
        away = mesh_copy(
            source, target, self.sems.at[0, k], self.sems.at[1, there[2]], there[:2]
        )
        return elsewhere(there), away, pltpu.make_async_copy(source, target, self.sems.at[2, k])

    def begin(self):
        pass

    def send(self):
        for k in range(2):
            apart, away, stay = self.copies(k)

            @pl.when(apart)
            def _():
                away.start()

            @pl.when(jnp.logical_not(apart))
            def _():
                stay.start()

    def finish(self):
        f, c = lax.axis_index("fsdp"), lax.axis_index("ctx")
        for k in range(2):
            apart, away, stay = self.copies(k)

            @pl.when(apart)
            def _():
                away.wait_send()

            @pl.when(jnp.logical_not(apart))
            def _():
                stay.wait()

            origin = self.back(f, c, k)
            arrival = mesh_copy(
                self.blocks.at[0],
                self.out.at[k],
                self.sems.at[0, 0],
                self.sems.at[1, k],
                origin[:2],
            )

            @pl.when(elsewhere(origin))
            def _():
                arrival.wait_recv()


def begin_guests(made):
    for guest in made:
        guest.begin()
    early_guests(made)


def early_guests(made):
    for guest in made:
        if isinstance(guest, ScatterStep):
            guest.send()


def send_guests(made):
    for guest in made:
        if not isinstance(guest, ScatterStep):
            guest.send()


def pass_on_guests(made):
    for guest in made:
        if isinstance(guest, SideGather):
            guest.side.pass_on()


def needs_of(guest):
    kind, step = guest[0], guest[1]
    if kind is TradeGuest:
        return step[0]
    if kind is SwapGuest:
        return step
    return kind.NEEDS


def split_refs(refs, counts):
    parts, at = [], 0
    for count in counts:
        parts.append(refs[at : at + count])
        at += count
    return parts


def hosted(nf, nc, guests, ins, outs, scratch):
    made, a, b, c = [], 0, 0, 0
    for kind, step, n_in, n_out, n_scratch in guests:
        made.append(
            kind(nf, nc, step, ins[a : a + n_in], outs[b : b + n_out], scratch[c : c + n_scratch])
        )
        a, b, c = a + n_in, b + n_out, c + n_scratch
    return made


def run_guests(made):
    for step in (3, 4):
        for guest in made:
            if isinstance(guest, ScatterRing):
                guest.more(step)
    for guest in made:
        guest.finish()


def lone_kernel(nf, nc, guests, *refs):
    n_in = sum(g[2] for g in guests)
    n_out = sum(g[3] for g in guests)
    ins, outs, scratch = split_refs(refs, (n_in, n_out, len(refs) - n_in - n_out))
    made = hosted(nf, nc, guests, ins, outs, scratch)
    greet_all(nc, {needs_of(g) for g in guests})
    begin_guests(made)
    send_guests(made)
    run_guests(made)


def gather_fsdp_kernel(nf, nc, guests, *refs):
    n_in = sum(g[2] for g in guests)
    n_out = sum(g[3] for g in guests)
    own, ins, out, outs, sems, scratch = split_refs(
        refs, (1, n_in, 1, n_out, 1, len(refs) - n_in - n_out - 3)
    )
    side = FsdpGather(own[0], out[0], sems[0])
    made = hosted(nf, nc, guests, ins, outs, scratch)
    greet_all(nc, {"near"} | {needs_of(g) for g in guests})
    side.begin()
    begin_guests(made)
    send_guests(made)
    side.pass_on()
    side.finish()
    run_guests(made)


def scatter_fsdp_kernel(nf, nc, guests, turned, *refs):
    n_in = sum(g[2] for g in guests)
    n_out = sum(g[3] for g in guests)
    operands, ins, result, outs, own_scratch, scratch = split_refs(
        refs, (2, n_in, 1, n_out, 6, len(refs) - n_in - n_out - 9)
    )
    left_ref, right_ref = operands
    out_ref = result[0]
    part_ref, first_in, own_in, chip_sum, across_in, sems = own_scratch
    shard, partner, cross, corner = fsdp_places()
    place = lax.axis_index("ctx")
    made = hosted(nf, nc, guests, ins, outs, scratch)
    greet_all(nc, {"near"} | {needs_of(g) for g in guests})
    for guest in made:
        guest.begin()
    count, width = out_ref.shape
    chunks = chunks_of(count, 4)

    def copy(kind, k):
        at, size = chunks[k]
        rows = pl.ds(at, size)
        if kind == 0:
            source, target, device = part_ref.at[corner, rows], first_in, partner
        elif kind == 1:
            source, target, device = part_ref.at[partner, rows], own_in, partner
        else:
            source, target, device = chip_sum.at[rows], across_in, cross
        return mesh_copy(
            source,
            target.at[rows],
            sems.at[2 * kind, k],
            sems.at[2 * kind + 1, k],
            (device, place),
        )

    half = count // 2
    early, late = chunks[: len(chunks) // 2], chunks[len(chunks) // 2 :]

    def add_and_send(first, some):
        for k, (at, size) in enumerate(some, first):
            copy(0, k).wait_recv()

            @pl.loop(0, size // 32)
            def _(step):
                rows = pl.ds(pl.multiple_of(at + step * 32, 32), 32)
                chip_sum[rows] = (
                    part_ref[cross, rows].astype(jnp.float32)
                    + first_in[rows].astype(jnp.float32)
                ).astype(chip_sum.dtype)

            copy(2, k).start()

    @pl.loop(0, 8)
    def _(turn):
        pair = turn // 4
        of_two = (turn % 2) * (1 - pair) + (turn // 2 % 2) * pair
        upper = (turn // 2 % 2) * (1 - pair) + (turn % 2) * pair
        base = partner * (1 - of_two) + shard * of_two
        block = (base + 2 * (1 - pair)) % 4
        start = pl.multiple_of(upper * half, half)
        rows = left_ref[pl.ds(pl.multiple_of(block * count + start, half), half), :]
        for at in range(0, width, 512):
            size = 512 if at + 1024 <= width else width - at
            if turned:
                piece = times_transposed(rows, right_ref[at : at + size, :])
            else:
                piece = jnp.dot(
                    rows, right_ref[:, at : at + size], preferred_element_type=jnp.float32
                )
            part_ref[block, pl.ds(start, half), at : at + size] = piece.astype(part_ref.dtype)
            if at + size == width:
                break

        @pl.when(turn == 0)
        def _():
            for k in range(len(early)):
                copy(0, k).start()
            early_guests(made)

        @pl.when(turn == 1)
        def _():
            add_and_send(0, early)

        @pl.when(turn == 2)
        def _():
            for k in range(len(early), len(chunks)):
                copy(0, k).start()

        @pl.when(turn == 3)
        def _():
            add_and_send(len(early), late)
            send_guests(made)

        @pl.when(turn == 5)
        def _():
            for k in range(len(chunks)):
                copy(1, k).start()

    for k, (at, size) in enumerate(chunks):
        copy(1, k).wait_recv()
        copy(2, k).wait_recv()

        @pl.loop(0, size // 32)
        def _(turn):
            rows = pl.ds(pl.multiple_of(at + turn * 32, 32), 32)
            out_ref[rows] = (
                part_ref[shard, rows].astype(jnp.float32)
                + own_in[rows].astype(jnp.float32)
                + across_in[rows].astype(jnp.float32)
            )

    for kind in range(3):
        for k in range(len(chunks)):
            copy(kind, k).wait_send()
    run_guests(made)


def startup_kernel(nf, nc, spans, row_count, *refs):
    ring_count = len(spans)
    total = ring_count + row_count
    ins, outs, sems, extra = split_refs(refs, (total, total, total, 3))
    block, trade_sems, give_sems = extra
    rest = ins[0].shape[1] * nf - block.shape[0]
    rest = rest // (nf - 1)
    thin = ins[0].shape[1] - rest
    trade = Trade(
        "fsdp",
        nf,
        lambda k: ins[0].at[k, pl.ds(0, thin)],
        lambda k: block.at[pl.ds(pl.multiple_of(k * thin, 8), thin)],
        trade_sems,
    )
    giver = lax.axis_index("ctx") // (nc // nf)
    shard = lax.axis_index("fsdp")

    def give(k):
        return mesh_copy(
            ins[0].at[(shard + k) % nf, pl.ds(thin, rest)],
            block.at[pl.ds(nf * thin, rest)],
            give_sems.at[0, k],
            give_sems.at[1, 0],
            ((shard + k) % nf, lax.axis_index("ctx")),
        )

    own_rest = pltpu.make_async_copy(
        ins[0].at[shard, pl.ds(thin, rest)],
        block.at[pl.ds(nf * thin, rest)],
        give_sems.at[0, 0],
    )
    parts = functools.partial(joint_parts, nf, nc, block.shape[0], outs[0].shape[0])
    rings = [
        RingGather(nc, block if k == 0 else ins[k], outs[k], sems[k], None if k else parts)
        for k in range(ring_count)
    ]
    sides = [FsdpGather(ins[k], outs[k], sems[k]) for k in range(ring_count, total)]
    greet(fsdp_peers(3) + ring_peers(nc))
    trade.begin()

    @pl.when(shard == giver)
    def _():
        own_rest.start()
        for k in range(1, nf):
            give(k).start()

    for ring in rings[1:]:
        ring.start(1)
    sides[0].begin()
    trade.finish()

    @pl.when(shard == giver)
    def _():
        own_rest.wait()
        for k in range(1, nf):
            give(k).wait_send()

    @pl.when(shard != giver)
    def _():
        give(1).wait_recv()

    rings[0].start(1)
    sides[0].pass_on()
    for side in sides[1:]:
        side.begin()
    for step in range(2, nc // 2 + 1):
        for ring, span in zip(rings, spans):
            if step <= span:
                ring.advance(step)
        if step == 2:
            for side in sides[1:]:
                side.pass_on()
    for side in sides:
        side.finish()
    for ring, span in zip(rings, spans):
        ring.finish(1, span)


def in_vmem():
    return pl.BlockSpec(memory_space=pltpu.VMEM)


def in_place():
    return pl.BlockSpec(memory_space=pl.ANY)


def widen(pieces):
    return jnp.pad(pieces, ((0, 0),) * (pieces.ndim - 1) + ((0, -pieces.shape[-1] % LANES),))


class Net:
    def __init__(self, nf, nc):
        self.nf, self.nc = nf, nc
        self.each = nc // nf
        self.ids = {}

    def call(self, kernel, key, outs, ins, in_specs, out_specs, scratch, aliases=None):
        ident = self.ids.setdefault(key, len(self.ids))
        return pl.pallas_call(
            kernel,
            out_shape=outs,
            in_specs=in_specs,
            out_specs=out_specs,
            scratch_shapes=scratch,
            input_output_aliases=aliases or {},
            compiler_params=pltpu.CompilerParams(
                collective_id=ident, has_side_effects=True, vmem_limit_bytes=60 << 20
            ),
        )(*ins)

    def swap(self, blocks, move, back):
        place = lax.axis_index("ctx")
        got = []
        for turn in range(self.each):
            slot = (move(0, place, 0)[2] + turn) % self.each
            piece = lax.dynamic_index_in_dim(blocks, slot, 0, keepdims=False)
            pairs = []
            for f in range(self.nf):
                for c in range(self.nc):
                    there = move(f, c, (move(f, c, 0)[2] + turn) % self.each)
                    pairs.append((f * self.nc + c, there[0] * self.nc + there[1]))
            got.append(lax.ppermute(piece, ("fsdp", "ctx"), pairs))
        order = (back(0, place, 0)[2] - jnp.arange(self.each)) % self.each
        return pick(jnp.stack(got), order)

    def total(self, mine, right, left):
        own = lax.dynamic_index_in_dim(mine, lax.axis_index("ctx"), 0, keepdims=False)
        return sum(part.astype(jnp.float32) for part in (own, right, left)).astype(mine.dtype)

    def lone(self, name, hosted_steps):
        plan, ins, outs, scratch, aliases = self.guests(hosted_steps, 0, 0)
        return self.call(
            functools.partial(lone_kernel, self.nf, self.nc, plan),
            name,
            tuple(outs),
            ins,
            self.specs(hosted_steps),
            [in_place()] * len(outs),
            scratch,
            aliases,
        )

    def specs(self, hosted_steps):
        made = []
        for kind, _, arrays in hosted_steps:
            made += [in_vmem() if kind.VMEM_IN else in_place()] * len(arrays)
        return made

    def startup(self, pieces, block_rows, whole_rows, blocks, spans, rows):
        nf, nc = self.nf, self.nc
        first = (block_rows, pieces.shape[2])
        arrays = [pieces] + list(blocks) + list(rows)
        outs = [jax.ShapeDtypeStruct((whole_rows, pieces.shape[2]), pieces.dtype)]
        outs += [jax.ShapeDtypeStruct((nc,) + a.shape, a.dtype) for a in blocks]
        outs += [jax.ShapeDtypeStruct((nf,) + a.shape, a.dtype) for a in rows]
        scratch = [pltpu.SemaphoreType.DMA((5, nc // 2, nf + 1)) for _ in range(1 + len(blocks))]
        scratch += [pltpu.SemaphoreType.DMA(FsdpGather.SEMS) for _ in rows]
        scratch += [pltpu.VMEM(first, pieces.dtype)] + [pltpu.SemaphoreType.DMA((3, nf))] * 2
        count = len(arrays)
        return self.call(
            functools.partial(startup_kernel, nf, nc, tuple(spans), len(rows)),
            "startup", tuple(outs), arrays, [in_vmem()] * count, [in_place()] * count, scratch,
        )

    def guests(self, hosted_steps, first_in, first_out):
        plan, ins, outs, scratch, aliases = [], [], [], [], {}
        for kind, step, arrays in hosted_steps:
            shapes, boxes, alias = kind.shapes(self.nf, self.nc, step, arrays)
            if alias:
                aliases[first_in + len(ins)] = first_out + len(outs)
            plan.append((kind, step, len(arrays), len(shapes), len(boxes)))
            ins += list(arrays)
            outs += shapes
            scratch += boxes
        return tuple(plan), ins, outs, scratch, aliases

    def gather_fsdp(self, name, rows, hosted_steps=()):
        plan, ins, outs, scratch, aliases = self.guests(hosted_steps, 1, 1)
        got = self.call(
            functools.partial(gather_fsdp_kernel, self.nf, self.nc, plan),
            name,
            (jax.ShapeDtypeStruct((self.nf,) + rows.shape, rows.dtype),) + tuple(outs),
            [rows] + ins,
            [in_vmem()] + self.specs(hosted_steps),
            [in_place()] * (1 + len(outs)),
            [pltpu.SemaphoreType.DMA(FsdpGather.SEMS)] + scratch,
            aliases,
        )
        return got[0].reshape((-1,) + rows.shape[1:]), got[1:]

    def scatter_fsdp(self, name, left, right, turned, hosted_steps=()):
        plan, ins, outs, scratch, aliases = self.guests(hosted_steps, 2, 1)
        count = left.shape[0] // self.nf
        block = (count, right.shape[0] if turned else right.shape[1])
        box = pltpu.VMEM(block, left.dtype)
        got = self.call(
            functools.partial(scatter_fsdp_kernel, self.nf, self.nc, plan, turned),
            name,
            (jax.ShapeDtypeStruct(block, jnp.float32),) + tuple(outs),
            [left, right] + ins,
            [in_vmem(), in_vmem()] + self.specs(hosted_steps),
            [in_vmem()] + [in_place()] * len(outs),
            [pltpu.VMEM((self.nf,) + block, left.dtype), box, box, box, box]
            + [pltpu.SemaphoreType.DMA((6, 4))]
            + scratch,
            aliases,
        )
        return got[0], got[1:]

    def attend_forward(self, segs, qkv, hosted_steps):
        rows, wide = qkv.shape
        slots = wide // 3
        pairs = slots // LANES
        plan, ins, outs, scratch, aliases = self.guests(hosted_steps, 3, 3)
        low = jnp.bfloat16
        got = self.call(
            functools.partial(attend_forward_kernel, self.nf, self.nc, plan),
            "attend_forward",
            (
                jax.ShapeDtypeStruct((rows, slots), low),
                jax.ShapeDtypeStruct((pairs, LANES, rows), jnp.float32),
                jax.ShapeDtypeStruct((pairs, 2, rows), jnp.float32),
            )
            + tuple(outs),
            [segs.reshape(1, rows), segs.reshape(rows, 1), qkv] + ins,
            [in_vmem()] * 3 + self.specs(hosted_steps),
            [in_vmem()] * 3 + [in_place()] * len(outs),
            [
                pltpu.VMEM((rows, LANES), low),
                pltpu.VMEM((rows, LANES), low),
                pltpu.VMEM((rows, LANES), low),
                pltpu.VMEM((LANES, rows), low),
                pltpu.VMEM((LANES, TILE), jnp.float32),
                pltpu.VMEM((2, 1, TILE), jnp.float32),
                pltpu.VMEM((2, 1, TILE), jnp.float32),
            ]
            + scratch,
            aliases,
        )
        return got[:3], got[3:]

    def attend_backward(self, segs, qkv, grads, turned, lse, hosted_steps):
        rows, wide = qkv.shape
        plan, ins, outs, scratch, aliases = self.guests(hosted_steps, 6, 1)
        low = jnp.bfloat16
        got = self.call(
            functools.partial(attend_backward_kernel, self.nf, self.nc, plan),
            "attend_backward",
            (jax.ShapeDtypeStruct((rows, wide), low),) + tuple(outs),
            [segs.reshape(1, rows), segs.reshape(rows, 1), qkv, grads, turned, lse] + ins,
            [in_vmem()] * 6 + self.specs(hosted_steps),
            [in_vmem()] + [in_place()] * len(outs),
            [
                pltpu.VMEM((rows, LANES), low),
                pltpu.VMEM((rows, LANES), low),
                pltpu.VMEM((rows, LANES), low),
                pltpu.VMEM((LANES, rows), low),
                pltpu.VMEM((rows, LANES), low),
                pltpu.VMEM((rows, LANES), low),
                pltpu.VMEM((rows, LANES), low),
                pltpu.VMEM((LANES, TILE), jnp.float32),
                pltpu.VMEM((rows, LANES), jnp.float32),
                pltpu.VMEM((rows, LANES), jnp.float32),
                pltpu.VMEM((2, 1, rows), jnp.float32),
            ]
            + scratch,
            aliases,
        )
        return got[0], got[1:]


def local_fast(
    net,
    inputs,
    cotangent,
    segments,
    stretch_order,
    prenorm_gain,
    prenorm_shift,
    joint_weight,
    query_bias,
    value_bias,
    mixer_weight,
    mixer_bias,
    midnorm_gain,
    midnorm_shift,
    expand_weight,
    expand_bias,
    shrink_weight,
    shrink_bias,
):
    nf, nc, each = net.nf, net.nc, net.each
    low, wide = jnp.bfloat16, jnp.float32
    _, stretch_len, width = inputs.shape
    heads_each = -(-(width // HEAD) // nf)
    span = heads_each * HEAD
    slots = slot_width(heads_each)
    rows_all = nc * stretch_len
    rows_own = each * stretch_len
    shard = lax.axis_index("fsdp")
    positions = stretch_order.reshape(each, nf).T.reshape(nc)
    inverse = jnp.sum(
        jnp.where(
            positions[None, :] == jnp.arange(nc, dtype=jnp.int32)[:, None],
            jnp.arange(nc, dtype=jnp.int32)[None, :],
            0,
        ),
        axis=1,
    ).astype(jnp.int32)

    narrow = prenorm_gain.shape[0]
    unit_each = expand_bias.shape[0] // nf

    depth = joint_weight.shape[0]
    thin = depth // (8 * nc) * 8
    rest = (depth - nc * thin) // each
    out_each = shrink_weight.shape[1]
    small_parts = (
        prenorm_gain, prenorm_shift, query_bias, value_bias, mixer_bias,
        midnorm_gain, midnorm_shift, shrink_bias, expand_bias,
    )
    small_count = len(small_parts) - 1 + nf
    small_rows = small_count + -small_count % 16
    last_rows = ((len(small_parts) - 1, small_rows - small_count), (0, 0))
    small_own = rows_of(small_parts[:-1], small_rows) + jnp.pad(
        expand_bias.reshape(nf, narrow), last_rows
    )
    small_own = widen(small_own)
    step = span - mixer_weight.shape[0]
    most = step * (nf - 1)
    columns = joint_weight.shape[1]
    joint_tall = jnp.concatenate(
        [
            joint_weight[: nc * thin].reshape(nc, thin, columns),
            jnp.tile(joint_weight[nc * thin :].reshape(each, rest, columns), (nf, 1, 1)),
        ],
        axis=1,
    )
    seg_own = jnp.broadcast_to(segments.astype(low)[:, None], (each, 16, stretch_len))
    joint_pieces, small_all, own_tokens, seg_own, above, expand_pieces, shrink_pieces = (
        net.lone(
            "first",
            [
                (TradeGuest, ("ctx", None), [widen(joint_tall)]),
                (TradeGuest, ("ctx", None), [small_own]),
                (SwapGuest, "column", [inputs]),
                (SwapGuest, "column", [seg_own]),
                (TradeGuest, ("fsdp", (nf - 1,)), [widen(mixer_weight[:most])]),
                (
                    TradeGuest,
                    ("fsdp", None),
                    [widen(expand_weight.T.reshape(nf, unit_each, depth))],
                ),
                (
                    TradeGuest,
                    ("fsdp", None),
                    [
                        widen(
                            shrink_weight.reshape(each, nf, unit_each, out_each)
                            .transpose(1, 0, 2, 3)
                            .reshape(nf, each * unit_each, out_each)
                        )
                    ],
                ),
            ],
        )
    )
    own_tokens = own_tokens.reshape(rows_own, width)
    joint_pieces = joint_pieces[..., :columns].transpose(1, 0, 2)
    joint_pieces = joint_split(joint_pieces.reshape(thin + rest, 3, width), nf, heads_each)
    expand_pieces = (
        expand_pieces[..., :depth].transpose(1, 0, 2).reshape(unit_each, width)
    )
    shrink_pieces = shrink_pieces[..., :out_each].reshape(nc * unit_each, out_each).T

    above = lax.dynamic_index_in_dim(above, (shard + 1) % nf, 0, keepdims=False)
    above = above[:, : mixer_weight.shape[1]]
    tall = jnp.concatenate([mixer_weight, above, jnp.zeros_like(above)])
    mixer_rows = lax.dynamic_slice_in_dim(tall, step * shard, span, 0)
    kept = shard * span + jnp.arange(span, dtype=jnp.int32) < width
    mixer_rows = jnp.where(kept[:, None], mixer_rows, jnp.zeros_like(mixer_rows))
    mixer_pieces = jnp.pad(mixer_rows.T, ((0, 0), (0, slots - span)))

    joint, mixer, expand, shrink, tokens, seg_blocks = net.startup(
        joint_pieces,
        nf * thin + rest,
        width,
        [mixer_pieces, expand_pieces, shrink_pieces],
        [nc // 2, nc // 2, 1, 1],
        [own_tokens, seg_own.reshape(each * 16, stretch_len)],
    )
    mixer = mixer.reshape(width, slots)
    tokens = tokens.reshape(rows_all, width)
    cotangent, tokens = lax.optimization_barrier((cotangent, tokens))
    own_tangent = net.swap(cotangent, to_column, to_origin).reshape(rows_own, width)
    segs = pick(seg_blocks.reshape(nc, 16, stretch_len)[:, 0], inverse)
    segs = segs.astype(jnp.int32)
    small_all = small_all[:, :small_count, :narrow].transpose(1, 0, 2).astype(wide)
    gain_one, shift_one, qbias, vbias, mbias, gain_two, shift_two, sbias = (
        small_all[: small_count - nf].reshape(small_count - nf, width)
    )
    ebias = small_all[small_count - nf :].reshape(nf, nc, unit_each)
    ebias = all_units(ebias, nc, nf, unit_each, shard)
    joint_bias = lax.dynamic_index_in_dim(
        joint_split(
            jnp.stack([qbias, jnp.zeros_like(qbias), vbias])[None], nf, heads_each
        ),
        shard, 0, keepdims=False,
    )

    tokens = pick(tokens.reshape(nc, stretch_len, width), inverse)
    token_values = tokens.reshape(rows_all, width).astype(wide)
    unit_one, _ = normalize(token_values)
    normed = (unit_one * gain_one + shift_one).astype(low)
    qkv = (
        jnp.dot(normed, joint, preferred_element_type=wide) + joint_bias
    ).astype(low)
    (attended, turned, lse), (expand, shrink, tangent) = net.attend_forward(
        segs,
        qkv,
        [
            (GatherStep, 2, [expand]),
            (GatherStep, 2, [shrink]),
            (SideGather, 0, [own_tangent]),
        ],
    )
    attended = pick(attended.reshape(nc, stretch_len, slots), positions)
    attended = attended.reshape(rows_all, slots)
    branch, (expand, shrink) = net.scatter_fsdp(
        "scatter_branch",
        attended,
        mixer,
        True,
        [
            (GatherStep, 3, [expand]),
            (GatherStep, 3, [shrink]),
        ],
    )
    tangent = tangent.reshape(rows_all, width)
    middle = own_tokens.astype(wide) + branch + mbias
    unit_two, inverse_two = normalize(middle)
    second_own = (unit_two * gain_two + shift_two).astype(low)
    second, (expand, shrink) = net.gather_fsdp(
        "gather_second", second_own, [(GatherStep, 4, [expand]), (GatherStep, 4, [shrink])]
    )
    expand = expand.reshape(nc * unit_each, width)
    shrink = shrink.reshape(width, nc * unit_each)
    expanded = times_transposed(second, expand) + ebias
    active, slope = gelu_parts(expanded)
    active = active.astype(low)

    shrink_rows = outer_sum(tangent, active).astype(low).reshape(nc, out_each, nc * unit_each)
    active_grad = jnp.dot(tangent, shrink, preferred_element_type=wide)
    expand_delta = (active_grad * slope).astype(low)
    expand_rows = outer_sum(expand_delta, second).astype(low).reshape(nc, unit_each, width)
    second_grad, boxes = net.scatter_fsdp(
        "scatter_second",
        expand_delta,
        expand,
        False,
        [(ScatterStep, 1, [expand_rows]), (ScatterStep, 1, [shrink_rows])],
    )
    middle_delta = own_tangent.astype(wide) + normalize_back(
        second_grad, gain_two, unit_two, inverse_two
    )
    branch_own = middle_delta.astype(low)
    branch_delta, boxes = net.gather_fsdp(
        "gather_branch",
        branch_own,
        [(ScatterStep, 2, [expand_rows, *boxes[:2]]), (ScatterStep, 2, [shrink_rows, *boxes[2:]])],
    )
    lifted, boxes = net.scatter_fsdp(
        "scatter_lifted",
        active,
        shrink,
        True,
        [(ScatterStep, 3, [expand_rows, *boxes[:2]]), (ScatterStep, 3, [shrink_rows, *boxes[2:]])],
    )
    out_rows = (middle + lifted + sbias).astype(low)
    block_output = net.swap(out_rows.reshape(each, stretch_len, width), to_origin, to_column)
    attended_delta = jnp.dot(branch_delta, mixer, preferred_element_type=wide).astype(low)
    mixer_rows = outer_sum(branch_delta, attended).astype(low).reshape(nc, out_each, slots)
    attended_delta = pick(attended_delta.reshape(nc, stretch_len, slots), inverse).reshape(
        rows_all, slots
    )
    joint_delta, boxes = net.attend_backward(
        segs,
        qkv,
        attended_delta,
        turned,
        lse,
        [(ScatterStep, 4, [expand_rows, *boxes[:2]]), (ScatterStep, 4, [shrink_rows, *boxes[2:]])],
    )
    expand_grad = net.total(expand_rows, *boxes[:2])
    shrink_grad = net.total(shrink_rows, *boxes[2:])
    joint_rows = outer_sum(normed, joint_delta).astype(low)
    normed_grad, (joint_grad, mixer_grad, expand_pieces, shrink_pieces) = (
        net.scatter_fsdp(
            "scatter_normed",
            pick(joint_delta.reshape(nc, stretch_len, 3 * slots), positions).reshape(
                rows_all, 3 * slots
            ),
            joint,
            True,
            [
                (ScatterRing, nf * thin + rest, [joint_rows]),
                (ScatterRing, 0, [mixer_rows]),
                (
                    TradeGuest,
                    ("fsdp", None),
                    [widen(expand_grad.reshape(unit_each, nf, depth).transpose(1, 0, 2))],
                ),
                (
                    TradeGuest,
                    ("fsdp", None),
                    [widen(shrink_grad.T.reshape(nf, each * unit_each, out_each))],
                ),
            ],
        )
    )
    unit_own, inverse_own = normalize(own_tokens.astype(wide))
    input_rows = middle_delta + normalize_back(normed_grad, gain_one, unit_own, inverse_own)
    mine = jnp.arange(nf, dtype=jnp.int32) == shard
    sums = jnp.sum(joint_delta.astype(wide), axis=0).reshape(3, slots)[:, :span]
    spread = jnp.where(mine[None, :, None], sums[:, None, :], 0.0).reshape(3, nf * span)
    unit_sums = jnp.sum(expand_delta.astype(wide), axis=0).reshape(nc, 1, unit_each)
    unit_sums = jnp.where(mine[None, :, None], unit_sums, 0.0).reshape(nc, nf * unit_each)
    vectors = (
        jnp.sum(normed_grad * unit_own, axis=0),
        jnp.sum(normed_grad, axis=0),
        spread[0, :width],
        spread[2, :width],
        jnp.sum(branch_own.astype(wide), axis=0),
        jnp.sum(second_grad * unit_two, axis=0),
        jnp.sum(second_grad, axis=0),
        jnp.sum(own_tangent.astype(wide), axis=0),
    )
    stacked = rows_of(vectors, len(vectors)).reshape(len(vectors), nc, narrow)
    unit_sums = unit_sums.reshape(nc, nf, narrow).transpose(1, 0, 2)
    small_blocks = jnp.concatenate(
        [stacked, unit_sums, jnp.zeros((small_rows - small_count, nc, narrow), wide)]
    )
    small_blocks = widen(small_blocks.astype(low)).transpose(1, 0, 2)
    small_lanes = small_blocks.shape[2]

    joint_pieces, joint_last, mixer_pieces, small_pieces, input_gradient = net.lone(
        "second",
        [
            (
                TradeGuest,
                ("fsdp", None),
                [joint_grad[: nf * thin].reshape(nf, thin, 3 * slots)],
            ),
            (TradeGuest, ("fsdp", None), [joint_grad[nf * thin :]]),
            (TradeGuest, ("fsdp", (1,)), [mixer_grad]),
            (TradeGuest, ("fsdp", None), [small_blocks.reshape(nc * small_rows, small_lanes)]),
            (SwapGuest, "origin", [input_rows.astype(low).reshape(each, stretch_len, width)]),
        ],
    )
    input_gradient = input_gradient.astype(wide)
    small_blocks = jnp.sum(small_pieces.astype(wide), axis=0).astype(low)
    joint_pieces = jnp.concatenate([joint_pieces, joint_last], axis=1)
    joint_pieces = joint_join(joint_pieces, heads_each, width)
    joint_pieces = joint_pieces.reshape(thin + rest, nc, columns).transpose(1, 0, 2)
    joint_pieces, small_pieces = net.lone(
        "third",
        [
            (TradeGuest, ("ctx", None), [widen(joint_pieces)]),
            (TradeGuest, ("ctx", None), [small_blocks.reshape(nc, small_rows, small_lanes)]),
        ],
    )
    joint_pieces = joint_pieces[..., :columns]
    joint_last = lax.dynamic_slice_in_dim(joint_pieces[:, thin:], each * shard, each, 0)
    joint_gradient = jnp.concatenate(
        [
            joint_pieces[:, :thin].reshape(nc * thin, columns),
            joint_last.reshape(each * rest, columns),
        ]
    ).astype(wide)
    expand_gradient = expand_pieces[..., :depth].reshape(nf * unit_each, depth).T.astype(wide)
    shrink_pieces = shrink_pieces[..., :out_each].reshape(nf, each, unit_each, out_each)
    shrink_pieces = shrink_pieces.transpose(1, 0, 2, 3)
    shrink_gradient = shrink_pieces.reshape(shrink_weight.shape).astype(wide)

    own_rows = lax.dynamic_index_in_dim(mixer_pieces, shard, 0, keepdims=False)[:, :span].T
    before = lax.dynamic_index_in_dim(mixer_pieces, (shard + nf - 1) % nf, 0, keepdims=False)
    below = lax.dynamic_slice_in_dim(
        jnp.pad(before[:, :span].T, ((0, most), (0, 0))),
        mixer_weight.shape[0] - step * ((shard + nf - 1) % nf),
        most,
        0,
    )
    moved = lax.dynamic_slice_in_dim(
        jnp.pad(own_rows, ((most, 0), (0, 0))), most - step * shard, mixer_weight.shape[0], 0
    )
    first_rows = jnp.arange(mixer_weight.shape[0], dtype=jnp.int32)[:, None] < step * shard
    below = jnp.pad(below, ((0, mixer_weight.shape[0] - most), (0, 0)))
    mixer_gradient = jnp.where(first_rows, below, moved).astype(wide)

    small_sum = jnp.sum(small_pieces.astype(wide), axis=0)[:small_count, :narrow]
    outs = [small_sum[k] for k in range(8)]
    return (
        block_output,
        input_gradient,
        outs[0],
        outs[1],
        joint_gradient,
        outs[2],
        outs[3],
        mixer_gradient,
        outs[4],
        outs[5],
        outs[6],
        expand_gradient,
        small_sum[8:].reshape(expand_bias.shape),
        shrink_gradient,
        outs[7],
    )


def solution(mesh):
    in_specs = (
        P("fsdp", "ctx", None),
        P("fsdp", "ctx", None),
        P("fsdp", "ctx"),
        P(),
        P("ctx"),
        P("ctx"),
        P("fsdp", "ctx"),
        P("ctx"),
        P("ctx"),
        P("fsdp", "ctx"),
        P("ctx"),
        P("ctx"),
        P("ctx"),
        P("fsdp", "ctx"),
        P("ctx"),
        P("fsdp", "ctx"),
        P("ctx"),
    )
    out_specs = (
        P("fsdp", "ctx", None),
        P("fsdp", "ctx", None),
        P("ctx"),
        P("ctx"),
        P("fsdp", "ctx"),
        P("ctx"),
        P("ctx"),
        P("fsdp", "ctx"),
        P("ctx"),
        P("ctx"),
        P("ctx"),
        P("fsdp", "ctx"),
        P("ctx"),
        P("fsdp", "ctx"),
        P("ctx"),
    )

    def run(*arrays):
        nf, nc = mesh.shape["fsdp"], mesh.shape["ctx"]
        whole_each = arrays[0].shape[0] == nc and (nf, nc) == (4, 8)
        if whole_each and arrays[0].shape[1] == nc * STRETCH:
            body = functools.partial(local_fast, Net(nf, nc))
        else:
            body = local
        return jax.shard_map(
            body, mesh=mesh, in_specs=in_specs, out_specs=out_specs, check_vma=False
        )(*arrays)

    return run
```

```python
import functools

import jax
import jax.numpy as jnp
from jax import lax
from jax.experimental import pallas as pl
from jax.experimental.pallas import tpu as pltpu
from jax.sharding import PartitionSpec as P


HEAD = 64
MICRO = 2
LANES = 128
STRETCH = 128
TILE = 256


epsilon = 1e-05
masked_score = -1e30


def layer_norm(values, gain, shift):
    center = values - jnp.mean(values, axis=-1, keepdims=True)
    spread = jnp.mean(center * center, axis=-1, keepdims=True)
    return center * lax.rsqrt(spread + epsilon) * gain + shift


def piece_size(count):
    size_now = min(count, 512)
    while count % size_now:
        size_now -= 1
    return size_now


def true_positions(stretch_order, first_index, count, stretch_len):
    stored = first_index + jnp.arange(count, dtype=jnp.int32)
    holder = stored // stretch_len
    picked = holder[:, None] == jnp.arange(stretch_order.shape[0], dtype=jnp.int32)[None, :]
    return (
        jnp.sum(jnp.where(picked, stretch_order[None, :], 0), axis=1) * stretch_len
        + stored % stretch_len
    )


def times_transposed(left, right):
    return lax.dot_general(
        left, right, (((1,), (1,)), ((), ())), preferred_element_type=jnp.float32
    )


def outer_sum(left, right):
    return lax.dot_general(
        left, right, (((0,), (0,)), ((), ())), preferred_element_type=jnp.float32
    )


def fetch_weights(local_parts):
    (
        joint_weight,
        mixer_weight,
        expand_weight,
        shrink_weight,
        prenorm_gain,
        prenorm_shift,
        query_bias,
        value_bias,
        mixer_bias,
        midnorm_gain,
        midnorm_shift,
        expand_bias,
        shrink_bias,
    ) = local_parts
    spread_out = (
        lax.all_gather(joint_weight, "ctx", axis=1, tiled=True),
        lax.all_gather(mixer_weight, "ctx", axis=1, tiled=True),
        lax.all_gather(expand_weight, "ctx", axis=1, tiled=True),
        lax.all_gather(shrink_weight, "ctx", axis=1, tiled=True),
        lax.all_gather(prenorm_gain, "ctx", axis=0, tiled=True),
        lax.all_gather(prenorm_shift, "ctx", axis=0, tiled=True),
        lax.all_gather(query_bias, "ctx", axis=0, tiled=True),
        lax.all_gather(value_bias, "ctx", axis=0, tiled=True),
        lax.all_gather(mixer_bias, "ctx", axis=0, tiled=True),
        lax.all_gather(midnorm_gain, "ctx", axis=0, tiled=True),
        lax.all_gather(midnorm_shift, "ctx", axis=0, tiled=True),
        lax.all_gather(expand_bias, "ctx", axis=0, tiled=True),
        lax.all_gather(shrink_bias, "ctx", axis=0, tiled=True),
    )
    whole_rows = (
        lax.all_gather(spread_out[0], "fsdp", axis=0, tiled=True),
        lax.all_gather(spread_out[1], "fsdp", axis=0, tiled=True),
        lax.all_gather(spread_out[2], "fsdp", axis=0, tiled=True),
        lax.all_gather(spread_out[3], "fsdp", axis=0, tiled=True),
    )
    return tuple(whole_rows) + tuple(spread_out[4:])


def reduce_gradients(matrices, smalls):
    small_sums = (
        lax.psum(smalls[0].astype(jnp.bfloat16), "fsdp").astype(jnp.float32),
        lax.psum(smalls[1].astype(jnp.bfloat16), "fsdp").astype(jnp.float32),
        lax.psum(smalls[2].astype(jnp.bfloat16), "fsdp").astype(jnp.float32),
        lax.psum(smalls[3].astype(jnp.bfloat16), "fsdp").astype(jnp.float32),
        lax.psum(smalls[4].astype(jnp.bfloat16), "fsdp").astype(jnp.float32),
        lax.psum(smalls[5].astype(jnp.bfloat16), "fsdp").astype(jnp.float32),
        lax.psum(smalls[6].astype(jnp.bfloat16), "fsdp").astype(jnp.float32),
        lax.psum(smalls[7].astype(jnp.bfloat16), "fsdp").astype(jnp.float32),
        lax.psum(smalls[8].astype(jnp.bfloat16), "fsdp").astype(jnp.float32),
    )
    column_part = (
        lax.psum_scatter(
            matrices[0].astype(jnp.bfloat16), "ctx", scatter_dimension=1, tiled=True
        ).astype(jnp.float32),
        lax.psum_scatter(
            matrices[1].astype(jnp.bfloat16), "ctx", scatter_dimension=1, tiled=True
        ).astype(jnp.float32),
        lax.psum_scatter(
            matrices[2].astype(jnp.bfloat16), "ctx", scatter_dimension=1, tiled=True
        ).astype(jnp.float32),
        lax.psum_scatter(
            matrices[3].astype(jnp.bfloat16), "ctx", scatter_dimension=1, tiled=True
        ).astype(jnp.float32),
        lax.psum_scatter(
            small_sums[0].astype(jnp.bfloat16), "ctx", scatter_dimension=0, tiled=True
        ).astype(jnp.float32),
        lax.psum_scatter(
            small_sums[1].astype(jnp.bfloat16), "ctx", scatter_dimension=0, tiled=True
        ).astype(jnp.float32),
        lax.psum_scatter(
            small_sums[2].astype(jnp.bfloat16), "ctx", scatter_dimension=0, tiled=True
        ).astype(jnp.float32),
        lax.psum_scatter(
            small_sums[3].astype(jnp.bfloat16), "ctx", scatter_dimension=0, tiled=True
        ).astype(jnp.float32),
        lax.psum_scatter(
            small_sums[4].astype(jnp.bfloat16), "ctx", scatter_dimension=0, tiled=True
        ).astype(jnp.float32),
        lax.psum_scatter(
            small_sums[5].astype(jnp.bfloat16), "ctx", scatter_dimension=0, tiled=True
        ).astype(jnp.float32),
        lax.psum_scatter(
            small_sums[6].astype(jnp.bfloat16), "ctx", scatter_dimension=0, tiled=True
        ).astype(jnp.float32),
        lax.psum_scatter(
            small_sums[7].astype(jnp.bfloat16), "ctx", scatter_dimension=0, tiled=True
        ).astype(jnp.float32),
        lax.psum_scatter(
            small_sums[8].astype(jnp.bfloat16), "ctx", scatter_dimension=0, tiled=True
        ).astype(jnp.float32),
    )
    row_part = (
        lax.psum_scatter(
            column_part[0].astype(jnp.bfloat16), "fsdp", scatter_dimension=0, tiled=True
        ).astype(jnp.float32),
        lax.psum_scatter(
            column_part[1].astype(jnp.bfloat16), "fsdp", scatter_dimension=0, tiled=True
        ).astype(jnp.float32),
        lax.psum_scatter(
            column_part[2].astype(jnp.bfloat16), "fsdp", scatter_dimension=0, tiled=True
        ).astype(jnp.float32),
        lax.psum_scatter(
            column_part[3].astype(jnp.bfloat16), "fsdp", scatter_dimension=0, tiled=True
        ).astype(jnp.float32),
    )
    return tuple(row_part) + tuple(column_part[4:])


def local(
    inputs,
    cotangent,
    segments,
    stretch_order,
    prenorm_gain,
    prenorm_shift,
    joint_weight,
    query_bias,
    value_bias,
    mixer_weight,
    mixer_bias,
    midnorm_gain,
    midnorm_shift,
    expand_weight,
    expand_bias,
    shrink_weight,
    shrink_bias,
):
    local_parts = (
        joint_weight,
        mixer_weight,
        expand_weight,
        shrink_weight,
        prenorm_gain,
        prenorm_shift,
        query_bias,
        value_bias,
        mixer_bias,
        midnorm_gain,
        midnorm_shift,
        expand_bias,
        shrink_bias,
    )
    seq_local, stretch_len, model_width = inputs.shape
    head_count = model_width // HEAD
    group_size = seq_local // MICRO
    row_count = group_size * stretch_len
    score_scale = HEAD ** (-0.5)
    ctx_place = lax.axis_index("ctx")
    own_stretch = jnp.sum(
        jnp.where(
            jnp.arange(stretch_order.shape[0], dtype=jnp.int32) == ctx_place, stretch_order, 0
        )
    )
    own_pos = own_stretch * stretch_len + jnp.arange(stretch_len, dtype=jnp.int32)
    all_segments = lax.all_gather(segments, "ctx", axis=1, tiled=True)

    def backward_micro(weights, kept_values, micro_index):
        (
            joint_full,
            mixer_full,
            expand_full,
            shrink_full,
            gain_one,
            shift_one,
            _,
            _,
            _,
            gain_two,
            shift_two,
            _,
            _,
        ) = weights
        (
            tokens,
            seg_local,
            seg_whole,
            normed,
            queries,
            keys_local,
            values_local,
            mixed_rows,
            attended,
            log_total,
            middle,
            second,
            expanded,
            active,
        ) = kept_values
        lower = micro_index * group_size
        tangent_rows = cotangent[lower : lower + group_size].reshape(row_count, model_width)
        active_grad = times_transposed(tangent_rows, shrink_full)
        gelu_pull = jax.vjp(lambda value_in: jax.nn.gelu(value_in, approximate=True), expanded)[1]
        expand_delta = gelu_pull(active_grad)[0].astype(jnp.bfloat16)
        second_grad = times_transposed(expand_delta, expand_full)
        mid_pull = jax.vjp(
            layer_norm, middle, gain_two.astype(jnp.float32), shift_two.astype(jnp.float32)
        )[1]
        middle_grad, gain_two_grad, shift_two_grad = mid_pull(second_grad)
        middle_grad = middle_grad + tangent_rows.astype(jnp.float32)
        branch_delta = middle_grad.astype(jnp.bfloat16)
        attended_delta = times_transposed(branch_delta, mixer_full).astype(jnp.bfloat16)
        grad_heads = attended_delta.reshape(group_size, stretch_len, head_count, HEAD)
        delta_heads = jnp.sum(
            grad_heads.transpose(0, 2, 1, 3).astype(jnp.float32) * attended, axis=-1
        )
        delta_rows = delta_heads.transpose(0, 2, 1)
        log_rows = log_total.transpose(0, 2, 1)
        lse_whole, delta_whole = (
            lax.all_gather(log_rows, "ctx", axis=1, tiled=True),
            lax.all_gather(delta_rows, "ctx", axis=1, tiled=True),
        )
        query_heads = queries.reshape(group_size, stretch_len, head_count, HEAD)
        key_heads = keys_local.reshape(group_size, stretch_len, head_count, HEAD)
        value_heads = values_local.reshape(group_size, stretch_len, head_count, HEAD)
        head_zeros = jnp.zeros((group_size, head_count, stretch_len, HEAD), jnp.float32)
        query_key_piece = lax.all_gather(keys_local, "ctx", axis=1, tiled=True)
        value_piece = lax.all_gather(values_local, "ctx", axis=1, tiled=True)
        count = query_key_piece.shape[1]
        step_len = piece_size(count)

        def query_block_step(turn_index, running):
            offset = turn_index * step_len
            key_block = lax.dynamic_slice_in_dim(query_key_piece, offset, step_len, 1).reshape(
                group_size, step_len, head_count, HEAD
            )
            value_block = lax.dynamic_slice_in_dim(value_piece, offset, step_len, 1).reshape(
                group_size, step_len, head_count, HEAD
            )
            key_pos = true_positions(stretch_order, offset, step_len, stretch_len)
            key_seg = lax.dynamic_slice_in_dim(seg_whole, offset, step_len, 1)
            allowed = (
                (seg_local[:, :, None] == key_seg[:, None, :])
                & (key_pos[None, None, :] <= own_pos[None, :, None])
            )[:, None]
            scores = (
                jnp.einsum(
                    "gqhd,gkhd->ghqk", query_heads, key_block, preferred_element_type=jnp.float32
                )
                * score_scale
            )
            probs = jnp.where(allowed, jnp.exp(scores - log_total[..., None]), 0.0)
            dots = jnp.einsum(
                "gqhd,gkhd->ghqk", grad_heads, value_block, preferred_element_type=jnp.float32
            )
            score_delta = (probs * (dots - delta_heads[..., None])).astype(jnp.bfloat16)
            return running + jnp.einsum(
                "ghqk,gkhd->ghqd", score_delta, key_block, preferred_element_type=jnp.float32
            )

        query_acc = lax.fori_loop(0, count // step_len, query_block_step, head_zeros)
        grad_rows3 = attended_delta.reshape(group_size, stretch_len, model_width)
        query_piece_rows = lax.all_gather(queries, "ctx", axis=1, tiled=True)
        grad_piece = lax.all_gather(grad_rows3, "ctx", axis=1, tiled=True)
        count = query_piece_rows.shape[1]
        key_step_len = piece_size(count)

        def key_block_step(turn_index, running):
            key_acc, value_acc = running
            offset = turn_index * key_step_len
            query_block = lax.dynamic_slice_in_dim(
                query_piece_rows, offset, key_step_len, 1
            ).reshape(group_size, key_step_len, head_count, HEAD)
            grad_block = lax.dynamic_slice_in_dim(grad_piece, offset, key_step_len, 1).reshape(
                group_size, key_step_len, head_count, HEAD
            )
            query_pos = true_positions(stretch_order, offset, key_step_len, stretch_len)
            query_seg = lax.dynamic_slice_in_dim(seg_whole, offset, key_step_len, 1)
            lse_block = lax.dynamic_slice_in_dim(lse_whole, offset, key_step_len, 1).transpose(
                0, 2, 1
            )
            delta_block = lax.dynamic_slice_in_dim(delta_whole, offset, key_step_len, 1).transpose(
                0, 2, 1
            )
            allowed = (
                (query_seg[:, :, None] == seg_local[:, None, :])
                & (own_pos[None, None, :] <= query_pos[None, :, None])
            )[:, None]
            scores = (
                jnp.einsum(
                    "gqhd,gkhd->ghqk", query_block, key_heads, preferred_element_type=jnp.float32
                )
                * score_scale
            )
            probs = jnp.where(allowed, jnp.exp(scores - lse_block[..., None]), 0.0)
            value_acc = value_acc + jnp.einsum(
                "ghqk,gqhd->ghkd",
                probs.astype(jnp.bfloat16),
                grad_block,
                preferred_element_type=jnp.float32,
            )
            dots = jnp.einsum(
                "gqhd,gkhd->ghqk", grad_block, value_heads, preferred_element_type=jnp.float32
            )
            score_delta = (probs * (dots - delta_block[..., None])).astype(jnp.bfloat16)
            key_acc = key_acc + jnp.einsum(
                "ghqk,gqhd->ghkd", score_delta, query_block, preferred_element_type=jnp.float32
            )
            return (key_acc, value_acc)

        key_acc, value_acc = lax.fori_loop(
            0, count // key_step_len, key_block_step, (head_zeros, head_zeros)
        )
        query_delta = (
            (query_acc * score_scale)
            .transpose(0, 2, 1, 3)
            .reshape(row_count, model_width)
            .astype(jnp.bfloat16)
        )
        key_delta = (
            (key_acc * score_scale)
            .transpose(0, 2, 1, 3)
            .reshape(row_count, model_width)
            .astype(jnp.bfloat16)
        )
        value_delta = (
            value_acc.transpose(0, 2, 1, 3).reshape(row_count, model_width).astype(jnp.bfloat16)
        )
        joint_delta = jnp.concatenate([query_delta, key_delta, value_delta], axis=1)
        normed_grad = times_transposed(joint_delta, joint_full)
        first_pull = jax.vjp(
            layer_norm,
            tokens.reshape(row_count, model_width),
            gain_one.astype(jnp.float32),
            shift_one.astype(jnp.float32),
        )[1]
        token_grad, gain_one_grad, shift_one_grad = first_pull(normed_grad)
        input_grad = (middle_grad + token_grad).reshape(group_size, stretch_len, model_width)
        small_terms = (
            gain_one_grad,
            shift_one_grad,
            jnp.sum(query_delta.astype(jnp.float32), axis=0),
            jnp.sum(value_delta.astype(jnp.float32), axis=0),
            jnp.sum(branch_delta.astype(jnp.float32), axis=0),
            gain_two_grad,
            shift_two_grad,
            jnp.sum(expand_delta.astype(jnp.float32), axis=0),
            jnp.sum(tangent_rows.astype(jnp.float32), axis=0),
        )
        factor_pairs = (
            normed.reshape(row_count, model_width),
            joint_delta,
            mixed_rows,
            branch_delta,
            second,
            expand_delta,
            active,
            tangent_rows,
        )
        return (input_grad, small_terms, factor_pairs)

    output_list = []
    input_list = []
    factor_list = []
    small_totals = None
    for micro_index in range(MICRO):
        forward_weights = fetch_weights(local_parts)
        (
            forward_joint_full,
            forward_mixer_full,
            forward_expand_full,
            forward_shrink_full,
            forward_gain_one,
            forward_shift_one,
            forward_qbias_full,
            forward_vbias_full,
            forward_mbias_full,
            forward_gain_two,
            forward_shift_two,
            forward_ebias_full,
            forward_sbias_full,
        ) = forward_weights
        forward_lower = micro_index * group_size
        forward_tokens = inputs[forward_lower : forward_lower + group_size].astype(jnp.float32)
        forward_seg_local = segments[forward_lower : forward_lower + group_size]
        forward_seg_whole = all_segments[forward_lower : forward_lower + group_size]
        forward_normed = layer_norm(
            forward_tokens,
            forward_gain_one.astype(jnp.float32),
            forward_shift_one.astype(jnp.float32),
        ).astype(jnp.bfloat16)
        joint_bias = jnp.concatenate(
            [forward_qbias_full, jnp.zeros_like(forward_qbias_full), forward_vbias_full]
        ).astype(jnp.float32)
        joint_rows = (
            jnp.dot(
                forward_normed.reshape(row_count, model_width),
                forward_joint_full,
                preferred_element_type=jnp.float32,
            )
            + joint_bias
        )
        joint_rows = joint_rows.astype(jnp.bfloat16).reshape(
            group_size, stretch_len, 3 * model_width
        )
        forward_queries = joint_rows[..., :model_width]
        forward_keys_local = joint_rows[..., model_width : 2 * model_width]
        forward_values_local = joint_rows[..., 2 * model_width :]
        forward_query_heads = forward_queries.reshape(group_size, stretch_len, head_count, HEAD)
        start_state = (
            jnp.full((group_size, head_count, stretch_len), masked_score, jnp.float32),
            jnp.zeros((group_size, head_count, stretch_len), jnp.float32),
            jnp.zeros((group_size, head_count, stretch_len, HEAD), jnp.float32),
        )
        forward_key_piece = lax.all_gather(forward_keys_local, "ctx", axis=1, tiled=True)
        forward_value_piece = lax.all_gather(forward_values_local, "ctx", axis=1, tiled=True)
        forward_count = forward_key_piece.shape[1]
        forward_step_len = piece_size(forward_count)

        def forward_block_step(turn_index, state):
            top_score, row_total, accumulated = state
            offset = turn_index * forward_step_len
            key_block = lax.dynamic_slice_in_dim(
                forward_key_piece, offset, forward_step_len, 1
            ).reshape(group_size, forward_step_len, head_count, HEAD)
            value_block = lax.dynamic_slice_in_dim(
                forward_value_piece, offset, forward_step_len, 1
            ).reshape(group_size, forward_step_len, head_count, HEAD)
            key_pos = true_positions(stretch_order, offset, forward_step_len, stretch_len)
            key_seg = lax.dynamic_slice_in_dim(forward_seg_whole, offset, forward_step_len, 1)
            allowed = (
                (forward_seg_local[:, :, None] == key_seg[:, None, :])
                & (key_pos[None, None, :] <= own_pos[None, :, None])
            )[:, None]
            scores = (
                jnp.einsum(
                    "gqhd,gkhd->ghqk",
                    forward_query_heads,
                    key_block,
                    preferred_element_type=jnp.float32,
                )
                * score_scale
            )
            scores = jnp.where(allowed, scores, masked_score)
            new_top = jnp.maximum(top_score, jnp.max(scores, axis=-1))
            weights_now = jnp.where(allowed, jnp.exp(scores - new_top[..., None]), 0.0)
            fade_factor = jnp.exp(top_score - new_top)
            row_total = row_total * fade_factor + jnp.sum(weights_now, axis=-1)
            accumulated = accumulated * fade_factor[..., None] + jnp.einsum(
                "ghqk,gkhd->ghqd",
                weights_now.astype(jnp.bfloat16),
                value_block,
                preferred_element_type=jnp.float32,
            )
            return (new_top, row_total, accumulated)

        top_score, row_total, accumulated = lax.fori_loop(
            0, forward_count // forward_step_len, forward_block_step, start_state
        )
        forward_attended = accumulated / row_total[..., None]
        forward_log_total = top_score + jnp.log(row_total)
        forward_mixed_rows = (
            forward_attended.transpose(0, 2, 1, 3)
            .reshape(row_count, model_width)
            .astype(jnp.bfloat16)
        )
        branch = jnp.dot(
            forward_mixed_rows, forward_mixer_full, preferred_element_type=jnp.float32
        ) + forward_mbias_full.astype(jnp.float32)
        forward_middle = forward_tokens.reshape(row_count, model_width) + branch
        forward_second = layer_norm(
            forward_middle,
            forward_gain_two.astype(jnp.float32),
            forward_shift_two.astype(jnp.float32),
        ).astype(jnp.bfloat16)
        forward_expanded = jnp.dot(
            forward_second, forward_expand_full, preferred_element_type=jnp.float32
        ) + forward_ebias_full.astype(jnp.float32)
        forward_active = jax.nn.gelu(forward_expanded, approximate=True).astype(jnp.bfloat16)
        output = (
            forward_middle
            + jnp.dot(forward_active, forward_shrink_full, preferred_element_type=jnp.float32)
            + forward_sbias_full.astype(jnp.float32)
        )
        forward_kept_values = (
            forward_tokens,
            forward_seg_local,
            forward_seg_whole,
            forward_normed,
            forward_queries,
            forward_keys_local,
            forward_values_local,
            forward_mixed_rows,
            forward_attended,
            forward_log_total,
            forward_middle,
            forward_second,
            forward_expanded,
            forward_active,
        )
        output_now = output.reshape(group_size, stretch_len, model_width).astype(jnp.bfloat16)
        kept_values = forward_kept_values
        backward_weights = fetch_weights(local_parts)
        input_now, small_terms, factor_pairs = backward_micro(
            backward_weights, kept_values, micro_index
        )
        output_list.append(output_now)
        input_list.append(input_now)
        factor_list.append(factor_pairs)
        if small_totals is None:
            small_totals = small_terms
        else:
            small_totals = tuple(
                (total_now + term_now for total_now, term_now in zip(small_totals, small_terms))
            )

    def joined(position):
        return jnp.concatenate([pairs_now[position] for pairs_now in factor_list], axis=0)

    matrices = (
        outer_sum(joined(0), joined(1)),
        outer_sum(joined(2), joined(3)),
        outer_sum(joined(4), joined(5)),
        outer_sum(joined(6), joined(7)),
    )
    reduced = reduce_gradients(matrices, small_totals)
    block_output = jnp.concatenate(output_list, axis=0)
    input_gradient = jnp.concatenate(input_list, axis=0)
    return (
        block_output,
        input_gradient,
        reduced[4],
        reduced[5],
        reduced[0],
        reduced[6],
        reduced[7],
        reduced[1],
        reduced[8],
        reduced[9],
        reduced[10],
        reduced[2],
        reduced[11],
        reduced[3],
        reduced[12],
    )


def joint_split(rows, parts, heads_each):
    count, three, width = rows.shape
    span = heads_each * HEAD
    slots = slot_width(heads_each)
    rows = jnp.pad(rows, ((0, 0), (0, 0), (0, parts * span - width)))
    rows = rows.reshape(count, three, parts, span)
    rows = jnp.pad(rows, ((0, 0), (0, 0), (0, 0), (0, slots - span)))
    return rows.transpose(2, 0, 1, 3).reshape(parts, count, three * slots)


def joint_join(pieces, heads_each, width):
    parts, count, wide = pieces.shape
    span = heads_each * HEAD
    rows = pieces.reshape(parts, count, 3, wide // 3)[..., :span]
    rows = rows.transpose(1, 2, 0, 3).reshape(count, 3, parts * span)
    return rows[..., :width].reshape(count, 3 * width)


def slot_width(heads_each):
    return -(-heads_each * HEAD // LANES) * LANES


def causal(k_block_is_diagonal, same):
    if k_block_is_diagonal:
        same = same & (
            lax.broadcasted_iota(jnp.int32, (TILE, TILE), 0)
            <= lax.broadcasted_iota(jnp.int32, (TILE, TILE), 1)
        )
    return same


def attend_forward_kernel(nf, nc, heads, guests, *refs):
    n_in = sum(g[2] for g in guests)
    n_out = sum(g[3] for g in guests)
    own, ins, results, outs, own_scratch, scratch = split_refs(
        refs, (3, n_in, 3, n_out, 7, len(refs) - n_in - n_out - 13)
    )
    seg_row, seg_col, qkv_ref = own
    out_ref, turned_ref, lse_ref = results
    q_low, q_high, keys, values_turned, acc, tops, sums = own_scratch
    made = hosted(nf, nc, guests, ins, outs, scratch)
    greet_all(nc, {needs_of(g) for g in guests})
    begin_guests(made)
    send_guests(made)
    slots = out_ref.shape[1]
    scale = HEAD ** (-0.5)
    halves = (q_low, q_high)

    def one_block(q_block, k_block, first, count):
        q_at = pl.ds(pl.multiple_of(q_block * TILE, TILE), TILE)
        k_at = pl.ds(pl.multiple_of(k_block * TILE, TILE), TILE)
        same = causal(first, seg_col[k_at, :] == seg_row[:, q_at])
        for half in range(count):
            dims = pl.ds(half * HEAD, HEAD)
            scores = times_transposed(keys[k_at, :], halves[half][q_at, :])
            scores = jnp.where(same, scores, masked_score)
            top = jnp.max(scores, axis=0, keepdims=True)
            if not first:
                old_top = tops[half]
                top = jnp.maximum(old_top, top)
            weights = jnp.exp(scores - top)
            total = jnp.sum(weights, axis=0, keepdims=True)
            part = jnp.dot(
                values_turned[dims, k_at],
                weights.astype(jnp.bfloat16),
                preferred_element_type=jnp.float32,
            )
            if not first:
                fade = jnp.exp(old_top - top)
                total = total + sums[half] * fade
                part = part + acc[dims, :] * fade
            tops[half] = top
            sums[half] = total
            acc[dims, :] = part

    def one_pair(pair, count):
        column = pl.multiple_of(pair * LANES, LANES)
        queries = qkv_ref[:, pl.ds(column, LANES)] * jnp.bfloat16(scale)
        low_half = lax.broadcasted_iota(jnp.int32, queries.shape, 1) < HEAD
        q_low[...] = jnp.where(low_half, queries, jnp.zeros_like(queries))
        q_high[...] = jnp.where(low_half, jnp.zeros_like(queries), queries)
        keys[...] = qkv_ref[:, pl.ds(slots + column, LANES)]
        values = qkv_ref[:, pl.ds(2 * slots + column, LANES)]
        values_turned[...] = values.astype(jnp.float32).T.astype(jnp.bfloat16)

        @pl.loop(0, qkv_ref.shape[0] // TILE)
        def _(q_block):
            one_block(q_block, q_block, True, count)

            @pl.loop(0, q_block)
            def _(k_block):
                one_block(q_block, k_block, False, count)

            q_at = pl.ds(pl.multiple_of(q_block * TILE, TILE), TILE)
            if count == 1:
                acc[HEAD:, :] = jnp.zeros((LANES - HEAD, TILE), jnp.float32)
                lse_ref[pair, pl.ds(1, 1), q_at] = jnp.zeros((1, TILE), jnp.float32)
            for half in range(count):
                dims = pl.ds(half * HEAD, HEAD)
                acc[dims, :] = acc[dims, :] / sums[half]
                lse_ref[pair, pl.ds(half, 1), q_at] = tops[half] + jnp.log(sums[half])
            turned_ref[pair, :, q_at] = acc[...]
            out_ref[q_at, pl.ds(column, LANES)] = acc[...].T.astype(jnp.bfloat16)

    @pl.loop(0, heads // 2)
    def _(pair):
        one_pair(pair, 2)

        @pl.when(pair == 2)
        def _():
            pass_on_guests(made)

    if heads % 2:
        one_pair(heads // 2, 1)
    run_guests(made)


def attend_backward_kernel(nf, nc, heads, guests, *refs):
    n_in = sum(g[2] for g in guests)
    n_out = sum(g[3] for g in guests)
    own, ins, results, outs, own_scratch, scratch = split_refs(
        refs, (7, n_in, 1, n_out, 11, len(refs) - n_in - n_out - 19)
    )
    seg_row, seg_col, qkv_ref, grad_ref, turned_ref, lse_ref, order_ref = own
    out_ref = results[0]
    (
        q_low, q_high, keys, keys_turned, values, g_low, g_high,
        query_acc, key_acc, value_acc, corrections,
    ) = own_scratch
    made = hosted(nf, nc, guests, ins, outs, scratch)
    greet_all(nc, {needs_of(g) for g in guests})
    begin_guests(made)
    slots = grad_ref.shape[2]
    scale = HEAD ** (-0.5)
    q_halves = (q_low, q_high)
    g_halves = (g_low, g_high)

    def one_block(pair, q_block, k_block, first, count):
        q_at = pl.ds(pl.multiple_of(q_block * TILE, TILE), TILE)
        k_at = pl.ds(pl.multiple_of(k_block * TILE, TILE), TILE)
        same = causal(first, seg_col[k_at, :] == seg_row[:, q_at])
        value_sum = value_acc[k_at, :]
        key_sum = key_acc[k_at, :]
        for half in range(count):
            dims = pl.ds(half * HEAD, HEAD)
            query_rows = q_halves[half][q_at, :]
            grad_rows = g_halves[half][q_at, :]
            scores = times_transposed(keys[k_at, :], query_rows)
            lse = lse_ref[pair, pl.ds(half, 1), q_at]
            probs = jnp.exp(jnp.where(same, scores - lse, masked_score))
            dots = times_transposed(values[k_at, :], grad_rows)
            delta = (probs * (dots - corrections[half, :, q_at])).astype(jnp.bfloat16)
            value_sum = value_sum + jnp.dot(
                probs.astype(jnp.bfloat16), grad_rows, preferred_element_type=jnp.float32
            )
            key_sum = key_sum + jnp.dot(delta, query_rows, preferred_element_type=jnp.float32)
            part = jnp.dot(keys_turned[dims, k_at], delta, preferred_element_type=jnp.float32)
            if first:
                query_acc[dims, :] = part
            else:
                query_acc[dims, :] += part
        value_acc[k_at, :] = value_sum
        key_acc[k_at, :] = key_sum

    def one_pair(pair, count):
        column = pl.multiple_of(pair * LANES, LANES)
        queries = qkv_ref[:, pl.ds(column, LANES)] * jnp.bfloat16(scale)
        low_half = lax.broadcasted_iota(jnp.int32, queries.shape, 1) < HEAD
        zeros = jnp.zeros_like(queries)
        q_low[...] = jnp.where(low_half, queries, zeros)
        q_high[...] = jnp.where(low_half, zeros, queries)
        grads = jnp.concatenate(
            [grad_ref[order_ref[k], :, pl.ds(column, LANES)] for k in range(grad_ref.shape[0])]
        )
        g_low[...] = jnp.where(low_half, grads, zeros)
        g_high[...] = jnp.where(low_half, zeros, grads)
        product = grads.astype(jnp.float32).T * turned_ref[pair]
        corrections[0] = jnp.sum(product[:HEAD], axis=0, keepdims=True)
        corrections[1] = jnp.sum(product[HEAD:], axis=0, keepdims=True)
        keys_now = qkv_ref[:, pl.ds(slots + column, LANES)]
        keys[...] = keys_now
        keys_turned[...] = keys_now.astype(jnp.float32).T.astype(jnp.bfloat16)
        values[...] = qkv_ref[:, pl.ds(2 * slots + column, LANES)]
        key_acc[...] = jnp.zeros_like(key_acc)
        value_acc[...] = jnp.zeros_like(value_acc)
        if count == 1:
            query_acc[HEAD:, :] = jnp.zeros((LANES - HEAD, TILE), jnp.float32)

        @pl.loop(0, qkv_ref.shape[0] // TILE)
        def _(q_block):
            one_block(pair, q_block, q_block, True, count)

            @pl.loop(0, q_block)
            def _(k_block):
                one_block(pair, q_block, k_block, False, count)

            q_at = pl.ds(pl.multiple_of(q_block * TILE, TILE), TILE)
            out_ref[q_at, pl.ds(column, LANES)] = (query_acc[...].T * scale).astype(jnp.bfloat16)

        out_ref[:, pl.ds(slots + column, LANES)] = key_acc[...].astype(jnp.bfloat16)
        out_ref[:, pl.ds(2 * slots + column, LANES)] = value_acc[...].astype(jnp.bfloat16)

    @pl.loop(0, heads // 2)
    def _(pair):
        one_pair(pair, 2)

        @pl.when(pair == 0)
        def _():
            send_guests(made)

    if heads % 2:
        one_pair(heads // 2, 1)
    run_guests(made)


def pick(blocks, order):
    return blocks.at[order].get(mode="promise_in_bounds", unique_indices=True)


def all_units(vector, nc, nf, unit_each, shard):
    vector = vector.transpose(1, 0, 2).reshape(nc, nf, unit_each)
    return lax.dynamic_index_in_dim(vector, shard, 1, keepdims=False).reshape(nc * unit_each)


def rows_of(vectors, count):
    row = jnp.arange(count, dtype=jnp.int32)[:, None]
    total = jnp.where(row == 0, vectors[0][None], jnp.zeros_like(vectors[0][None]))
    for k, vector in enumerate(vectors[1:], 1):
        total = jnp.where(row == k, vector[None], total)
    return total


def normalize(rows):
    center = rows - jnp.mean(rows, axis=-1, keepdims=True)
    spread = jnp.mean(center * center, axis=-1, keepdims=True)
    inverse = lax.rsqrt(spread + epsilon)
    return center * inverse, inverse


def normalize_back(grads, gain, unit, inverse):
    pulled = grads * gain
    return inverse * (
        pulled
        - jnp.mean(pulled, axis=-1, keepdims=True)
        - unit * jnp.mean(pulled * unit, axis=-1, keepdims=True)
    )


def gelu_parts(value):
    root = 0.7978845608028654
    inner = root * (value + 0.044715 * value * value * value)
    bend = jnp.tanh(inner)
    slope = 0.5 * (1.0 + bend) + 0.5 * value * (1.0 - bend * bend) * root * (
        1.0 + 3 * 0.044715 * value * value
    )
    return 0.5 * value * (1.0 + bend), slope


def mesh_copy(source, target, send, receive, device):
    return pltpu.make_async_remote_copy(
        src_ref=source,
        dst_ref=target,
        send_sem=send,
        recv_sem=receive,
        device_id=device,
        device_id_type=pl.DeviceIdType.MESH,
    )


def greet(devices, swaps=()):
    barrier = pltpu.get_barrier_semaphore()
    for device in devices:
        pl.semaphore_signal(
            barrier, inc=1, device_id=device, device_id_type=pl.DeviceIdType.MESH
        )
    for device in swaps:

        @pl.when(elsewhere(device))
        def _():
            pl.semaphore_signal(
                barrier, inc=1, device_id=device, device_id_type=pl.DeviceIdType.MESH
            )

    count = len(devices)
    for device in swaps:
        count = count + jnp.where(elsewhere(device), 1, 0)
    pl.semaphore_wait(barrier, count)


def elsewhere(device):
    apart = (device[0] - lax.axis_index("fsdp")) * 64 + device[1] - lax.axis_index("ctx")
    return apart != 0


def to_column(f, c, i):
    return 2 * (c // 2 % 2) + c % 2, 2 * (2 * i + f % 2) + (f // 2 + f % 2) % 2, c // 4


def to_origin(f, c, j):
    core = c // 2 % 2
    return 2 * ((c % 2 + core) % 2) + core, 2 * (2 * j + f // 2) + f % 2, c // 4


def swap_peers(move, back):
    f, c = lax.axis_index("fsdp"), lax.axis_index("ctx")
    return [way(f, c, k)[:2] for way in (move, back) for k in range(2)]


def ctx_peers(nc):
    f, c = lax.axis_index("fsdp"), lax.axis_index("ctx")
    return [(f, (c + k) % nc) for k in range(1, nc)]


def greet_all(nc, needs):
    devices, swaps = [], []
    if "fsdp" in needs:
        devices += fsdp_peers(3)
    elif "near" in needs:
        devices += fsdp_peers(2)
    if "ctx" in needs:
        devices += ctx_peers(nc)
    elif "ring" in needs:
        devices += ring_peers(nc)
    if "column" in needs:
        swaps += swap_peers(to_column, to_origin)
    if "origin" in needs:
        swaps += swap_peers(to_origin, to_column)
    greet(devices, swaps)


def fsdp_places():
    shard = lax.axis_index("fsdp")
    partner = shard + 1 - 2 * (shard % 2)
    return shard, partner, (shard + 2) % 4, (partner + 2) % 4


def ring_places(nc):
    place = lax.axis_index("ctx")
    z, y = place // 2, place % 2
    spot = z * (1 - y) + (nc - 1 - z) * y

    def holder(at):
        at = (at + nc) % nc
        side = at // (nc // 2)
        return (1 - side) * 2 * at + side * (2 * (nc - 1 - at) + 1)

    return spot, holder


def ring_peers(nc):
    spot, holder = ring_places(nc)
    shard = lax.axis_index("fsdp")
    return [(shard, holder(spot + way)) for way in (1, -1)]


def fsdp_peers(count):
    place = lax.axis_index("ctx")
    return [(at, place) for at in fsdp_places()[1 : 1 + count]]


def chunks_of(rows, count):
    step = -(-rows // count // 16) * 16
    return [(at, min(step, rows - at)) for at in range(0, rows, step)]


def row_step(size):
    return next(step for step in (56, 40, 32, 16, 8) if size % step == 0)


class FsdpGather:
    SEMS = (7, 4)

    def __init__(self, own, out, sems):
        self.own, self.out, self.sems = own, out, sems
        self.shard, self.partner, self.cross, self.corner = fsdp_places()
        self.place = lax.axis_index("ctx")
        self.chunks = chunks_of(own.shape[0], 4)

    def copy(self, kind, k):
        at, size = self.chunks[k]
        rows = pl.ds(at, size)
        if kind == "own":
            return pltpu.make_async_copy(
                self.own.at[rows], self.out.at[self.shard, rows], self.sems.at[6, k]
            )
        if kind == "across":
            source, slot, device, sem = self.own.at[rows], self.shard, self.cross, 0
        elif kind == "beside":
            source, slot, device, sem = self.own.at[rows], self.shard, self.partner, 2
        else:
            slot, device, sem = self.cross, self.partner, 4
            source = self.out.at[slot, rows]
        return mesh_copy(
            source,
            self.out.at[slot, rows],
            self.sems.at[sem, k],
            self.sems.at[sem + 1, k],
            (device, self.place),
        )

    def begin(self):
        for kind in ("across", "beside", "own"):
            for k in range(len(self.chunks)):
                self.copy(kind, k).start()

    def pass_on(self):
        for k in range(len(self.chunks)):
            self.copy("across", k).wait_recv()
            self.copy("on", k).start()

    def finish(self):
        for k in range(len(self.chunks)):
            self.copy("across", k).wait_send()
            self.copy("beside", k).wait()
            self.copy("on", k).wait()
            self.copy("own", k).wait()


def joint_parts(nf, nc, rows, depth, place):
    thin = depth // nf // (8 * nc) * 8
    rest, each = rows - nf * thin, nc // nf
    parts = []
    for f in range(nf):
        parts.append((f * thin, pl.multiple_of(f * (depth // nf) + place * thin, 8), thin))
    last = (place // each) * (depth // nf) + nc * thin + (place % each) * rest
    parts.append((nf * thin, pl.multiple_of(last, 8), rest))
    return parts


def half_of(parts, way):
    middle = (len(parts) - 1) // 2
    return parts[:middle] if way == 1 else parts[middle:]


class RingGather:
    def __init__(self, nc, own, out, sems, parts=None):
        self.nc, self.own, self.out, self.sems = nc, own, out, sems
        self.spot, self.holder = ring_places(nc)
        self.shard = lax.axis_index("fsdp")
        self.parts = parts
        if parts is None:
            self.rows = out.shape[1]
            self.half = self.rows // 2 // 8 * 8

    def pieces(self, origin, way, step):
        if self.parts is not None:
            parts = self.parts(origin)
            if step == self.nc // 2:
                parts = half_of(parts, way)
            return [(pl.ds(at, size), self.out.at[pl.ds(there, size)]) for at, there, size in parts]
        rows = pl.ds(0, self.rows)
        if step == self.nc // 2:
            rows = pl.ds(0, self.half) if way == 1 else pl.ds(self.half, self.rows - self.half)
        return [(rows, self.out.at[origin, rows])]

    def copies(self, way, step):
        origin = self.holder(self.spot - way * (step - 1))
        side = 0 if way == 1 else 2
        made = []
        for k, (rows, whole) in enumerate(self.pieces(origin, way, step)):
            made.append(
                mesh_copy(
                    self.own.at[rows] if step == 1 else whole,
                    whole,
                    self.sems.at[side, step - 1, k],
                    self.sems.at[side + 1, step - 1, k],
                    (self.shard, self.holder(self.spot + way)),
                )
            )
        return made

    def keeps(self):
        return [
            pltpu.make_async_copy(self.own.at[rows], whole, self.sems.at[4, 0, k])
            for k, (rows, whole) in enumerate(self.pieces(lax.axis_index("ctx"), 1, 1))
        ]

    def start(self, step):
        for way in (1, -1):
            for copy in self.copies(way, step):
                copy.start()
        if step == 1:
            for copy in self.keeps():
                copy.start()

    def arrived(self, way, step):
        for copy in self.copies(way, step):
            copy.wait_recv()

    def advance(self, step):
        for way in (1, -1):
            self.arrived(way, step - 1)
            for copy in self.copies(way, step):
                copy.start()

    def finish(self, first, last):
        for way in (1, -1):
            for step in range(first, last + 1):
                for copy in self.copies(way, step):
                    copy.wait_send()
            self.arrived(way, last)
        if first == 1:
            for copy in self.keeps():
                copy.wait()


class RingScatter:
    def __init__(self, nc, mine, out, right, left, sems, parts=None):
        self.nc, self.mine, self.out, self.sems = nc, mine, out, sems
        self.inbox = {1: right, -1: left}
        self.spot, self.holder = ring_places(nc)
        self.shard = lax.axis_index("fsdp")
        self.rows = out.shape[0]
        self.half = self.rows // 2 // 8 * 8
        self.parts = parts

    def copies(self, way, step):
        inbox = self.inbox[way]
        if step > 1:
            sources = [(pl.ds(0, self.rows), inbox.at[step - 2])]
        else:
            place = self.holder(self.spot + self.nc // 2)
            if self.parts is not None:
                sources = [
                    (pl.ds(at, size), self.mine.at[pl.ds(there, size)])
                    for at, there, size in half_of(self.parts(place), way)
                ]
            else:
                low, high = pl.ds(0, self.half), pl.ds(self.half, self.rows - self.half)
                rows = low if way == 1 else high
                sources = [(rows, self.mine.at[place, rows])]
        side = 0 if way == 1 else 2
        return [
            mesh_copy(
                source,
                inbox.at[step - 1, rows],
                self.sems.at[side, step - 1, k],
                self.sems.at[side + 1, step - 1, k],
                (self.shard, self.holder(self.spot + way)),
            )
            for k, (rows, source) in enumerate(sources)
        ]

    def begin(self):
        for way in (1, -1):
            for copy in self.copies(way, 1):
                copy.start()

    def advance(self, step):
        for way in (1, -1):
            for copy in self.copies(way, step - 1):
                copy.wait_recv()
            box = self.inbox[way].at[step - 2]
            place = self.holder(self.spot + way * (self.nc // 2 + 1 - step))
            if self.parts is not None:
                parts = self.parts(place)
                came = half_of(parts, way) if step == 2 else parts
                for part in parts:
                    at, there, size = part
                    target, source = box.at[pl.ds(at, size)], self.mine.at[pl.ds(there, size)]
                    if any(part is other for other in came):
                        add_rows(target, source, (0, size))
                    else:
                        set_rows(target, source, (0, size))
            else:
                join_rows(box, self.mine.at[place], step, way, self.rows, self.half)
            for copy in self.copies(way, step):
                copy.start()

    def finish(self):
        last = self.nc // 2
        for way in (1, -1):
            for copy in self.copies(way, last):
                copy.wait_recv()
        right, left = self.inbox[1].at[last - 1], self.inbox[-1].at[last - 1]
        place = lax.axis_index("ctx")
        if self.parts is not None:
            for at, there, size in self.parts(place):
                rows = pl.ds(at, size)
                sum_rows(
                    self.out.at[rows], self.mine.at[pl.ds(there, size)], right.at[rows], left.at[rows]
                )
        else:
            sum_rows(self.out, self.mine.at[place], right, left)
        for way in (1, -1):
            for step in range(1, last + 1):
                for copy in self.copies(way, step):
                    copy.wait_send()


def join_rows(box, mine, step, way, rows, half):
    low, high = (0, half), (half, rows - half)
    if step == 2:
        got, rest = (low, high) if way == 1 else (high, low)
        set_rows(box, mine, rest)
    else:
        got = (0, rows)
    add_rows(box, mine, got)


def add_rows(target, source, rows):
    first, size = rows
    step = row_step(size)

    @pl.loop(0, size // step)
    def _(turn):
        at = pl.ds(pl.multiple_of(first + turn * step, 8), step)
        target[at] = (target[at].astype(jnp.float32) + source[at].astype(jnp.float32)).astype(
            target.dtype
        )


def set_rows(target, source, rows):
    first, size = rows
    step = row_step(size)

    @pl.loop(0, size // step)
    def _(turn):
        at = pl.ds(pl.multiple_of(first + turn * step, 8), step)
        target[at] = source[at]


def sum_rows(out, mine, right, left):
    step = row_step(out.shape[0])

    @pl.loop(0, out.shape[0] // step)
    def _(turn):
        at = pl.ds(pl.multiple_of(turn * step, 8), step)
        out[at] = (
            mine[at].astype(jnp.float32)
            + right[at].astype(jnp.float32)
            + left[at].astype(jnp.float32)
        ).astype(out.dtype)


class GatherStep:
    NEEDS = "ring"
    VMEM_IN = 0

    def __init__(self, nf, nc, step, ins, outs, scratch):
        self.step = step
        self.ring = RingGather(nc, None, outs[0], scratch[0])

    @staticmethod
    def shapes(nf, nc, step, arrays):
        (whole,) = arrays
        return (
            [jax.ShapeDtypeStruct(whole.shape, whole.dtype)],
            [pltpu.SemaphoreType.DMA((5, nc // 2, 1))],
            True,
        )

    def begin(self):
        self.ring.start(self.step)

    def send(self):
        pass

    def finish(self):
        self.ring.finish(self.step, self.step)


class SideGather:
    NEEDS = "near"
    VMEM_IN = 1

    def __init__(self, nf, nc, step, ins, outs, scratch):
        self.side = FsdpGather(ins[0], outs[0], scratch[0])

    @staticmethod
    def shapes(nf, nc, step, arrays):
        (array,) = arrays
        return (
            [jax.ShapeDtypeStruct((nf,) + array.shape, array.dtype)],
            [pltpu.SemaphoreType.DMA(FsdpGather.SEMS)],
            False,
        )

    def begin(self):
        pass

    def send(self):
        self.side.begin()

    def finish(self):
        self.side.finish()


class ScatterRing:
    NEEDS = "ring"
    VMEM_IN = 1

    def __init__(self, nf, nc, step, ins, outs, scratch):
        right, left, total, self.put_sem, sems = scratch
        self.out, self.total = outs[0], total
        parts = None
        if step:
            parts = functools.partial(joint_parts, nf, nc, step, ins[0].shape[0])
        self.ring = RingScatter(nc, ins[0], total, right, left, sems, parts)

    @staticmethod
    def shapes(nf, nc, step, arrays):
        mine = arrays[0]
        shape = (step,) + mine.shape[1:] if step else mine.shape[1:]
        box = pltpu.VMEM((nc // 2,) + shape, mine.dtype)
        return (
            [jax.ShapeDtypeStruct(shape, mine.dtype)],
            [
                box,
                box,
                pltpu.VMEM(shape, mine.dtype),
                pltpu.SemaphoreType.DMA((1,)),
                pltpu.SemaphoreType.DMA((4, nc // 2, nf + 1)),
            ],
            False,
        )

    def begin(self):
        self.ring.begin()

    def send(self):
        self.ring.advance(2)

    def more(self, step):
        self.ring.advance(step)

    def finish(self):
        self.ring.finish()
        put = pltpu.make_async_copy(self.total, self.out, self.put_sem.at[0])
        put.start()
        put.wait()


class ScatterStep:
    NEEDS = "ring"
    VMEM_IN = 0

    def __init__(self, nf, nc, step, ins, outs, scratch):
        self.nc, self.step = nc, step
        self.mine, self.before, self.outs = ins[0], ins[1:], outs
        self.sems = scratch[-1]
        self.boxes = scratch[:-1]
        self.spot, self.holder = ring_places(nc)
        self.shard = lax.axis_index("fsdp")
        self.rows = outs[0].shape[0]
        self.half = self.rows // 2 // 8 * 8

    @staticmethod
    def shapes(nf, nc, step, arrays):
        mine = arrays[0]
        block = jax.ShapeDtypeStruct(mine.shape[1:], mine.dtype)
        outs = [block, block]
        scratch = []
        if step > 1:
            scratch += [pltpu.VMEM(mine.shape[1:], mine.dtype)] * 4
        return outs, scratch + [pltpu.SemaphoreType.DMA((4, 4))], False

    def copy(self, k):
        way = (1, -1)[k]
        rows = pl.ds(0, self.rows)
        if self.step == 1:
            rows = pl.ds(0, self.half) if way == 1 else pl.ds(self.half, self.rows - self.half)
            source = self.mine.at[self.holder(self.spot + self.nc // 2), rows]
        else:
            source = self.boxes[k]
        return mesh_copy(
            source,
            self.outs[k].at[rows],
            self.sems.at[0, k],
            self.sems.at[1, k],
            (self.shard, self.holder(self.spot + way)),
        )

    def loads(self, k):
        way = (1, -1)[k]
        rows = pl.ds(0, self.rows)
        if self.step == 2:
            rows = pl.ds(0, self.half) if way == 1 else pl.ds(self.half, self.rows - self.half)
        place = self.holder(self.spot + way * (self.nc // 2 + 1 - self.step))
        return [
            pltpu.make_async_copy(
                self.before[k].at[rows], self.boxes[k].at[rows], self.sems.at[2, k]
            ),
            pltpu.make_async_copy(self.mine.at[place], self.boxes[2 + k], self.sems.at[3, k]),
        ]

    def begin(self):
        for k in range(2):
            if self.step == 1:
                self.copy(k).start()
            else:
                for load in self.loads(k):
                    load.start()

    def send(self):
        if self.step > 1:
            for k in range(2):
                for load in self.loads(k):
                    load.wait()
                way = (1, -1)[k]
                join_rows(self.boxes[k], self.boxes[2 + k], self.step, way, self.rows, self.half)
                self.copy(k).start()

    def finish(self):
        for k in range(2):
            self.copy(k).wait()


class Trade:
    def __init__(self, axis, size, source, target, sems, hops=None):
        self.axis, self.size = axis, size
        self.hops = hops or tuple(range(1, size))
        self.source, self.target, self.sems = source, target, sems
        self.me = lax.axis_index(axis)

    def copies(self):
        made = []
        for k in self.hops:
            other = (self.me + k) % self.size
            device = (
                (other, lax.axis_index("ctx"))
                if self.axis == "fsdp"
                else (lax.axis_index("fsdp"), other)
            )
            made.append(
                mesh_copy(
                    self.source(other),
                    self.target(self.me),
                    self.sems.at[0, k],
                    self.sems.at[1, k],
                    device,
                )
            )
        made.append(
            pltpu.make_async_copy(
                self.source(self.me), self.target(self.me), self.sems.at[2, 0]
            )
        )
        return made

    def begin(self):
        for copy in self.copies():
            copy.start()

    def finish(self):
        for copy in self.copies():
            copy.wait()


class TradeGuest:
    VMEM_IN = 1

    def __init__(self, nf, nc, step, ins, outs, scratch):
        axis, hops = step
        size = nf if axis == "fsdp" else nc
        whole = len(ins[0].shape) < len(outs[0].shape)
        self.trade = Trade(
            axis,
            size,
            (lambda k: ins[0]) if whole else (lambda k: ins[0].at[k]),
            lambda k: outs[0].at[k],
            scratch[0],
            hops,
        )

    @staticmethod
    def shapes(nf, nc, step, arrays):
        (array,) = arrays
        size = nf if step[0] == "fsdp" else nc
        shape = array.shape if array.ndim == 3 else (size,) + array.shape
        return (
            [jax.ShapeDtypeStruct(shape, array.dtype)],
            [pltpu.SemaphoreType.DMA((3, size))],
            False,
        )

    def begin(self):
        pass

    def send(self):
        self.trade.begin()

    def finish(self):
        self.trade.finish()


def window(part, parts, width):
    size = max(
        -(-(k + 1) * (width // parts) // LANES) * LANES - k * (width // parts) // LANES * LANES
        for k in range(parts)
    )
    return part * (width // parts) // LANES * LANES, size


class WindowTrade:
    VMEM_IN = 1

    def __init__(self, nf, nc, step, ins, outs, scratch):
        def source(k):
            start, size = window(k, nf, step)
            return ins[0].at[:, pl.ds(pl.multiple_of(start, LANES), size)]

        self.trade = Trade("fsdp", nf, source, lambda k: outs[0].at[k], scratch[0])

    @staticmethod
    def shapes(nf, nc, step, arrays):
        (array,) = arrays
        shape = (nf, array.shape[0], window(0, nf, step)[1])
        return (
            [jax.ShapeDtypeStruct(shape, array.dtype)],
            [pltpu.SemaphoreType.DMA((3, nf))],
            False,
        )

    def begin(self):
        pass

    def send(self):
        self.trade.begin()

    def finish(self):
        self.trade.finish()


class SwapGuest:
    VMEM_IN = 1

    def __init__(self, nf, nc, step, ins, outs, scratch):
        self.blocks, self.out, self.sems = ins[0], outs[0], scratch[0]
        self.move, self.back = (
            (to_column, to_origin) if step == "column" else (to_origin, to_column)
        )

    @staticmethod
    def shapes(nf, nc, step, arrays):
        (array,) = arrays
        return (
            [jax.ShapeDtypeStruct(array.shape, array.dtype)],
            [pltpu.SemaphoreType.DMA((3, 2))],
            False,
        )

    def copies(self, k):
        f, c = lax.axis_index("fsdp"), lax.axis_index("ctx")
        there = self.move(f, c, k)
        source, target = self.blocks.at[k], self.out.at[there[2]]
        away = mesh_copy(
            source, target, self.sems.at[0, k], self.sems.at[1, there[2]], there[:2]
        )
        return elsewhere(there), away, pltpu.make_async_copy(source, target, self.sems.at[2, k])

    def begin(self):
        pass

    def send(self):
        for k in range(2):
            apart, away, stay = self.copies(k)

            @pl.when(apart)
            def _():
                away.start()

            @pl.when(jnp.logical_not(apart))
            def _():
                stay.start()

    def finish(self):
        f, c = lax.axis_index("fsdp"), lax.axis_index("ctx")
        for k in range(2):
            apart, away, stay = self.copies(k)

            @pl.when(apart)
            def _():
                away.wait_send()

            @pl.when(jnp.logical_not(apart))
            def _():
                stay.wait()

            origin = self.back(f, c, k)
            arrival = mesh_copy(
                self.blocks.at[0],
                self.out.at[k],
                self.sems.at[0, 0],
                self.sems.at[1, k],
                origin[:2],
            )

            @pl.when(elsewhere(origin))
            def _():
                arrival.wait_recv()


def begin_guests(made):
    for guest in made:
        guest.begin()
    early_guests(made)


def early_guests(made):
    for guest in made:
        if isinstance(guest, ScatterStep):
            guest.send()


def send_guests(made):
    for guest in made:
        if not isinstance(guest, ScatterStep):
            guest.send()


def pass_on_guests(made):
    for guest in made:
        if isinstance(guest, SideGather):
            guest.side.pass_on()


def needs_of(guest):
    kind, step = guest[0], guest[1]
    if kind is TradeGuest:
        return step[0]
    if kind is WindowTrade:
        return "fsdp"
    if kind is SwapGuest:
        return step
    return kind.NEEDS


def split_refs(refs, counts):
    parts, at = [], 0
    for count in counts:
        parts.append(refs[at : at + count])
        at += count
    return parts


def hosted(nf, nc, guests, ins, outs, scratch):
    made, a, b, c = [], 0, 0, 0
    for kind, step, n_in, n_out, n_scratch in guests:
        made.append(
            kind(nf, nc, step, ins[a : a + n_in], outs[b : b + n_out], scratch[c : c + n_scratch])
        )
        a, b, c = a + n_in, b + n_out, c + n_scratch
    return made


def run_guests(made):
    for step in (3, 4):
        for guest in made:
            if isinstance(guest, ScatterRing):
                guest.more(step)
    for guest in made:
        guest.finish()


def lone_kernel(nf, nc, guests, *refs):
    n_in = sum(g[2] for g in guests)
    n_out = sum(g[3] for g in guests)
    ins, outs, scratch = split_refs(refs, (n_in, n_out, len(refs) - n_in - n_out))
    made = hosted(nf, nc, guests, ins, outs, scratch)
    greet_all(nc, {needs_of(g) for g in guests})
    begin_guests(made)
    send_guests(made)
    run_guests(made)


def gather_fsdp_kernel(nf, nc, guests, *refs):
    n_in = sum(g[2] for g in guests)
    n_out = sum(g[3] for g in guests)
    own, ins, out, outs, sems, scratch = split_refs(
        refs, (1, n_in, 1, n_out, 1, len(refs) - n_in - n_out - 3)
    )
    side = FsdpGather(own[0], out[0], sems[0])
    made = hosted(nf, nc, guests, ins, outs, scratch)
    greet_all(nc, {"near"} | {needs_of(g) for g in guests})
    side.begin()
    begin_guests(made)
    send_guests(made)
    side.pass_on()
    side.finish()
    run_guests(made)


def scatter_fsdp_kernel(nf, nc, guests, turned, ordered, *refs):
    n_in = sum(g[2] for g in guests)
    n_out = sum(g[3] for g in guests)
    count_own = 3 if ordered else 2
    operands, ins, result, outs, own_scratch, scratch = split_refs(
        refs, (count_own, n_in, 1, n_out, 6, len(refs) - n_in - n_out - 7 - count_own)
    )
    left_ref, right_ref = operands[:2]
    out_ref = result[0]
    part_ref, first_in, own_in, chip_sum, across_in, sems = own_scratch
    shard, partner, cross, corner = fsdp_places()
    place = lax.axis_index("ctx")
    made = hosted(nf, nc, guests, ins, outs, scratch)
    greet_all(nc, {"near"} | {needs_of(g) for g in guests})
    for guest in made:
        guest.begin()
    count, width = out_ref.shape
    chunks = chunks_of(count, 4)

    def copy(kind, k):
        at, size = chunks[k]
        rows = pl.ds(at, size)
        if kind == 0:
            source, target, device = part_ref.at[corner, rows], first_in, partner
        elif kind == 1:
            source, target, device = part_ref.at[partner, rows], own_in, partner
        else:
            source, target, device = chip_sum.at[rows], across_in, cross
        return mesh_copy(
            source,
            target.at[rows],
            sems.at[2 * kind, k],
            sems.at[2 * kind + 1, k],
            (device, place),
        )

    half = count // 2
    early, late = chunks[: len(chunks) // 2], chunks[len(chunks) // 2 :]

    def add_and_send(first, some):
        for k, (at, size) in enumerate(some, first):
            copy(0, k).wait_recv()

            @pl.loop(0, size // 32)
            def _(step):
                rows = pl.ds(pl.multiple_of(at + step * 32, 32), 32)
                chip_sum[rows] = (
                    part_ref[cross, rows].astype(jnp.float32)
                    + first_in[rows].astype(jnp.float32)
                ).astype(chip_sum.dtype)

            copy(2, k).start()

    @pl.loop(0, 8)
    def _(turn):
        pair = turn // 4
        of_two = (turn % 2) * (1 - pair) + (turn // 2 % 2) * pair
        upper = (turn // 2 % 2) * (1 - pair) + (turn % 2) * pair
        base = partner * (1 - of_two) + shard * of_two
        block = (base + 2 * (1 - pair)) % 4
        start = pl.multiple_of(upper * half, half)
        if ordered:
            rows = left_ref[operands[2][block * 2 + upper]]
        else:
            rows = left_ref[block * 2 + upper]
        for at in range(0, width, 512):
            size = 512 if at + 1024 <= width else width - at
            if turned:
                piece = times_transposed(rows, right_ref[at : at + size, :])
            else:
                piece = jnp.dot(
                    rows, right_ref[:, at : at + size], preferred_element_type=jnp.float32
                )
            part_ref[block, pl.ds(start, half), at : at + size] = piece.astype(part_ref.dtype)
            if at + size == width:
                break

        @pl.when(turn == 0)
        def _():
            for k in range(len(early)):
                copy(0, k).start()
            early_guests(made)

        @pl.when(turn == 1)
        def _():
            add_and_send(0, early)

        @pl.when(turn == 2)
        def _():
            for k in range(len(early), len(chunks)):
                copy(0, k).start()

        @pl.when(turn == 3)
        def _():
            add_and_send(len(early), late)
            send_guests(made)

        @pl.when(turn == 5)
        def _():
            for k in range(len(chunks)):
                copy(1, k).start()

    for k, (at, size) in enumerate(chunks):
        copy(1, k).wait_recv()
        copy(2, k).wait_recv()

        @pl.loop(0, size // 32)
        def _(turn):
            rows = pl.ds(pl.multiple_of(at + turn * 32, 32), 32)
            out_ref[rows] = (
                part_ref[shard, rows].astype(jnp.float32)
                + own_in[rows].astype(jnp.float32)
                + across_in[rows].astype(jnp.float32)
            )

    for kind in range(3):
        for k in range(len(chunks)):
            copy(kind, k).wait_send()
    run_guests(made)


def startup_kernel(nf, nc, spans, row_count, *refs):
    ring_count = len(spans)
    total = ring_count + row_count
    ins, outs, sems, extra = split_refs(refs, (total, total, total, 3))
    block, trade_sems, give_sems = extra
    rest = ins[0].shape[1] * nf - block.shape[0]
    rest = rest // (nf - 1)
    thin = ins[0].shape[1] - rest
    trade = Trade(
        "fsdp",
        nf,
        lambda k: ins[0].at[k, pl.ds(0, thin)],
        lambda k: block.at[pl.ds(pl.multiple_of(k * thin, 8), thin)],
        trade_sems,
    )
    giver = lax.axis_index("ctx") // (nc // nf)
    shard = lax.axis_index("fsdp")

    def give(k):
        return mesh_copy(
            ins[0].at[(shard + k) % nf, pl.ds(thin, rest)],
            block.at[pl.ds(nf * thin, rest)],
            give_sems.at[0, k],
            give_sems.at[1, 0],
            ((shard + k) % nf, lax.axis_index("ctx")),
        )

    own_rest = pltpu.make_async_copy(
        ins[0].at[shard, pl.ds(thin, rest)],
        block.at[pl.ds(nf * thin, rest)],
        give_sems.at[0, 0],
    )
    parts = functools.partial(joint_parts, nf, nc, block.shape[0], outs[0].shape[0])
    rings = [
        RingGather(nc, block if k == 0 else ins[k], outs[k], sems[k], None if k else parts)
        for k in range(ring_count)
    ]
    sides = [FsdpGather(ins[k], outs[k], sems[k]) for k in range(ring_count, total)]
    greet(fsdp_peers(3) + ring_peers(nc))
    trade.begin()

    @pl.when(shard == giver)
    def _():
        own_rest.start()
        for k in range(1, nf):
            give(k).start()

    for ring in rings[1:]:
        ring.start(1)
    sides[0].begin()
    trade.finish()

    @pl.when(shard == giver)
    def _():
        own_rest.wait()
        for k in range(1, nf):
            give(k).wait_send()

    @pl.when(shard != giver)
    def _():
        give(1).wait_recv()

    rings[0].start(1)
    sides[0].pass_on()
    for side in sides[1:]:
        side.begin()
    for step in range(2, nc // 2 + 1):
        for ring, span in zip(rings, spans):
            if step <= span:
                ring.advance(step)
        if step == 2:
            for side in sides[1:]:
                side.pass_on()
    for side in sides:
        side.finish()
    for ring, span in zip(rings, spans):
        ring.finish(1, span)


def in_vmem():
    return pl.BlockSpec(memory_space=pltpu.VMEM)


def in_smem():
    return pl.BlockSpec(memory_space=pltpu.SMEM)


def in_place():
    return pl.BlockSpec(memory_space=pl.ANY)


def widen(pieces):
    return jnp.pad(pieces, ((0, 0),) * (pieces.ndim - 1) + ((0, -pieces.shape[-1] % LANES),))


class Net:
    def __init__(self, nf, nc):
        self.nf, self.nc = nf, nc
        self.each = nc // nf
        self.ids = {}

    def call(self, kernel, key, outs, ins, in_specs, out_specs, scratch, aliases=None):
        ident = self.ids.setdefault(key, len(self.ids))
        return pl.pallas_call(
            kernel,
            out_shape=outs,
            in_specs=in_specs,
            out_specs=out_specs,
            scratch_shapes=scratch,
            input_output_aliases=aliases or {},
            compiler_params=pltpu.CompilerParams(
                collective_id=ident, has_side_effects=True, vmem_limit_bytes=60 << 20
            ),
        )(*ins)

    def swap(self, blocks, move, back):
        place = lax.axis_index("ctx")
        got = []
        for turn in range(self.each):
            slot = (move(0, place, 0)[2] + turn) % self.each
            piece = lax.dynamic_index_in_dim(blocks, slot, 0, keepdims=False)
            pairs = []
            for f in range(self.nf):
                for c in range(self.nc):
                    there = move(f, c, (move(f, c, 0)[2] + turn) % self.each)
                    pairs.append((f * self.nc + c, there[0] * self.nc + there[1]))
            got.append(lax.ppermute(piece, ("fsdp", "ctx"), pairs))
        order = (back(0, place, 0)[2] - jnp.arange(self.each)) % self.each
        return pick(jnp.stack(got), order)

    def total(self, mine, right, left):
        own = lax.dynamic_index_in_dim(mine, lax.axis_index("ctx"), 0, keepdims=False)
        return sum(part.astype(jnp.float32) for part in (own, right, left)).astype(mine.dtype)

    def lone(self, name, hosted_steps):
        plan, ins, outs, scratch, aliases = self.guests(hosted_steps, 0, 0)
        return self.call(
            functools.partial(lone_kernel, self.nf, self.nc, plan),
            name,
            tuple(outs),
            ins,
            self.specs(hosted_steps),
            [in_place()] * len(outs),
            scratch,
            aliases,
        )

    def specs(self, hosted_steps):
        made = []
        for kind, _, arrays in hosted_steps:
            made += [in_vmem() if kind.VMEM_IN else in_place()] * len(arrays)
        return made

    def startup(self, pieces, block_rows, whole_rows, blocks, spans, rows):
        nf, nc = self.nf, self.nc
        first = (block_rows, pieces.shape[2])
        arrays = [pieces] + list(blocks) + list(rows)
        outs = [jax.ShapeDtypeStruct((whole_rows, pieces.shape[2]), pieces.dtype)]
        outs += [jax.ShapeDtypeStruct((nc,) + a.shape, a.dtype) for a in blocks]
        outs += [jax.ShapeDtypeStruct((nf,) + a.shape, a.dtype) for a in rows]
        scratch = [pltpu.SemaphoreType.DMA((5, nc // 2, nf + 1)) for _ in range(1 + len(blocks))]
        scratch += [pltpu.SemaphoreType.DMA(FsdpGather.SEMS) for _ in rows]
        scratch += [pltpu.VMEM(first, pieces.dtype)] + [pltpu.SemaphoreType.DMA((3, nf))] * 2
        count = len(arrays)
        return self.call(
            functools.partial(startup_kernel, nf, nc, tuple(spans), len(rows)),
            "startup", tuple(outs), arrays, [in_vmem()] * count, [in_place()] * count, scratch,
        )

    def guests(self, hosted_steps, first_in, first_out):
        plan, ins, outs, scratch, aliases = [], [], [], [], {}
        for kind, step, arrays in hosted_steps:
            shapes, boxes, alias = kind.shapes(self.nf, self.nc, step, arrays)
            if alias:
                aliases[first_in + len(ins)] = first_out + len(outs)
            plan.append((kind, step, len(arrays), len(shapes), len(boxes)))
            ins += list(arrays)
            outs += shapes
            scratch += boxes
        return tuple(plan), ins, outs, scratch, aliases

    def gather_fsdp(self, name, rows, hosted_steps=()):
        plan, ins, outs, scratch, aliases = self.guests(hosted_steps, 1, 1)
        got = self.call(
            functools.partial(gather_fsdp_kernel, self.nf, self.nc, plan),
            name,
            (jax.ShapeDtypeStruct((self.nf,) + rows.shape, rows.dtype),) + tuple(outs),
            [rows] + ins,
            [in_vmem()] + self.specs(hosted_steps),
            [in_place()] * (1 + len(outs)),
            [pltpu.SemaphoreType.DMA(FsdpGather.SEMS)] + scratch,
            aliases,
        )
        return got[0].reshape((-1,) + rows.shape[1:]), got[1:]

    def scatter_fsdp(self, name, left, right, turned, hosted_steps=(), order=None):
        count = left.shape[0] // self.nf
        own = [left.reshape(2 * self.nf, count // 2, left.shape[1]), right]
        own += [] if order is None else [order]
        plan, ins, outs, scratch, aliases = self.guests(hosted_steps, len(own), 1)
        block = (count, right.shape[0] if turned else right.shape[1])
        box = pltpu.VMEM(block, left.dtype)
        got = self.call(
            functools.partial(
                scatter_fsdp_kernel, self.nf, self.nc, plan, turned, order is not None
            ),
            name,
            (jax.ShapeDtypeStruct(block, jnp.float32),) + tuple(outs),
            own + ins,
            [in_vmem(), in_vmem(), in_smem()][: len(own)] + self.specs(hosted_steps),
            [in_vmem()] + [in_place()] * len(outs),
            [pltpu.VMEM((self.nf,) + block, left.dtype), box, box, box, box]
            + [pltpu.SemaphoreType.DMA((6, 4))]
            + scratch,
            aliases,
        )
        return got[0], got[1:]

    def attend_forward(self, segs, qkv, heads, hosted_steps):
        rows, wide = qkv.shape
        slots = wide // 3
        pairs = slots // LANES
        plan, ins, outs, scratch, aliases = self.guests(hosted_steps, 3, 3)
        low = jnp.bfloat16
        got = self.call(
            functools.partial(attend_forward_kernel, self.nf, self.nc, heads, plan),
            "attend_forward",
            (
                jax.ShapeDtypeStruct((rows, slots), low),
                jax.ShapeDtypeStruct((pairs, LANES, rows), jnp.float32),
                jax.ShapeDtypeStruct((pairs, 2, rows), jnp.float32),
            )
            + tuple(outs),
            [segs.reshape(1, rows), segs.reshape(rows, 1), qkv] + ins,
            [in_vmem()] * 3 + self.specs(hosted_steps),
            [in_vmem()] * 3 + [in_place()] * len(outs),
            [
                pltpu.VMEM((rows, LANES), low),
                pltpu.VMEM((rows, LANES), low),
                pltpu.VMEM((rows, LANES), low),
                pltpu.VMEM((LANES, rows), low),
                pltpu.VMEM((LANES, TILE), jnp.float32),
                pltpu.VMEM((2, 1, TILE), jnp.float32),
                pltpu.VMEM((2, 1, TILE), jnp.float32),
            ]
            + scratch,
            aliases,
        )
        return got[:3], got[3:]

    def attend_backward(self, segs, order, qkv, grads, turned, lse, heads, hosted_steps):
        rows, wide = qkv.shape
        plan, ins, outs, scratch, aliases = self.guests(hosted_steps, 7, 1)
        low = jnp.bfloat16
        got = self.call(
            functools.partial(attend_backward_kernel, self.nf, self.nc, heads, plan),
            "attend_backward",
            (jax.ShapeDtypeStruct((rows, wide), low),) + tuple(outs),
            [segs.reshape(1, rows), segs.reshape(rows, 1), qkv, grads, turned, lse, order] + ins,
            [in_vmem()] * 6 + [in_smem()] + self.specs(hosted_steps),
            [in_vmem()] + [in_place()] * len(outs),
            [
                pltpu.VMEM((rows, LANES), low),
                pltpu.VMEM((rows, LANES), low),
                pltpu.VMEM((rows, LANES), low),
                pltpu.VMEM((LANES, rows), low),
                pltpu.VMEM((rows, LANES), low),
                pltpu.VMEM((rows, LANES), low),
                pltpu.VMEM((rows, LANES), low),
                pltpu.VMEM((LANES, TILE), jnp.float32),
                pltpu.VMEM((rows, LANES), jnp.float32),
                pltpu.VMEM((rows, LANES), jnp.float32),
                pltpu.VMEM((2, 1, rows), jnp.float32),
            ]
            + scratch,
            aliases,
        )
        return got[0], got[1:]


def local_fast(
    net,
    inputs,
    cotangent,
    segments,
    stretch_order,
    prenorm_gain,
    prenorm_shift,
    joint_weight,
    query_bias,
    value_bias,
    mixer_weight,
    mixer_bias,
    midnorm_gain,
    midnorm_shift,
    expand_weight,
    expand_bias,
    shrink_weight,
    shrink_bias,
):
    nf, nc, each = net.nf, net.nc, net.each
    low, wide = jnp.bfloat16, jnp.float32
    _, stretch_len, width = inputs.shape
    heads_each = -(-(width // HEAD) // nf)
    span = heads_each * HEAD
    slots = slot_width(heads_each)
    rows_all = nc * stretch_len
    rows_own = each * stretch_len
    shard = lax.axis_index("fsdp")
    positions = stretch_order.reshape(each, nf).T.reshape(nc)
    inverse = jnp.sum(
        jnp.where(
            positions[None, :] == jnp.arange(nc, dtype=jnp.int32)[:, None],
            jnp.arange(nc, dtype=jnp.int32)[None, :],
            0,
        ),
        axis=1,
    ).astype(jnp.int32)

    narrow = prenorm_gain.shape[0]
    unit_each = expand_bias.shape[0] // nf

    depth = joint_weight.shape[0]
    thin = depth // (8 * nc) * 8
    rest = (depth - nc * thin) // each
    out_each = shrink_weight.shape[1]
    small_parts = (
        prenorm_gain, prenorm_shift, query_bias, value_bias, mixer_bias,
        midnorm_gain, midnorm_shift, shrink_bias, expand_bias,
    )
    small_count = len(small_parts) - 1 + nf
    small_rows = small_count + -small_count % 16
    last_rows = ((len(small_parts) - 1, small_rows - small_count), (0, 0))
    small_own = rows_of(small_parts[:-1], small_rows) + jnp.pad(
        expand_bias.reshape(nf, narrow), last_rows
    )
    small_own = widen(small_own)
    step = span - mixer_weight.shape[0]
    most = step * (nf - 1)
    columns = joint_weight.shape[1]
    joint_tall = jnp.concatenate(
        [
            joint_weight[: nc * thin].reshape(nc, thin, columns),
            jnp.tile(joint_weight[nc * thin :].reshape(each, rest, columns), (nf, 1, 1)),
        ],
        axis=1,
    )
    seg_own = jnp.broadcast_to(segments.astype(low)[:, None], (each, 16, stretch_len))
    joint_pieces, small_all, own_tokens, seg_own, above, expand_pieces, shrink_pieces = (
        net.lone(
            "first",
            [
                (TradeGuest, ("ctx", None), [widen(joint_tall)]),
                (TradeGuest, ("ctx", None), [small_own]),
                (SwapGuest, "column", [inputs]),
                (SwapGuest, "column", [seg_own]),
                (TradeGuest, ("fsdp", (nf - 1,)), [widen(mixer_weight[:most])]),
                (
                    TradeGuest,
                    ("fsdp", None),
                    [widen(expand_weight.T.reshape(nf, unit_each, depth))],
                ),
                (
                    TradeGuest,
                    ("fsdp", None),
                    [
                        widen(
                            shrink_weight.reshape(each, nf, unit_each, out_each)
                            .transpose(1, 0, 2, 3)
                            .reshape(nf, each * unit_each, out_each)
                        )
                    ],
                ),
            ],
        )
    )
    own_tokens = own_tokens.reshape(rows_own, width)
    joint_pieces = joint_pieces[..., :columns].transpose(1, 0, 2)
    joint_pieces = joint_split(joint_pieces.reshape(thin + rest, 3, width), nf, heads_each)
    expand_pieces = (
        expand_pieces[..., :depth].transpose(1, 0, 2).reshape(unit_each, width)
    )
    shrink_pieces = shrink_pieces[..., :out_each].reshape(nc * unit_each, out_each).T

    above = lax.dynamic_index_in_dim(above, (shard + 1) % nf, 0, keepdims=False)
    above = above[:, : mixer_weight.shape[1]]
    tall = jnp.concatenate([mixer_weight, above, jnp.zeros_like(above)])
    mixer_rows = lax.dynamic_slice_in_dim(tall, step * shard, span, 0)
    kept = shard * span + jnp.arange(span, dtype=jnp.int32) < width
    mixer_rows = jnp.where(kept[:, None], mixer_rows, jnp.zeros_like(mixer_rows))
    mixer_pieces = jnp.pad(mixer_rows.T, ((0, 0), (0, slots - span)))

    joint, mixer, expand, shrink, tokens, seg_blocks = net.startup(
        joint_pieces,
        nf * thin + rest,
        width,
        [mixer_pieces, expand_pieces, shrink_pieces],
        [nc // 2, nc // 2, 1, 1],
        [own_tokens, seg_own.reshape(each * 16, stretch_len)],
    )
    mixer = mixer.reshape(width, slots)
    tokens = tokens.reshape(rows_all, width)
    cotangent, tokens = lax.optimization_barrier((cotangent, tokens))
    own_tangent = net.swap(cotangent, to_column, to_origin).reshape(rows_own, width)
    segs = pick(seg_blocks.reshape(nc, 16, stretch_len)[:, 0], inverse)
    segs = segs.astype(jnp.int32)
    small_all = small_all[:, :small_count, :narrow].transpose(1, 0, 2).astype(wide)
    gain_one, shift_one, qbias, vbias, mbias, gain_two, shift_two, sbias = (
        small_all[: small_count - nf].reshape(small_count - nf, width)
    )
    ebias = small_all[small_count - nf :].reshape(nf, nc, unit_each)
    ebias = all_units(ebias, nc, nf, unit_each, shard)
    joint_bias = lax.dynamic_index_in_dim(
        joint_split(
            jnp.stack([qbias, jnp.zeros_like(qbias), vbias])[None], nf, heads_each
        ),
        shard, 0, keepdims=False,
    )

    tokens = pick(tokens.reshape(nc, stretch_len, width), inverse)
    token_values = tokens.reshape(rows_all, width).astype(wide)
    unit_one, _ = normalize(token_values)
    normed = (unit_one * gain_one + shift_one).astype(low)
    qkv = (
        jnp.dot(normed, joint, preferred_element_type=wide) + joint_bias
    ).astype(low)
    (attended, turned, lse), (expand, shrink, tangent) = net.attend_forward(
        segs,
        qkv,
        heads_each,
        [
            (GatherStep, 2, [expand]),
            (GatherStep, 2, [shrink]),
            (SideGather, 0, [own_tangent]),
        ],
    )
    attended = pick(attended.reshape(nc, stretch_len, slots), positions)
    attended = attended.reshape(rows_all, slots)
    branch, (expand, shrink) = net.scatter_fsdp(
        "scatter_branch",
        attended,
        mixer,
        True,
        [
            (GatherStep, 3, [expand]),
            (GatherStep, 3, [shrink]),
        ],
    )
    tangent = tangent.reshape(rows_all, width)
    middle = own_tokens.astype(wide) + branch + mbias
    unit_two, inverse_two = normalize(middle)
    second_own = (unit_two * gain_two + shift_two).astype(low)
    second, (expand, shrink) = net.gather_fsdp(
        "gather_second", second_own, [(GatherStep, 4, [expand]), (GatherStep, 4, [shrink])]
    )
    expand = expand.reshape(nc * unit_each, width)
    shrink = shrink.reshape(width, nc * unit_each)
    expanded = times_transposed(second, expand) + ebias
    active, slope = gelu_parts(expanded)
    active = active.astype(low)

    shrink_rows = outer_sum(tangent, active).astype(low).reshape(nc, out_each, nc * unit_each)
    active_grad = jnp.dot(tangent, shrink, preferred_element_type=wide)
    expand_delta = (active_grad * slope).astype(low)
    expand_rows = outer_sum(expand_delta, second).astype(low).reshape(nc, unit_each, width)
    second_grad, boxes = net.scatter_fsdp(
        "scatter_second",
        expand_delta,
        expand,
        False,
        [(ScatterStep, 1, [expand_rows]), (ScatterStep, 1, [shrink_rows])],
    )
    middle_delta = own_tangent.astype(wide) + normalize_back(
        second_grad, gain_two, unit_two, inverse_two
    )
    branch_own = middle_delta.astype(low)
    branch_delta, boxes = net.gather_fsdp(
        "gather_branch",
        branch_own,
        [(ScatterStep, 2, [expand_rows, *boxes[:2]]), (ScatterStep, 2, [shrink_rows, *boxes[2:]])],
    )
    lifted, boxes = net.scatter_fsdp(
        "scatter_lifted",
        active,
        shrink,
        True,
        [(ScatterStep, 3, [expand_rows, *boxes[:2]]), (ScatterStep, 3, [shrink_rows, *boxes[2:]])],
    )
    out_rows = (middle + lifted + sbias).astype(low)
    block_output = net.swap(out_rows.reshape(each, stretch_len, width), to_origin, to_column)
    attended_delta = jnp.dot(branch_delta, mixer, preferred_element_type=wide).astype(low)
    mixer_rows = outer_sum(branch_delta, attended).astype(low).reshape(nc, out_each, slots)
    attended_delta = attended_delta.reshape(nc, stretch_len, slots)
    joint_delta, boxes = net.attend_backward(
        segs,
        inverse,
        qkv,
        attended_delta,
        turned,
        lse,
        heads_each,
        [(ScatterStep, 4, [expand_rows, *boxes[:2]]), (ScatterStep, 4, [shrink_rows, *boxes[2:]])],
    )
    expand_grad = net.total(expand_rows, *boxes[:2])
    shrink_grad = net.total(shrink_rows, *boxes[2:])
    joint_rows = outer_sum(normed, joint_delta).astype(low)
    normed_grad, (joint_grad, mixer_grad, expand_pieces, shrink_pieces) = (
        net.scatter_fsdp(
            "scatter_normed",
            joint_delta,
            joint,
            True,
            [
                (ScatterRing, nf * thin + rest, [joint_rows]),
                (ScatterRing, 0, [mixer_rows]),
                (WindowTrade, width, [widen(expand_grad)]),
                (WindowTrade, nc * unit_each, [widen(shrink_grad)]),
            ],
            positions,
        )
    )
    unit_own, inverse_own = normalize(own_tokens.astype(wide))
    input_rows = middle_delta + normalize_back(normed_grad, gain_one, unit_own, inverse_own)
    mine = jnp.arange(nf, dtype=jnp.int32) == shard
    sums = jnp.sum(joint_delta.astype(wide), axis=0).reshape(3, slots)[:, :span]
    spread = jnp.where(mine[None, :, None], sums[:, None, :], 0.0).reshape(3, nf * span)
    unit_sums = jnp.sum(expand_delta.astype(wide), axis=0).reshape(nc, 1, unit_each)
    unit_sums = jnp.where(mine[None, :, None], unit_sums, 0.0).reshape(nc, nf * unit_each)
    vectors = (
        jnp.sum(normed_grad * unit_own, axis=0),
        jnp.sum(normed_grad, axis=0),
        spread[0, :width],
        spread[2, :width],
        jnp.sum(branch_own.astype(wide), axis=0),
        jnp.sum(second_grad * unit_two, axis=0),
        jnp.sum(second_grad, axis=0),
        jnp.sum(own_tangent.astype(wide), axis=0),
    )
    stacked = rows_of(vectors, len(vectors)).reshape(len(vectors), nc, narrow)
    unit_sums = unit_sums.reshape(nc, nf, narrow).transpose(1, 0, 2)
    small_blocks = jnp.concatenate(
        [stacked, unit_sums, jnp.zeros((small_rows - small_count, nc, narrow), wide)]
    )
    small_blocks = widen(small_blocks.astype(low)).transpose(1, 0, 2)
    small_lanes = small_blocks.shape[2]

    joint_pieces, joint_last, mixer_pieces, small_pieces, input_gradient = net.lone(
        "second",
        [
            (
                TradeGuest,
                ("fsdp", None),
                [joint_grad[: nf * thin].reshape(nf, thin, 3 * slots)],
            ),
            (TradeGuest, ("fsdp", None), [joint_grad[nf * thin :]]),
            (TradeGuest, ("fsdp", (1,)), [mixer_grad]),
            (TradeGuest, ("fsdp", None), [small_blocks.reshape(nc * small_rows, small_lanes)]),
            (SwapGuest, "origin", [input_rows.astype(low).reshape(each, stretch_len, width)]),
        ],
    )
    input_gradient = input_gradient.astype(wide)
    small_blocks = jnp.sum(small_pieces.astype(wide), axis=0).astype(low)
    joint_pieces = jnp.concatenate([joint_pieces, joint_last], axis=1)
    joint_pieces = joint_join(joint_pieces, heads_each, width)
    joint_pieces = joint_pieces.reshape(thin + rest, nc, columns).transpose(1, 0, 2)
    joint_pieces, small_pieces = net.lone(
        "third",
        [
            (TradeGuest, ("ctx", None), [widen(joint_pieces)]),
            (TradeGuest, ("ctx", None), [small_blocks.reshape(nc, small_rows, small_lanes)]),
        ],
    )
    joint_pieces = joint_pieces[..., :columns]
    joint_last = lax.dynamic_slice_in_dim(joint_pieces[:, thin:], each * shard, each, 0)
    joint_gradient = jnp.concatenate(
        [
            joint_pieces[:, :thin].reshape(nc * thin, columns),
            joint_last.reshape(each * rest, columns),
        ]
    ).astype(wide)
    at = shard * depth - window(shard, nf, width)[0]
    expand_pieces = lax.dynamic_slice_in_dim(expand_pieces, at, depth, 2)
    expand_gradient = expand_pieces.reshape(nf * unit_each, depth).T.astype(wide)
    units = each * unit_each
    at = shard * units - window(shard, nf, nf * units)[0]
    shrink_pieces = lax.dynamic_slice_in_dim(shrink_pieces, at, units, 2)
    shrink_pieces = shrink_pieces.reshape(nf, out_each, each, unit_each).transpose(2, 0, 3, 1)
    shrink_gradient = shrink_pieces.reshape(shrink_weight.shape).astype(wide)

    own_rows = lax.dynamic_index_in_dim(mixer_pieces, shard, 0, keepdims=False)[:, :span].T
    before = lax.dynamic_index_in_dim(mixer_pieces, (shard + nf - 1) % nf, 0, keepdims=False)
    below = lax.dynamic_slice_in_dim(
        jnp.pad(before[:, :span].T, ((0, most), (0, 0))),
        mixer_weight.shape[0] - step * ((shard + nf - 1) % nf),
        most,
        0,
    )
    moved = lax.dynamic_slice_in_dim(
        jnp.pad(own_rows, ((most, 0), (0, 0))), most - step * shard, mixer_weight.shape[0], 0
    )
    first_rows = jnp.arange(mixer_weight.shape[0], dtype=jnp.int32)[:, None] < step * shard
    below = jnp.pad(below, ((0, mixer_weight.shape[0] - most), (0, 0)))
    mixer_gradient = jnp.where(first_rows, below, moved).astype(wide)

    small_sum = jnp.sum(small_pieces.astype(wide), axis=0)[:small_count, :narrow]
    outs = [small_sum[k] for k in range(8)]
    return (
        block_output,
        input_gradient,
        outs[0],
        outs[1],
        joint_gradient,
        outs[2],
        outs[3],
        mixer_gradient,
        outs[4],
        outs[5],
        outs[6],
        expand_gradient,
        small_sum[8:].reshape(expand_bias.shape),
        shrink_gradient,
        outs[7],
    )


def solution(mesh):
    in_specs = (
        P("fsdp", "ctx", None),
        P("fsdp", "ctx", None),
        P("fsdp", "ctx"),
        P(),
        P("ctx"),
        P("ctx"),
        P("fsdp", "ctx"),
        P("ctx"),
        P("ctx"),
        P("fsdp", "ctx"),
        P("ctx"),
        P("ctx"),
        P("ctx"),
        P("fsdp", "ctx"),
        P("ctx"),
        P("fsdp", "ctx"),
        P("ctx"),
    )
    out_specs = (
        P("fsdp", "ctx", None),
        P("fsdp", "ctx", None),
        P("ctx"),
        P("ctx"),
        P("fsdp", "ctx"),
        P("ctx"),
        P("ctx"),
        P("fsdp", "ctx"),
        P("ctx"),
        P("ctx"),
        P("ctx"),
        P("fsdp", "ctx"),
        P("ctx"),
        P("fsdp", "ctx"),
        P("ctx"),
    )

    def run(*arrays):
        nf, nc = mesh.shape["fsdp"], mesh.shape["ctx"]
        whole_each = arrays[0].shape[0] == nc and (nf, nc) == (4, 8)
        if whole_each and arrays[0].shape[1] == nc * STRETCH:
            body = functools.partial(local_fast, Net(nf, nc))
        else:
            body = local
        return jax.shard_map(
            body, mesh=mesh, in_specs=in_specs, out_specs=out_specs, check_vma=False
        )(*arrays)

    return run
```

```python
import functools

import jax
import jax.numpy as jnp
from jax import lax
from jax.experimental import pallas as pl
from jax.experimental.pallas import tpu as pltpu
from jax.sharding import PartitionSpec as P


HEAD = 64
MICRO = 2
LANES = 128
STRETCH = 128
TILE = 256


epsilon = 1e-05
masked_score = -1e30


def layer_norm(values, gain, shift):
    center = values - jnp.mean(values, axis=-1, keepdims=True)
    spread = jnp.mean(center * center, axis=-1, keepdims=True)
    return center * lax.rsqrt(spread + epsilon) * gain + shift


def piece_size(count):
    size_now = min(count, 512)
    while count % size_now:
        size_now -= 1
    return size_now


def true_positions(stretch_order, first_index, count, stretch_len):
    stored = first_index + jnp.arange(count, dtype=jnp.int32)
    holder = stored // stretch_len
    picked = holder[:, None] == jnp.arange(stretch_order.shape[0], dtype=jnp.int32)[None, :]
    return (
        jnp.sum(jnp.where(picked, stretch_order[None, :], 0), axis=1) * stretch_len
        + stored % stretch_len
    )


def times_transposed(left, right):
    return lax.dot_general(
        left, right, (((1,), (1,)), ((), ())), preferred_element_type=jnp.float32
    )


def outer_sum(left, right):
    return lax.dot_general(
        left, right, (((0,), (0,)), ((), ())), preferred_element_type=jnp.float32
    )


def fetch_weights(local_parts):
    (
        joint_weight,
        mixer_weight,
        expand_weight,
        shrink_weight,
        prenorm_gain,
        prenorm_shift,
        query_bias,
        value_bias,
        mixer_bias,
        midnorm_gain,
        midnorm_shift,
        expand_bias,
        shrink_bias,
    ) = local_parts
    spread_out = (
        lax.all_gather(joint_weight, "ctx", axis=1, tiled=True),
        lax.all_gather(mixer_weight, "ctx", axis=1, tiled=True),
        lax.all_gather(expand_weight, "ctx", axis=1, tiled=True),
        lax.all_gather(shrink_weight, "ctx", axis=1, tiled=True),
        lax.all_gather(prenorm_gain, "ctx", axis=0, tiled=True),
        lax.all_gather(prenorm_shift, "ctx", axis=0, tiled=True),
        lax.all_gather(query_bias, "ctx", axis=0, tiled=True),
        lax.all_gather(value_bias, "ctx", axis=0, tiled=True),
        lax.all_gather(mixer_bias, "ctx", axis=0, tiled=True),
        lax.all_gather(midnorm_gain, "ctx", axis=0, tiled=True),
        lax.all_gather(midnorm_shift, "ctx", axis=0, tiled=True),
        lax.all_gather(expand_bias, "ctx", axis=0, tiled=True),
        lax.all_gather(shrink_bias, "ctx", axis=0, tiled=True),
    )
    whole_rows = (
        lax.all_gather(spread_out[0], "fsdp", axis=0, tiled=True),
        lax.all_gather(spread_out[1], "fsdp", axis=0, tiled=True),
        lax.all_gather(spread_out[2], "fsdp", axis=0, tiled=True),
        lax.all_gather(spread_out[3], "fsdp", axis=0, tiled=True),
    )
    return tuple(whole_rows) + tuple(spread_out[4:])


def reduce_gradients(matrices, smalls):
    small_sums = (
        lax.psum(smalls[0].astype(jnp.bfloat16), "fsdp").astype(jnp.float32),
        lax.psum(smalls[1].astype(jnp.bfloat16), "fsdp").astype(jnp.float32),
        lax.psum(smalls[2].astype(jnp.bfloat16), "fsdp").astype(jnp.float32),
        lax.psum(smalls[3].astype(jnp.bfloat16), "fsdp").astype(jnp.float32),
        lax.psum(smalls[4].astype(jnp.bfloat16), "fsdp").astype(jnp.float32),
        lax.psum(smalls[5].astype(jnp.bfloat16), "fsdp").astype(jnp.float32),
        lax.psum(smalls[6].astype(jnp.bfloat16), "fsdp").astype(jnp.float32),
        lax.psum(smalls[7].astype(jnp.bfloat16), "fsdp").astype(jnp.float32),
        lax.psum(smalls[8].astype(jnp.bfloat16), "fsdp").astype(jnp.float32),
    )
    column_part = (
        lax.psum_scatter(
            matrices[0].astype(jnp.bfloat16), "ctx", scatter_dimension=1, tiled=True
        ).astype(jnp.float32),
        lax.psum_scatter(
            matrices[1].astype(jnp.bfloat16), "ctx", scatter_dimension=1, tiled=True
        ).astype(jnp.float32),
        lax.psum_scatter(
            matrices[2].astype(jnp.bfloat16), "ctx", scatter_dimension=1, tiled=True
        ).astype(jnp.float32),
        lax.psum_scatter(
            matrices[3].astype(jnp.bfloat16), "ctx", scatter_dimension=1, tiled=True
        ).astype(jnp.float32),
        lax.psum_scatter(
            small_sums[0].astype(jnp.bfloat16), "ctx", scatter_dimension=0, tiled=True
        ).astype(jnp.float32),
        lax.psum_scatter(
            small_sums[1].astype(jnp.bfloat16), "ctx", scatter_dimension=0, tiled=True
        ).astype(jnp.float32),
        lax.psum_scatter(
            small_sums[2].astype(jnp.bfloat16), "ctx", scatter_dimension=0, tiled=True
        ).astype(jnp.float32),
        lax.psum_scatter(
            small_sums[3].astype(jnp.bfloat16), "ctx", scatter_dimension=0, tiled=True
        ).astype(jnp.float32),
        lax.psum_scatter(
            small_sums[4].astype(jnp.bfloat16), "ctx", scatter_dimension=0, tiled=True
        ).astype(jnp.float32),
        lax.psum_scatter(
            small_sums[5].astype(jnp.bfloat16), "ctx", scatter_dimension=0, tiled=True
        ).astype(jnp.float32),
        lax.psum_scatter(
            small_sums[6].astype(jnp.bfloat16), "ctx", scatter_dimension=0, tiled=True
        ).astype(jnp.float32),
        lax.psum_scatter(
            small_sums[7].astype(jnp.bfloat16), "ctx", scatter_dimension=0, tiled=True
        ).astype(jnp.float32),
        lax.psum_scatter(
            small_sums[8].astype(jnp.bfloat16), "ctx", scatter_dimension=0, tiled=True
        ).astype(jnp.float32),
    )
    row_part = (
        lax.psum_scatter(
            column_part[0].astype(jnp.bfloat16), "fsdp", scatter_dimension=0, tiled=True
        ).astype(jnp.float32),
        lax.psum_scatter(
            column_part[1].astype(jnp.bfloat16), "fsdp", scatter_dimension=0, tiled=True
        ).astype(jnp.float32),
        lax.psum_scatter(
            column_part[2].astype(jnp.bfloat16), "fsdp", scatter_dimension=0, tiled=True
        ).astype(jnp.float32),
        lax.psum_scatter(
            column_part[3].astype(jnp.bfloat16), "fsdp", scatter_dimension=0, tiled=True
        ).astype(jnp.float32),
    )
    return tuple(row_part) + tuple(column_part[4:])


def local(
    inputs,
    cotangent,
    segments,
    stretch_order,
    prenorm_gain,
    prenorm_shift,
    joint_weight,
    query_bias,
    value_bias,
    mixer_weight,
    mixer_bias,
    midnorm_gain,
    midnorm_shift,
    expand_weight,
    expand_bias,
    shrink_weight,
    shrink_bias,
):
    local_parts = (
        joint_weight,
        mixer_weight,
        expand_weight,
        shrink_weight,
        prenorm_gain,
        prenorm_shift,
        query_bias,
        value_bias,
        mixer_bias,
        midnorm_gain,
        midnorm_shift,
        expand_bias,
        shrink_bias,
    )
    seq_local, stretch_len, model_width = inputs.shape
    head_count = model_width // HEAD
    group_size = seq_local // MICRO
    row_count = group_size * stretch_len
    score_scale = HEAD ** (-0.5)
    ctx_place = lax.axis_index("ctx")
    own_stretch = jnp.sum(
        jnp.where(
            jnp.arange(stretch_order.shape[0], dtype=jnp.int32) == ctx_place, stretch_order, 0
        )
    )
    own_pos = own_stretch * stretch_len + jnp.arange(stretch_len, dtype=jnp.int32)
    all_segments = lax.all_gather(segments, "ctx", axis=1, tiled=True)

    def backward_micro(weights, kept_values, micro_index):
        (
            joint_full,
            mixer_full,
            expand_full,
            shrink_full,
            gain_one,
            shift_one,
            _,
            _,
            _,
            gain_two,
            shift_two,
            _,
            _,
        ) = weights
        (
            tokens,
            seg_local,
            seg_whole,
            normed,
            queries,
            keys_local,
            values_local,
            mixed_rows,
            attended,
            log_total,
            middle,
            second,
            expanded,
            active,
        ) = kept_values
        lower = micro_index * group_size
        tangent_rows = cotangent[lower : lower + group_size].reshape(row_count, model_width)
        active_grad = times_transposed(tangent_rows, shrink_full)
        gelu_pull = jax.vjp(lambda value_in: jax.nn.gelu(value_in, approximate=True), expanded)[1]
        expand_delta = gelu_pull(active_grad)[0].astype(jnp.bfloat16)
        second_grad = times_transposed(expand_delta, expand_full)
        mid_pull = jax.vjp(
            layer_norm, middle, gain_two.astype(jnp.float32), shift_two.astype(jnp.float32)
        )[1]
        middle_grad, gain_two_grad, shift_two_grad = mid_pull(second_grad)
        middle_grad = middle_grad + tangent_rows.astype(jnp.float32)
        branch_delta = middle_grad.astype(jnp.bfloat16)
        attended_delta = times_transposed(branch_delta, mixer_full).astype(jnp.bfloat16)
        grad_heads = attended_delta.reshape(group_size, stretch_len, head_count, HEAD)
        delta_heads = jnp.sum(
            grad_heads.transpose(0, 2, 1, 3).astype(jnp.float32) * attended, axis=-1
        )
        delta_rows = delta_heads.transpose(0, 2, 1)
        log_rows = log_total.transpose(0, 2, 1)
        lse_whole, delta_whole = (
            lax.all_gather(log_rows, "ctx", axis=1, tiled=True),
            lax.all_gather(delta_rows, "ctx", axis=1, tiled=True),
        )
        query_heads = queries.reshape(group_size, stretch_len, head_count, HEAD)
        key_heads = keys_local.reshape(group_size, stretch_len, head_count, HEAD)
        value_heads = values_local.reshape(group_size, stretch_len, head_count, HEAD)
        head_zeros = jnp.zeros((group_size, head_count, stretch_len, HEAD), jnp.float32)
        query_key_piece = lax.all_gather(keys_local, "ctx", axis=1, tiled=True)
        value_piece = lax.all_gather(values_local, "ctx", axis=1, tiled=True)
        count = query_key_piece.shape[1]
        step_len = piece_size(count)

        def query_block_step(turn_index, running):
            offset = turn_index * step_len
            key_block = lax.dynamic_slice_in_dim(query_key_piece, offset, step_len, 1).reshape(
                group_size, step_len, head_count, HEAD
            )
            value_block = lax.dynamic_slice_in_dim(value_piece, offset, step_len, 1).reshape(
                group_size, step_len, head_count, HEAD
            )
            key_pos = true_positions(stretch_order, offset, step_len, stretch_len)
            key_seg = lax.dynamic_slice_in_dim(seg_whole, offset, step_len, 1)
            allowed = (
                (seg_local[:, :, None] == key_seg[:, None, :])
                & (key_pos[None, None, :] <= own_pos[None, :, None])
            )[:, None]
            scores = (
                jnp.einsum(
                    "gqhd,gkhd->ghqk", query_heads, key_block, preferred_element_type=jnp.float32
                )
                * score_scale
            )
            probs = jnp.where(allowed, jnp.exp(scores - log_total[..., None]), 0.0)
            dots = jnp.einsum(
                "gqhd,gkhd->ghqk", grad_heads, value_block, preferred_element_type=jnp.float32
            )
            score_delta = (probs * (dots - delta_heads[..., None])).astype(jnp.bfloat16)
            return running + jnp.einsum(
                "ghqk,gkhd->ghqd", score_delta, key_block, preferred_element_type=jnp.float32
            )

        query_acc = lax.fori_loop(0, count // step_len, query_block_step, head_zeros)
        grad_rows3 = attended_delta.reshape(group_size, stretch_len, model_width)
        query_piece_rows = lax.all_gather(queries, "ctx", axis=1, tiled=True)
        grad_piece = lax.all_gather(grad_rows3, "ctx", axis=1, tiled=True)
        count = query_piece_rows.shape[1]
        key_step_len = piece_size(count)

        def key_block_step(turn_index, running):
            key_acc, value_acc = running
            offset = turn_index * key_step_len
            query_block = lax.dynamic_slice_in_dim(
                query_piece_rows, offset, key_step_len, 1
            ).reshape(group_size, key_step_len, head_count, HEAD)
            grad_block = lax.dynamic_slice_in_dim(grad_piece, offset, key_step_len, 1).reshape(
                group_size, key_step_len, head_count, HEAD
            )
            query_pos = true_positions(stretch_order, offset, key_step_len, stretch_len)
            query_seg = lax.dynamic_slice_in_dim(seg_whole, offset, key_step_len, 1)
            lse_block = lax.dynamic_slice_in_dim(lse_whole, offset, key_step_len, 1).transpose(
                0, 2, 1
            )
            delta_block = lax.dynamic_slice_in_dim(delta_whole, offset, key_step_len, 1).transpose(
                0, 2, 1
            )
            allowed = (
                (query_seg[:, :, None] == seg_local[:, None, :])
                & (own_pos[None, None, :] <= query_pos[None, :, None])
            )[:, None]
            scores = (
                jnp.einsum(
                    "gqhd,gkhd->ghqk", query_block, key_heads, preferred_element_type=jnp.float32
                )
                * score_scale
            )
            probs = jnp.where(allowed, jnp.exp(scores - lse_block[..., None]), 0.0)
            value_acc = value_acc + jnp.einsum(
                "ghqk,gqhd->ghkd",
                probs.astype(jnp.bfloat16),
                grad_block,
                preferred_element_type=jnp.float32,
            )
            dots = jnp.einsum(
                "gqhd,gkhd->ghqk", grad_block, value_heads, preferred_element_type=jnp.float32
            )
            score_delta = (probs * (dots - delta_block[..., None])).astype(jnp.bfloat16)
            key_acc = key_acc + jnp.einsum(
                "ghqk,gqhd->ghkd", score_delta, query_block, preferred_element_type=jnp.float32
            )
            return (key_acc, value_acc)

        key_acc, value_acc = lax.fori_loop(
            0, count // key_step_len, key_block_step, (head_zeros, head_zeros)
        )
        query_delta = (
            (query_acc * score_scale)
            .transpose(0, 2, 1, 3)
            .reshape(row_count, model_width)
            .astype(jnp.bfloat16)
        )
        key_delta = (
            (key_acc * score_scale)
            .transpose(0, 2, 1, 3)
            .reshape(row_count, model_width)
            .astype(jnp.bfloat16)
        )
        value_delta = (
            value_acc.transpose(0, 2, 1, 3).reshape(row_count, model_width).astype(jnp.bfloat16)
        )
        joint_delta = jnp.concatenate([query_delta, key_delta, value_delta], axis=1)
        normed_grad = times_transposed(joint_delta, joint_full)
        first_pull = jax.vjp(
            layer_norm,
            tokens.reshape(row_count, model_width),
            gain_one.astype(jnp.float32),
            shift_one.astype(jnp.float32),
        )[1]
        token_grad, gain_one_grad, shift_one_grad = first_pull(normed_grad)
        input_grad = (middle_grad + token_grad).reshape(group_size, stretch_len, model_width)
        small_terms = (
            gain_one_grad,
            shift_one_grad,
            jnp.sum(query_delta.astype(jnp.float32), axis=0),
            jnp.sum(value_delta.astype(jnp.float32), axis=0),
            jnp.sum(branch_delta.astype(jnp.float32), axis=0),
            gain_two_grad,
            shift_two_grad,
            jnp.sum(expand_delta.astype(jnp.float32), axis=0),
            jnp.sum(tangent_rows.astype(jnp.float32), axis=0),
        )
        factor_pairs = (
            normed.reshape(row_count, model_width),
            joint_delta,
            mixed_rows,
            branch_delta,
            second,
            expand_delta,
            active,
            tangent_rows,
        )
        return (input_grad, small_terms, factor_pairs)

    output_list = []
    input_list = []
    factor_list = []
    small_totals = None
    for micro_index in range(MICRO):
        forward_weights = fetch_weights(local_parts)
        (
            forward_joint_full,
            forward_mixer_full,
            forward_expand_full,
            forward_shrink_full,
            forward_gain_one,
            forward_shift_one,
            forward_qbias_full,
            forward_vbias_full,
            forward_mbias_full,
            forward_gain_two,
            forward_shift_two,
            forward_ebias_full,
            forward_sbias_full,
        ) = forward_weights
        forward_lower = micro_index * group_size
        forward_tokens = inputs[forward_lower : forward_lower + group_size].astype(jnp.float32)
        forward_seg_local = segments[forward_lower : forward_lower + group_size]
        forward_seg_whole = all_segments[forward_lower : forward_lower + group_size]
        forward_normed = layer_norm(
            forward_tokens,
            forward_gain_one.astype(jnp.float32),
            forward_shift_one.astype(jnp.float32),
        ).astype(jnp.bfloat16)
        joint_bias = jnp.concatenate(
            [forward_qbias_full, jnp.zeros_like(forward_qbias_full), forward_vbias_full]
        ).astype(jnp.float32)
        joint_rows = (
            jnp.dot(
                forward_normed.reshape(row_count, model_width),
                forward_joint_full,
                preferred_element_type=jnp.float32,
            )
            + joint_bias
        )
        joint_rows = joint_rows.astype(jnp.bfloat16).reshape(
            group_size, stretch_len, 3 * model_width
        )
        forward_queries = joint_rows[..., :model_width]
        forward_keys_local = joint_rows[..., model_width : 2 * model_width]
        forward_values_local = joint_rows[..., 2 * model_width :]
        forward_query_heads = forward_queries.reshape(group_size, stretch_len, head_count, HEAD)
        start_state = (
            jnp.full((group_size, head_count, stretch_len), masked_score, jnp.float32),
            jnp.zeros((group_size, head_count, stretch_len), jnp.float32),
            jnp.zeros((group_size, head_count, stretch_len, HEAD), jnp.float32),
        )
        forward_key_piece = lax.all_gather(forward_keys_local, "ctx", axis=1, tiled=True)
        forward_value_piece = lax.all_gather(forward_values_local, "ctx", axis=1, tiled=True)
        forward_count = forward_key_piece.shape[1]
        forward_step_len = piece_size(forward_count)

        def forward_block_step(turn_index, state):
            top_score, row_total, accumulated = state
            offset = turn_index * forward_step_len
            key_block = lax.dynamic_slice_in_dim(
                forward_key_piece, offset, forward_step_len, 1
            ).reshape(group_size, forward_step_len, head_count, HEAD)
            value_block = lax.dynamic_slice_in_dim(
                forward_value_piece, offset, forward_step_len, 1
            ).reshape(group_size, forward_step_len, head_count, HEAD)
            key_pos = true_positions(stretch_order, offset, forward_step_len, stretch_len)
            key_seg = lax.dynamic_slice_in_dim(forward_seg_whole, offset, forward_step_len, 1)
            allowed = (
                (forward_seg_local[:, :, None] == key_seg[:, None, :])
                & (key_pos[None, None, :] <= own_pos[None, :, None])
            )[:, None]
            scores = (
                jnp.einsum(
                    "gqhd,gkhd->ghqk",
                    forward_query_heads,
                    key_block,
                    preferred_element_type=jnp.float32,
                )
                * score_scale
            )
            scores = jnp.where(allowed, scores, masked_score)
            new_top = jnp.maximum(top_score, jnp.max(scores, axis=-1))
            weights_now = jnp.where(allowed, jnp.exp(scores - new_top[..., None]), 0.0)
            fade_factor = jnp.exp(top_score - new_top)
            row_total = row_total * fade_factor + jnp.sum(weights_now, axis=-1)
            accumulated = accumulated * fade_factor[..., None] + jnp.einsum(
                "ghqk,gkhd->ghqd",
                weights_now.astype(jnp.bfloat16),
                value_block,
                preferred_element_type=jnp.float32,
            )
            return (new_top, row_total, accumulated)

        top_score, row_total, accumulated = lax.fori_loop(
            0, forward_count // forward_step_len, forward_block_step, start_state
        )
        forward_attended = accumulated / row_total[..., None]
        forward_log_total = top_score + jnp.log(row_total)
        forward_mixed_rows = (
            forward_attended.transpose(0, 2, 1, 3)
            .reshape(row_count, model_width)
            .astype(jnp.bfloat16)
        )
        branch = jnp.dot(
            forward_mixed_rows, forward_mixer_full, preferred_element_type=jnp.float32
        ) + forward_mbias_full.astype(jnp.float32)
        forward_middle = forward_tokens.reshape(row_count, model_width) + branch
        forward_second = layer_norm(
            forward_middle,
            forward_gain_two.astype(jnp.float32),
            forward_shift_two.astype(jnp.float32),
        ).astype(jnp.bfloat16)
        forward_expanded = jnp.dot(
            forward_second, forward_expand_full, preferred_element_type=jnp.float32
        ) + forward_ebias_full.astype(jnp.float32)
        forward_active = jax.nn.gelu(forward_expanded, approximate=True).astype(jnp.bfloat16)
        output = (
            forward_middle
            + jnp.dot(forward_active, forward_shrink_full, preferred_element_type=jnp.float32)
            + forward_sbias_full.astype(jnp.float32)
        )
        forward_kept_values = (
            forward_tokens,
            forward_seg_local,
            forward_seg_whole,
            forward_normed,
            forward_queries,
            forward_keys_local,
            forward_values_local,
            forward_mixed_rows,
            forward_attended,
            forward_log_total,
            forward_middle,
            forward_second,
            forward_expanded,
            forward_active,
        )
        output_now = output.reshape(group_size, stretch_len, model_width).astype(jnp.bfloat16)
        kept_values = forward_kept_values
        backward_weights = fetch_weights(local_parts)
        input_now, small_terms, factor_pairs = backward_micro(
            backward_weights, kept_values, micro_index
        )
        output_list.append(output_now)
        input_list.append(input_now)
        factor_list.append(factor_pairs)
        if small_totals is None:
            small_totals = small_terms
        else:
            small_totals = tuple(
                (total_now + term_now for total_now, term_now in zip(small_totals, small_terms))
            )

    def joined(position):
        return jnp.concatenate([pairs_now[position] for pairs_now in factor_list], axis=0)

    matrices = (
        outer_sum(joined(0), joined(1)),
        outer_sum(joined(2), joined(3)),
        outer_sum(joined(4), joined(5)),
        outer_sum(joined(6), joined(7)),
    )
    reduced = reduce_gradients(matrices, small_totals)
    block_output = jnp.concatenate(output_list, axis=0)
    input_gradient = jnp.concatenate(input_list, axis=0)
    return (
        block_output,
        input_gradient,
        reduced[4],
        reduced[5],
        reduced[0],
        reduced[6],
        reduced[7],
        reduced[1],
        reduced[8],
        reduced[9],
        reduced[10],
        reduced[2],
        reduced[11],
        reduced[3],
        reduced[12],
    )


def joint_split(rows, parts, heads_each):
    count, three, width = rows.shape
    span = heads_each * HEAD
    slots = slot_width(heads_each)
    rows = jnp.pad(rows, ((0, 0), (0, 0), (0, parts * span - width)))
    rows = rows.reshape(count, three, parts, span)
    rows = jnp.pad(rows, ((0, 0), (0, 0), (0, 0), (0, slots - span)))
    return rows.transpose(2, 0, 1, 3).reshape(parts, count, three * slots)


def joint_join(pieces, heads_each, width):
    parts, count, wide = pieces.shape
    span = heads_each * HEAD
    rows = pieces.reshape(parts, count, 3, wide // 3)[..., :span]
    rows = rows.transpose(1, 2, 0, 3).reshape(count, 3, parts * span)
    return rows[..., :width].reshape(count, 3 * width)


def slot_width(heads_each):
    return -(-heads_each * HEAD // LANES) * LANES


def causal(k_block_is_diagonal, same):
    if k_block_is_diagonal:
        same = same & (
            lax.broadcasted_iota(jnp.int32, (TILE, TILE), 0)
            <= lax.broadcasted_iota(jnp.int32, (TILE, TILE), 1)
        )
    return same


def attend_forward_kernel(nf, nc, heads, guests, *refs):
    n_in = sum(g[2] for g in guests)
    n_out = sum(g[3] for g in guests)
    own, ins, results, outs, own_scratch, scratch = split_refs(
        refs, (3, n_in, 3, n_out, 7, len(refs) - n_in - n_out - 13)
    )
    seg_row, seg_col, qkv_ref = own
    out_ref, turned_ref, lse_ref = results
    q_low, q_high, keys, values_turned, acc, tops, sums = own_scratch
    made = hosted(nf, nc, guests, ins, outs, scratch)
    greet_all(nc, {needs_of(g) for g in guests})
    begin_guests(made)
    send_guests(made)
    slots = out_ref.shape[1]
    scale = HEAD ** (-0.5)
    halves = (q_low, q_high)

    def one_block(q_block, k_block, first, count):
        q_at = pl.ds(pl.multiple_of(q_block * TILE, TILE), TILE)
        k_at = pl.ds(pl.multiple_of(k_block * TILE, TILE), TILE)
        same = causal(first, seg_col[k_at, :] == seg_row[:, q_at])
        for half in range(count):
            dims = pl.ds(half * HEAD, HEAD)
            scores = times_transposed(keys[k_at, :], halves[half][q_at, :])
            scores = jnp.where(same, scores, masked_score)
            top = jnp.max(scores, axis=0, keepdims=True)
            if not first:
                old_top = tops[half]
                top = jnp.maximum(old_top, top)
            weights = jnp.exp(scores - top)
            total = jnp.sum(weights, axis=0, keepdims=True)
            part = jnp.dot(
                values_turned[dims, k_at],
                weights.astype(jnp.bfloat16),
                preferred_element_type=jnp.float32,
            )
            if not first:
                fade = jnp.exp(old_top - top)
                total = total + sums[half] * fade
                part = part + acc[dims, :] * fade
            tops[half] = top
            sums[half] = total
            acc[dims, :] = part

    def one_pair(pair, count):
        column = pl.multiple_of(pair * LANES, LANES)
        queries = qkv_ref[:, pl.ds(column, LANES)] * jnp.bfloat16(scale)
        low_half = lax.broadcasted_iota(jnp.int32, queries.shape, 1) < HEAD
        q_low[...] = jnp.where(low_half, queries, jnp.zeros_like(queries))
        q_high[...] = jnp.where(low_half, jnp.zeros_like(queries), queries)
        keys[...] = qkv_ref[:, pl.ds(slots + column, LANES)]
        values = qkv_ref[:, pl.ds(2 * slots + column, LANES)]
        values_turned[...] = values.astype(jnp.float32).T.astype(jnp.bfloat16)

        @pl.loop(0, qkv_ref.shape[0] // TILE)
        def _(q_block):
            one_block(q_block, q_block, True, count)

            @pl.loop(0, q_block)
            def _(k_block):
                one_block(q_block, k_block, False, count)

            q_at = pl.ds(pl.multiple_of(q_block * TILE, TILE), TILE)
            if count == 1:
                acc[HEAD:, :] = jnp.zeros((LANES - HEAD, TILE), jnp.float32)
                lse_ref[pair, pl.ds(1, 1), q_at] = jnp.zeros((1, TILE), jnp.float32)
            for half in range(count):
                dims = pl.ds(half * HEAD, HEAD)
                acc[dims, :] = acc[dims, :] / sums[half]
                lse_ref[pair, pl.ds(half, 1), q_at] = tops[half] + jnp.log(sums[half])
            turned_ref[pair, :, q_at] = acc[...]
            out_ref[q_at, pl.ds(column, LANES)] = acc[...].T.astype(jnp.bfloat16)

    @pl.loop(0, heads // 2)
    def _(pair):
        one_pair(pair, 2)

        @pl.when(pair == 2)
        def _():
            pass_on_guests(made)

    if heads % 2:
        one_pair(heads // 2, 1)
    run_guests(made)


def attend_backward_kernel(nf, nc, heads, guests, *refs):
    n_in = sum(g[2] for g in guests)
    n_out = sum(g[3] for g in guests)
    own, ins, results, outs, own_scratch, scratch = split_refs(
        refs, (7, n_in, 1, n_out, 11, len(refs) - n_in - n_out - 19)
    )
    seg_row, seg_col, qkv_ref, grad_ref, turned_ref, lse_ref, order_ref = own
    out_ref = results[0]
    (
        q_low, q_high, keys, keys_turned, values, g_low, g_high,
        query_acc, key_acc, value_acc, corrections,
    ) = own_scratch
    made = hosted(nf, nc, guests, ins, outs, scratch)
    greet_all(nc, {needs_of(g) for g in guests})
    begin_guests(made)
    slots = grad_ref.shape[2]
    scale = HEAD ** (-0.5)
    q_halves = (q_low, q_high)
    g_halves = (g_low, g_high)

    def one_block(pair, q_block, k_block, first, count):
        q_at = pl.ds(pl.multiple_of(q_block * TILE, TILE), TILE)
        k_at = pl.ds(pl.multiple_of(k_block * TILE, TILE), TILE)
        same = causal(first, seg_col[k_at, :] == seg_row[:, q_at])
        value_sum = value_acc[k_at, :]
        key_sum = key_acc[k_at, :]
        for half in range(count):
            dims = pl.ds(half * HEAD, HEAD)
            query_rows = q_halves[half][q_at, :]
            grad_rows = g_halves[half][q_at, :]
            scores = times_transposed(keys[k_at, :], query_rows)
            lse = lse_ref[pair, pl.ds(half, 1), q_at]
            probs = jnp.exp(jnp.where(same, scores - lse, masked_score))
            dots = times_transposed(values[k_at, :], grad_rows)
            delta = (probs * (dots - corrections[half, :, q_at])).astype(jnp.bfloat16)
            value_sum = value_sum + jnp.dot(
                probs.astype(jnp.bfloat16), grad_rows, preferred_element_type=jnp.float32
            )
            key_sum = key_sum + jnp.dot(delta, query_rows, preferred_element_type=jnp.float32)
            part = jnp.dot(keys_turned[dims, k_at], delta, preferred_element_type=jnp.float32)
            if first:
                query_acc[dims, :] = part
            else:
                query_acc[dims, :] += part
        value_acc[k_at, :] = value_sum
        key_acc[k_at, :] = key_sum

    def one_pair(pair, count):
        column = pl.multiple_of(pair * LANES, LANES)
        queries = qkv_ref[:, pl.ds(column, LANES)] * jnp.bfloat16(scale)
        low_half = lax.broadcasted_iota(jnp.int32, queries.shape, 1) < HEAD
        zeros = jnp.zeros_like(queries)
        q_low[...] = jnp.where(low_half, queries, zeros)
        q_high[...] = jnp.where(low_half, zeros, queries)
        grads = jnp.concatenate(
            [grad_ref[order_ref[k], :, pl.ds(column, LANES)] for k in range(grad_ref.shape[0])]
        )
        g_low[...] = jnp.where(low_half, grads, zeros)
        g_high[...] = jnp.where(low_half, zeros, grads)
        product = grads.astype(jnp.float32).T * turned_ref[pair]
        corrections[0] = jnp.sum(product[:HEAD], axis=0, keepdims=True)
        corrections[1] = jnp.sum(product[HEAD:], axis=0, keepdims=True)
        keys_now = qkv_ref[:, pl.ds(slots + column, LANES)]
        keys[...] = keys_now
        keys_turned[...] = keys_now.astype(jnp.float32).T.astype(jnp.bfloat16)
        values[...] = qkv_ref[:, pl.ds(2 * slots + column, LANES)]
        key_acc[...] = jnp.zeros_like(key_acc)
        value_acc[...] = jnp.zeros_like(value_acc)
        if count == 1:
            query_acc[HEAD:, :] = jnp.zeros((LANES - HEAD, TILE), jnp.float32)

        @pl.loop(0, qkv_ref.shape[0] // TILE)
        def _(q_block):
            one_block(pair, q_block, q_block, True, count)

            @pl.loop(0, q_block)
            def _(k_block):
                one_block(pair, q_block, k_block, False, count)

            q_at = pl.ds(pl.multiple_of(q_block * TILE, TILE), TILE)
            out_ref[q_at, pl.ds(column, LANES)] = (query_acc[...].T * scale).astype(jnp.bfloat16)

        out_ref[:, pl.ds(slots + column, LANES)] = key_acc[...].astype(jnp.bfloat16)
        out_ref[:, pl.ds(2 * slots + column, LANES)] = value_acc[...].astype(jnp.bfloat16)

    @pl.loop(0, heads // 2)
    def _(pair):
        one_pair(pair, 2)

        @pl.when(pair == 0)
        def _():
            send_guests(made)

    if heads % 2:
        one_pair(heads // 2, 1)
    run_guests(made)


def pick(blocks, order):
    return blocks.at[order].get(mode="promise_in_bounds", unique_indices=True)


def all_units(vector, nc, nf, unit_each, shard):
    vector = vector.transpose(1, 0, 2).reshape(nc, nf, unit_each)
    return lax.dynamic_index_in_dim(vector, shard, 1, keepdims=False).reshape(nc * unit_each)


def rows_of(vectors, count):
    row = jnp.arange(count, dtype=jnp.int32)[:, None]
    total = jnp.where(row == 0, vectors[0][None], jnp.zeros_like(vectors[0][None]))
    for k, vector in enumerate(vectors[1:], 1):
        total = jnp.where(row == k, vector[None], total)
    return total


def normalize(rows):
    center = rows - jnp.mean(rows, axis=-1, keepdims=True)
    spread = jnp.mean(center * center, axis=-1, keepdims=True)
    inverse = lax.rsqrt(spread + epsilon)
    return center * inverse, inverse


def normalize_back(grads, gain, unit, inverse):
    pulled = grads * gain
    return inverse * (
        pulled
        - jnp.mean(pulled, axis=-1, keepdims=True)
        - unit * jnp.mean(pulled * unit, axis=-1, keepdims=True)
    )


def gelu_parts(value):
    root = 0.7978845608028654
    inner = root * (value + 0.044715 * value * value * value)
    bend = jnp.tanh(inner)
    slope = 0.5 * (1.0 + bend) + 0.5 * value * (1.0 - bend * bend) * root * (
        1.0 + 3 * 0.044715 * value * value
    )
    return 0.5 * value * (1.0 + bend), slope


def mesh_copy(source, target, send, receive, device):
    return pltpu.make_async_remote_copy(
        src_ref=source,
        dst_ref=target,
        send_sem=send,
        recv_sem=receive,
        device_id=device,
        device_id_type=pl.DeviceIdType.MESH,
    )


def greet(devices, swaps=()):
    barrier = pltpu.get_barrier_semaphore()
    for device in devices:
        pl.semaphore_signal(
            barrier, inc=1, device_id=device, device_id_type=pl.DeviceIdType.MESH
        )
    for device in swaps:

        @pl.when(elsewhere(device))
        def _():
            pl.semaphore_signal(
                barrier, inc=1, device_id=device, device_id_type=pl.DeviceIdType.MESH
            )

    count = len(devices)
    for device in swaps:
        count = count + jnp.where(elsewhere(device), 1, 0)
    pl.semaphore_wait(barrier, count)


def elsewhere(device):
    apart = (device[0] - lax.axis_index("fsdp")) * 64 + device[1] - lax.axis_index("ctx")
    return apart != 0


def to_column(f, c, i):
    return 2 * (c // 2 % 2) + c % 2, 2 * (2 * i + f % 2) + (f // 2 + f % 2) % 2, c // 4


def to_origin(f, c, j):
    core = c // 2 % 2
    return 2 * ((c % 2 + core) % 2) + core, 2 * (2 * j + f // 2) + f % 2, c // 4


def swap_peers(move, back):
    f, c = lax.axis_index("fsdp"), lax.axis_index("ctx")
    return [way(f, c, k)[:2] for way in (move, back) for k in range(2)]


def ctx_peers(nc):
    f, c = lax.axis_index("fsdp"), lax.axis_index("ctx")
    return [(f, (c + k) % nc) for k in range(1, nc)]


def greet_all(nc, needs):
    devices, swaps = [], []
    if "fsdp" in needs:
        devices += fsdp_peers(3)
    elif "near" in needs:
        devices += fsdp_peers(2)
    if "ctx" in needs:
        devices += ctx_peers(nc)
    elif "ring" in needs:
        devices += ring_peers(nc)
    if "column" in needs:
        swaps += swap_peers(to_column, to_origin)
    if "origin" in needs:
        swaps += swap_peers(to_origin, to_column)
    greet(devices, swaps)


def fsdp_places():
    shard = lax.axis_index("fsdp")
    partner = shard + 1 - 2 * (shard % 2)
    return shard, partner, (shard + 2) % 4, (partner + 2) % 4


def ring_places(nc):
    place = lax.axis_index("ctx")
    z, y = place // 2, place % 2
    spot = z * (1 - y) + (nc - 1 - z) * y

    def holder(at):
        at = (at + nc) % nc
        side = at // (nc // 2)
        return (1 - side) * 2 * at + side * (2 * (nc - 1 - at) + 1)

    return spot, holder


def ring_peers(nc):
    spot, holder = ring_places(nc)
    shard = lax.axis_index("fsdp")
    return [(shard, holder(spot + way)) for way in (1, -1)]


def fsdp_peers(count):
    place = lax.axis_index("ctx")
    return [(at, place) for at in fsdp_places()[1 : 1 + count]]


def chunks_of(rows, count):
    step = -(-rows // count // 16) * 16
    return [(at, min(step, rows - at)) for at in range(0, rows, step)]


def row_step(size):
    return next(step for step in (56, 40, 32, 16, 8) if size % step == 0)


class FsdpGather:
    SEMS = (7, 4)

    def __init__(self, own, out, sems):
        self.own, self.out, self.sems = own, out, sems
        self.shard, self.partner, self.cross, self.corner = fsdp_places()
        self.place = lax.axis_index("ctx")
        self.chunks = chunks_of(own.shape[0], 4)

    def copy(self, kind, k):
        at, size = self.chunks[k]
        rows = pl.ds(at, size)
        if kind == "own":
            return pltpu.make_async_copy(
                self.own.at[rows], self.out.at[self.shard, rows], self.sems.at[6, k]
            )
        if kind == "across":
            source, slot, device, sem = self.own.at[rows], self.shard, self.cross, 0
        elif kind == "beside":
            source, slot, device, sem = self.own.at[rows], self.shard, self.partner, 2
        else:
            slot, device, sem = self.cross, self.partner, 4
            source = self.out.at[slot, rows]
        return mesh_copy(
            source,
            self.out.at[slot, rows],
            self.sems.at[sem, k],
            self.sems.at[sem + 1, k],
            (device, self.place),
        )

    def begin(self):
        for kind in ("across", "beside", "own"):
            for k in range(len(self.chunks)):
                self.copy(kind, k).start()

    def pass_on(self):
        for k in range(len(self.chunks)):
            self.copy("across", k).wait_recv()
            self.copy("on", k).start()

    def finish(self):
        for k in range(len(self.chunks)):
            self.copy("across", k).wait_send()
            self.copy("beside", k).wait()
            self.copy("on", k).wait()
            self.copy("own", k).wait()


def joint_parts(nf, nc, rows, depth, place):
    thin = depth // nf // (8 * nc) * 8
    rest, each = rows - nf * thin, nc // nf
    parts = []
    for f in range(nf):
        parts.append((f * thin, pl.multiple_of(f * (depth // nf) + place * thin, 8), thin))
    last = (place // each) * (depth // nf) + nc * thin + (place % each) * rest
    parts.append((nf * thin, pl.multiple_of(last, 8), rest))
    return parts


def half_of(parts, way):
    middle = (len(parts) - 1) // 2
    return parts[:middle] if way == 1 else parts[middle:]


class RingGather:
    def __init__(self, nc, own, out, sems, parts=None):
        self.nc, self.own, self.out, self.sems = nc, own, out, sems
        self.spot, self.holder = ring_places(nc)
        self.shard = lax.axis_index("fsdp")
        self.parts = parts
        if parts is None:
            self.rows = out.shape[1]
            self.half = self.rows // 2 // 8 * 8

    def pieces(self, origin, way, step):
        if self.parts is not None:
            parts = self.parts(origin)
            if step == self.nc // 2:
                parts = half_of(parts, way)
            return [(pl.ds(at, size), self.out.at[pl.ds(there, size)]) for at, there, size in parts]
        rows = pl.ds(0, self.rows)
        if step == self.nc // 2:
            rows = pl.ds(0, self.half) if way == 1 else pl.ds(self.half, self.rows - self.half)
        return [(rows, self.out.at[origin, rows])]

    def copies(self, way, step):
        origin = self.holder(self.spot - way * (step - 1))
        side = 0 if way == 1 else 2
        made = []
        for k, (rows, whole) in enumerate(self.pieces(origin, way, step)):
            made.append(
                mesh_copy(
                    self.own.at[rows] if step == 1 else whole,
                    whole,
                    self.sems.at[side, step - 1, k],
                    self.sems.at[side + 1, step - 1, k],
                    (self.shard, self.holder(self.spot + way)),
                )
            )
        return made

    def keeps(self):
        return [
            pltpu.make_async_copy(self.own.at[rows], whole, self.sems.at[4, 0, k])
            for k, (rows, whole) in enumerate(self.pieces(lax.axis_index("ctx"), 1, 1))
        ]

    def start(self, step):
        for way in (1, -1):
            for copy in self.copies(way, step):
                copy.start()
        if step == 1:
            for copy in self.keeps():
                copy.start()

    def arrived(self, way, step):
        for copy in self.copies(way, step):
            copy.wait_recv()

    def advance(self, step):
        for way in (1, -1):
            self.arrived(way, step - 1)
            for copy in self.copies(way, step):
                copy.start()

    def finish(self, first, last):
        for way in (1, -1):
            for step in range(first, last + 1):
                for copy in self.copies(way, step):
                    copy.wait_send()
            self.arrived(way, last)
        if first == 1:
            for copy in self.keeps():
                copy.wait()


class RingScatter:
    def __init__(self, nc, mine, out, right, left, sems, parts=None):
        self.nc, self.mine, self.out, self.sems = nc, mine, out, sems
        self.inbox = {1: right, -1: left}
        self.spot, self.holder = ring_places(nc)
        self.shard = lax.axis_index("fsdp")
        self.rows = out.shape[0]
        self.half = self.rows // 2 // 8 * 8
        self.parts = parts

    def copies(self, way, step):
        inbox = self.inbox[way]
        if step > 1:
            sources = [(pl.ds(0, self.rows), inbox.at[step - 2])]
        else:
            place = self.holder(self.spot + self.nc // 2)
            if self.parts is not None:
                sources = [
                    (pl.ds(at, size), self.mine.at[pl.ds(there, size)])
                    for at, there, size in half_of(self.parts(place), way)
                ]
            else:
                low, high = pl.ds(0, self.half), pl.ds(self.half, self.rows - self.half)
                rows = low if way == 1 else high
                sources = [(rows, self.mine.at[place, rows])]
        side = 0 if way == 1 else 2
        return [
            mesh_copy(
                source,
                inbox.at[step - 1, rows],
                self.sems.at[side, step - 1, k],
                self.sems.at[side + 1, step - 1, k],
                (self.shard, self.holder(self.spot + way)),
            )
            for k, (rows, source) in enumerate(sources)
        ]

    def begin(self):
        for way in (1, -1):
            for copy in self.copies(way, 1):
                copy.start()

    def advance(self, step):
        for way in (1, -1):
            for copy in self.copies(way, step - 1):
                copy.wait_recv()
            box = self.inbox[way].at[step - 2]
            place = self.holder(self.spot + way * (self.nc // 2 + 1 - step))
            if self.parts is not None:
                parts = self.parts(place)
                came = half_of(parts, way) if step == 2 else parts
                for part in parts:
                    at, there, size = part
                    target, source = box.at[pl.ds(at, size)], self.mine.at[pl.ds(there, size)]
                    if any(part is other for other in came):
                        add_rows(target, source, (0, size))
                    else:
                        set_rows(target, source, (0, size))
            else:
                join_rows(box, self.mine.at[place], step, way, self.rows, self.half)
            for copy in self.copies(way, step):
                copy.start()

    def finish(self):
        last = self.nc // 2
        for way in (1, -1):
            for copy in self.copies(way, last):
                copy.wait_recv()
        right, left = self.inbox[1].at[last - 1], self.inbox[-1].at[last - 1]
        place = lax.axis_index("ctx")
        if self.parts is not None:
            for at, there, size in self.parts(place):
                rows = pl.ds(at, size)
                sum_rows(
                    self.out.at[rows], self.mine.at[pl.ds(there, size)], right.at[rows], left.at[rows]
                )
        else:
            sum_rows(self.out, self.mine.at[place], right, left)
        for way in (1, -1):
            for step in range(1, last + 1):
                for copy in self.copies(way, step):
                    copy.wait_send()


def join_rows(box, mine, step, way, rows, half):
    low, high = (0, half), (half, rows - half)
    if step == 2:
        got, rest = (low, high) if way == 1 else (high, low)
        set_rows(box, mine, rest)
    else:
        got = (0, rows)
    add_rows(box, mine, got)


def add_rows(target, source, rows):
    first, size = rows
    step = row_step(size)

    @pl.loop(0, size // step)
    def _(turn):
        at = pl.ds(pl.multiple_of(first + turn * step, 8), step)
        target[at] = (target[at].astype(jnp.float32) + source[at].astype(jnp.float32)).astype(
            target.dtype
        )


def set_rows(target, source, rows):
    first, size = rows
    step = row_step(size)

    @pl.loop(0, size // step)
    def _(turn):
        at = pl.ds(pl.multiple_of(first + turn * step, 8), step)
        target[at] = source[at]


def sum_rows(out, mine, right, left):
    step = row_step(out.shape[0])

    @pl.loop(0, out.shape[0] // step)
    def _(turn):
        at = pl.ds(pl.multiple_of(turn * step, 8), step)
        out[at] = (
            mine[at].astype(jnp.float32)
            + right[at].astype(jnp.float32)
            + left[at].astype(jnp.float32)
        ).astype(out.dtype)


class GatherStep:
    NEEDS = "ring"
    VMEM_IN = 0

    def __init__(self, nf, nc, step, ins, outs, scratch):
        self.step = step
        self.ring = RingGather(nc, None, outs[0], scratch[0])

    @staticmethod
    def shapes(nf, nc, step, arrays):
        (whole,) = arrays
        return (
            [jax.ShapeDtypeStruct(whole.shape, whole.dtype)],
            [pltpu.SemaphoreType.DMA((5, nc // 2, 1))],
            True,
        )

    def begin(self):
        self.ring.start(self.step)

    def send(self):
        pass

    def finish(self):
        self.ring.finish(self.step, self.step)


class SideGather:
    NEEDS = "near"
    VMEM_IN = 1

    def __init__(self, nf, nc, step, ins, outs, scratch):
        self.side = FsdpGather(ins[0], outs[0], scratch[0])

    @staticmethod
    def shapes(nf, nc, step, arrays):
        (array,) = arrays
        return (
            [jax.ShapeDtypeStruct((nf,) + array.shape, array.dtype)],
            [pltpu.SemaphoreType.DMA(FsdpGather.SEMS)],
            False,
        )

    def begin(self):
        pass

    def send(self):
        self.side.begin()

    def finish(self):
        self.side.finish()


class ScatterRing:
    NEEDS = "ring"
    VMEM_IN = 1

    def __init__(self, nf, nc, step, ins, outs, scratch):
        right, left, total, self.put_sem, sems = scratch
        self.out, self.total = outs[0], total
        parts = None
        if step:
            parts = functools.partial(joint_parts, nf, nc, step, ins[0].shape[0])
        self.ring = RingScatter(nc, ins[0], total, right, left, sems, parts)

    @staticmethod
    def shapes(nf, nc, step, arrays):
        mine = arrays[0]
        shape = (step,) + mine.shape[1:] if step else mine.shape[1:]
        box = pltpu.VMEM((nc // 2,) + shape, mine.dtype)
        return (
            [jax.ShapeDtypeStruct(shape, mine.dtype)],
            [
                box,
                box,
                pltpu.VMEM(shape, mine.dtype),
                pltpu.SemaphoreType.DMA((1,)),
                pltpu.SemaphoreType.DMA((4, nc // 2, nf + 1)),
            ],
            False,
        )

    def begin(self):
        self.ring.begin()

    def send(self):
        self.ring.advance(2)

    def more(self, step):
        self.ring.advance(step)

    def finish(self):
        self.ring.finish()
        put = pltpu.make_async_copy(self.total, self.out, self.put_sem.at[0])
        put.start()
        put.wait()


class ScatterStep:
    NEEDS = "ring"
    VMEM_IN = 0

    def __init__(self, nf, nc, step, ins, outs, scratch):
        self.nc, self.step = nc, step
        self.mine, self.before, self.outs = ins[0], ins[1:], outs
        self.sems = scratch[-1]
        self.boxes = scratch[:-1]
        self.spot, self.holder = ring_places(nc)
        self.shard = lax.axis_index("fsdp")
        self.rows = outs[0].shape[0]
        self.half = self.rows // 2 // 8 * 8

    @staticmethod
    def shapes(nf, nc, step, arrays):
        mine = arrays[0]
        block = jax.ShapeDtypeStruct(mine.shape[1:], mine.dtype)
        outs = [block, block]
        scratch = []
        if step > 1:
            scratch += [pltpu.VMEM(mine.shape[1:], mine.dtype)] * 4
        return outs, scratch + [pltpu.SemaphoreType.DMA((4, 4))], False

    def copy(self, k):
        way = (1, -1)[k]
        rows = pl.ds(0, self.rows)
        if self.step == 1:
            rows = pl.ds(0, self.half) if way == 1 else pl.ds(self.half, self.rows - self.half)
            source = self.mine.at[self.holder(self.spot + self.nc // 2), rows]
        else:
            source = self.boxes[k]
        return mesh_copy(
            source,
            self.outs[k].at[rows],
            self.sems.at[0, k],
            self.sems.at[1, k],
            (self.shard, self.holder(self.spot + way)),
        )

    def loads(self, k):
        way = (1, -1)[k]
        rows = pl.ds(0, self.rows)
        if self.step == 2:
            rows = pl.ds(0, self.half) if way == 1 else pl.ds(self.half, self.rows - self.half)
        place = self.holder(self.spot + way * (self.nc // 2 + 1 - self.step))
        return [
            pltpu.make_async_copy(
                self.before[k].at[rows], self.boxes[k].at[rows], self.sems.at[2, k]
            ),
            pltpu.make_async_copy(self.mine.at[place], self.boxes[2 + k], self.sems.at[3, k]),
        ]

    def begin(self):
        for k in range(2):
            if self.step == 1:
                self.copy(k).start()
            else:
                for load in self.loads(k):
                    load.start()

    def send(self):
        if self.step > 1:
            for k in range(2):
                for load in self.loads(k):
                    load.wait()
                way = (1, -1)[k]
                join_rows(self.boxes[k], self.boxes[2 + k], self.step, way, self.rows, self.half)
                self.copy(k).start()

    def finish(self):
        for k in range(2):
            self.copy(k).wait()


class Trade:
    def __init__(self, axis, size, source, target, sems, hops=None):
        self.axis, self.size = axis, size
        self.hops = hops or tuple(range(1, size))
        self.source, self.target, self.sems = source, target, sems
        self.me = lax.axis_index(axis)

    def copies(self):
        made = []
        for k in self.hops:
            other = (self.me + k) % self.size
            device = (
                (other, lax.axis_index("ctx"))
                if self.axis == "fsdp"
                else (lax.axis_index("fsdp"), other)
            )
            made.append(
                mesh_copy(
                    self.source(other),
                    self.target(self.me),
                    self.sems.at[0, k],
                    self.sems.at[1, k],
                    device,
                )
            )
        made.append(
            pltpu.make_async_copy(
                self.source(self.me), self.target(self.me), self.sems.at[2, 0]
            )
        )
        return made

    def begin(self):
        for copy in self.copies():
            copy.start()

    def finish(self):
        for copy in self.copies():
            copy.wait()


class TradeGuest:
    VMEM_IN = 1

    def __init__(self, nf, nc, step, ins, outs, scratch):
        axis, hops = step
        size = nf if axis == "fsdp" else nc
        whole = len(ins[0].shape) < len(outs[0].shape)
        self.trade = Trade(
            axis,
            size,
            (lambda k: ins[0]) if whole else (lambda k: ins[0].at[k]),
            lambda k: outs[0].at[k],
            scratch[0],
            hops,
        )

    @staticmethod
    def shapes(nf, nc, step, arrays):
        (array,) = arrays
        size = nf if step[0] == "fsdp" else nc
        shape = array.shape if array.ndim == 3 else (size,) + array.shape
        return (
            [jax.ShapeDtypeStruct(shape, array.dtype)],
            [pltpu.SemaphoreType.DMA((3, size))],
            False,
        )

    def begin(self):
        pass

    def send(self):
        self.trade.begin()

    def finish(self):
        self.trade.finish()


def window(part, parts, width):
    size = max(
        -(-(k + 1) * (width // parts) // LANES) * LANES - k * (width // parts) // LANES * LANES
        for k in range(parts)
    )
    return part * (width // parts) // LANES * LANES, size


class WindowTrade:
    VMEM_IN = 1

    def __init__(self, nf, nc, step, ins, outs, scratch):
        def source(k):
            start, size = window(k, nf, step)
            return ins[0].at[:, pl.ds(pl.multiple_of(start, LANES), size)]

        self.trade = Trade("fsdp", nf, source, lambda k: outs[0].at[k], scratch[0])

    @staticmethod
    def shapes(nf, nc, step, arrays):
        (array,) = arrays
        shape = (nf, array.shape[0], window(0, nf, step)[1])
        return (
            [jax.ShapeDtypeStruct(shape, array.dtype)],
            [pltpu.SemaphoreType.DMA((3, nf))],
            False,
        )

    def begin(self):
        pass

    def send(self):
        self.trade.begin()

    def finish(self):
        self.trade.finish()


class SwapGuest:
    VMEM_IN = 1

    def __init__(self, nf, nc, step, ins, outs, scratch):
        self.blocks, self.out, self.sems = ins[0], outs[0], scratch[0]
        self.move, self.back = (
            (to_column, to_origin) if step == "column" else (to_origin, to_column)
        )

    @staticmethod
    def shapes(nf, nc, step, arrays):
        (array,) = arrays
        return (
            [jax.ShapeDtypeStruct(array.shape, array.dtype)],
            [pltpu.SemaphoreType.DMA((3, 2))],
            False,
        )

    def copies(self, k):
        f, c = lax.axis_index("fsdp"), lax.axis_index("ctx")
        there = self.move(f, c, k)
        source, target = self.blocks.at[k], self.out.at[there[2]]
        away = mesh_copy(
            source, target, self.sems.at[0, k], self.sems.at[1, there[2]], there[:2]
        )
        return elsewhere(there), away, pltpu.make_async_copy(source, target, self.sems.at[2, k])

    def begin(self):
        pass

    def send(self):
        for k in range(2):
            apart, away, stay = self.copies(k)

            @pl.when(apart)
            def _():
                away.start()

            @pl.when(jnp.logical_not(apart))
            def _():
                stay.start()

    def finish(self):
        f, c = lax.axis_index("fsdp"), lax.axis_index("ctx")
        for k in range(2):
            apart, away, stay = self.copies(k)

            @pl.when(apart)
            def _():
                away.wait_send()

            @pl.when(jnp.logical_not(apart))
            def _():
                stay.wait()

            origin = self.back(f, c, k)
            arrival = mesh_copy(
                self.blocks.at[0],
                self.out.at[k],
                self.sems.at[0, 0],
                self.sems.at[1, k],
                origin[:2],
            )

            @pl.when(elsewhere(origin))
            def _():
                arrival.wait_recv()


def begin_guests(made):
    for guest in made:
        guest.begin()
    early_guests(made)


def early_guests(made):
    for guest in made:
        if isinstance(guest, ScatterStep):
            guest.send()


def send_guests(made):
    for guest in made:
        if not isinstance(guest, ScatterStep):
            guest.send()


def pass_on_guests(made):
    for guest in made:
        if isinstance(guest, SideGather):
            guest.side.pass_on()


def needs_of(guest):
    kind, step = guest[0], guest[1]
    if kind is TradeGuest:
        return step[0]
    if kind is WindowTrade:
        return "fsdp"
    if kind is SwapGuest:
        return step
    return kind.NEEDS


def split_refs(refs, counts):
    parts, at = [], 0
    for count in counts:
        parts.append(refs[at : at + count])
        at += count
    return parts


def hosted(nf, nc, guests, ins, outs, scratch):
    made, a, b, c = [], 0, 0, 0
    for kind, step, n_in, n_out, n_scratch in guests:
        made.append(
            kind(nf, nc, step, ins[a : a + n_in], outs[b : b + n_out], scratch[c : c + n_scratch])
        )
        a, b, c = a + n_in, b + n_out, c + n_scratch
    return made


def run_guests(made):
    for step in (3, 4):
        for guest in made:
            if isinstance(guest, ScatterRing):
                guest.more(step)
    for guest in made:
        guest.finish()


def lone_kernel(nf, nc, guests, *refs):
    n_in = sum(g[2] for g in guests)
    n_out = sum(g[3] for g in guests)
    ins, outs, scratch = split_refs(refs, (n_in, n_out, len(refs) - n_in - n_out))
    made = hosted(nf, nc, guests, ins, outs, scratch)
    greet_all(nc, {needs_of(g) for g in guests})
    begin_guests(made)
    send_guests(made)
    run_guests(made)


def gather_fsdp_kernel(nf, nc, guests, *refs):
    n_in = sum(g[2] for g in guests)
    n_out = sum(g[3] for g in guests)
    own, ins, out, outs, sems, scratch = split_refs(
        refs, (1, n_in, 1, n_out, 1, len(refs) - n_in - n_out - 3)
    )
    side = FsdpGather(own[0], out[0], sems[0])
    made = hosted(nf, nc, guests, ins, outs, scratch)
    greet_all(nc, {"near"} | {needs_of(g) for g in guests})
    side.begin()
    begin_guests(made)
    send_guests(made)
    side.pass_on()
    side.finish()
    run_guests(made)


def scatter_fsdp_kernel(nf, nc, guests, turned, ordered, *refs):
    n_in = sum(g[2] for g in guests)
    n_out = sum(g[3] for g in guests)
    count_own = 3 if ordered else 2
    operands, ins, result, outs, own_scratch, scratch = split_refs(
        refs, (count_own, n_in, 1, n_out, 6, len(refs) - n_in - n_out - 7 - count_own)
    )
    left_ref, right_ref = operands[:2]
    out_ref = result[0]
    part_ref, first_in, own_in, chip_sum, across_in, sems = own_scratch
    shard, partner, cross, corner = fsdp_places()
    place = lax.axis_index("ctx")
    made = hosted(nf, nc, guests, ins, outs, scratch)
    greet_all(nc, {"near"} | {needs_of(g) for g in guests})
    for guest in made:
        guest.begin()
    count, width = out_ref.shape
    chunks = chunks_of(count, 4)

    def copy(kind, k):
        at, size = chunks[k]
        rows = pl.ds(at, size)
        if kind == 0:
            source, target, device = part_ref.at[corner, rows], first_in, partner
        elif kind == 1:
            source, target, device = part_ref.at[partner, rows], own_in, partner
        else:
            source, target, device = chip_sum.at[rows], across_in, cross
        return mesh_copy(
            source,
            target.at[rows],
            sems.at[2 * kind, k],
            sems.at[2 * kind + 1, k],
            (device, place),
        )

    half = count // 2
    early, late = chunks[: len(chunks) // 2], chunks[len(chunks) // 2 :]

    def add_and_send(first, some):
        for k, (at, size) in enumerate(some, first):
            copy(0, k).wait_recv()

            @pl.loop(0, size // 32)
            def _(step):
                rows = pl.ds(pl.multiple_of(at + step * 32, 32), 32)
                chip_sum[rows] = (
                    part_ref[cross, rows].astype(jnp.float32)
                    + first_in[rows].astype(jnp.float32)
                ).astype(chip_sum.dtype)

            copy(2, k).start()

    @pl.loop(0, 8)
    def _(turn):
        pair = turn // 4
        of_two = (turn % 2) * (1 - pair) + (turn // 2 % 2) * pair
        upper = (turn // 2 % 2) * (1 - pair) + (turn % 2) * pair
        base = partner * (1 - of_two) + shard * of_two
        block = (base + 2 * (1 - pair)) % 4
        start = pl.multiple_of(upper * half, half)
        if ordered:
            rows = left_ref[operands[2][block * 2 + upper]]
        else:
            rows = left_ref[pl.ds(pl.multiple_of(block * count + start, half), half), :]
        for at in range(0, width, 512):
            size = 512 if at + 1024 <= width else width - at
            if turned:
                piece = times_transposed(rows, right_ref[at : at + size, :])
            else:
                piece = jnp.dot(
                    rows, right_ref[:, at : at + size], preferred_element_type=jnp.float32
                )
            part_ref[block, pl.ds(start, half), at : at + size] = piece.astype(part_ref.dtype)
            if at + size == width:
                break

        @pl.when(turn == 0)
        def _():
            for k in range(len(early)):
                copy(0, k).start()
            early_guests(made)

        @pl.when(turn == 1)
        def _():
            add_and_send(0, early)

        @pl.when(turn == 2)
        def _():
            for k in range(len(early), len(chunks)):
                copy(0, k).start()

        @pl.when(turn == 3)
        def _():
            add_and_send(len(early), late)
            send_guests(made)

        @pl.when(turn == 5)
        def _():
            for k in range(len(chunks)):
                copy(1, k).start()

    for k, (at, size) in enumerate(chunks):
        copy(1, k).wait_recv()
        copy(2, k).wait_recv()

        @pl.loop(0, size // 32)
        def _(turn):
            rows = pl.ds(pl.multiple_of(at + turn * 32, 32), 32)
            out_ref[rows] = (
                part_ref[shard, rows].astype(jnp.float32)
                + own_in[rows].astype(jnp.float32)
                + across_in[rows].astype(jnp.float32)
            )

    for kind in range(3):
        for k in range(len(chunks)):
            copy(kind, k).wait_send()
    run_guests(made)


def startup_kernel(nf, nc, spans, row_count, *refs):
    ring_count = len(spans)
    total = ring_count + row_count
    ins, outs, sems, extra = split_refs(refs, (total, total, total, 3))
    block, trade_sems, give_sems = extra
    rest = ins[0].shape[1] * nf - block.shape[0]
    rest = rest // (nf - 1)
    thin = ins[0].shape[1] - rest
    trade = Trade(
        "fsdp",
        nf,
        lambda k: ins[0].at[k, pl.ds(0, thin)],
        lambda k: block.at[pl.ds(pl.multiple_of(k * thin, 8), thin)],
        trade_sems,
    )
    giver = lax.axis_index("ctx") // (nc // nf)
    shard = lax.axis_index("fsdp")

    def give(k):
        return mesh_copy(
            ins[0].at[(shard + k) % nf, pl.ds(thin, rest)],
            block.at[pl.ds(nf * thin, rest)],
            give_sems.at[0, k],
            give_sems.at[1, 0],
            ((shard + k) % nf, lax.axis_index("ctx")),
        )

    own_rest = pltpu.make_async_copy(
        ins[0].at[shard, pl.ds(thin, rest)],
        block.at[pl.ds(nf * thin, rest)],
        give_sems.at[0, 0],
    )
    parts = functools.partial(joint_parts, nf, nc, block.shape[0], outs[0].shape[0])
    rings = [
        RingGather(nc, block if k == 0 else ins[k], outs[k], sems[k], None if k else parts)
        for k in range(ring_count)
    ]
    sides = [FsdpGather(ins[k], outs[k], sems[k]) for k in range(ring_count, total)]
    greet(fsdp_peers(3) + ring_peers(nc))
    trade.begin()

    @pl.when(shard == giver)
    def _():
        own_rest.start()
        for k in range(1, nf):
            give(k).start()

    for ring in rings[1:]:
        ring.start(1)
    sides[0].begin()
    trade.finish()

    @pl.when(shard == giver)
    def _():
        own_rest.wait()
        for k in range(1, nf):
            give(k).wait_send()

    @pl.when(shard != giver)
    def _():
        give(1).wait_recv()

    rings[0].start(1)
    sides[0].pass_on()
    for side in sides[1:]:
        side.begin()
    for step in range(2, nc // 2 + 1):
        for ring, span in zip(rings, spans):
            if step <= span:
                ring.advance(step)
        if step == 2:
            for side in sides[1:]:
                side.pass_on()
    for side in sides:
        side.finish()
    for ring, span in zip(rings, spans):
        ring.finish(1, span)


def in_vmem():
    return pl.BlockSpec(memory_space=pltpu.VMEM)


def in_smem():
    return pl.BlockSpec(memory_space=pltpu.SMEM)


def in_place():
    return pl.BlockSpec(memory_space=pl.ANY)


def widen(pieces):
    return jnp.pad(pieces, ((0, 0),) * (pieces.ndim - 1) + ((0, -pieces.shape[-1] % LANES),))


class Net:
    def __init__(self, nf, nc):
        self.nf, self.nc = nf, nc
        self.each = nc // nf
        self.ids = {}

    def call(self, kernel, key, outs, ins, in_specs, out_specs, scratch, aliases=None):
        ident = self.ids.setdefault(key, len(self.ids))
        return pl.pallas_call(
            kernel,
            out_shape=outs,
            in_specs=in_specs,
            out_specs=out_specs,
            scratch_shapes=scratch,
            input_output_aliases=aliases or {},
            compiler_params=pltpu.CompilerParams(
                collective_id=ident, has_side_effects=True, vmem_limit_bytes=60 << 20
            ),
        )(*ins)

    def swap(self, blocks, move, back):
        place = lax.axis_index("ctx")
        got = []
        for turn in range(self.each):
            slot = (move(0, place, 0)[2] + turn) % self.each
            piece = lax.dynamic_index_in_dim(blocks, slot, 0, keepdims=False)
            pairs = []
            for f in range(self.nf):
                for c in range(self.nc):
                    there = move(f, c, (move(f, c, 0)[2] + turn) % self.each)
                    pairs.append((f * self.nc + c, there[0] * self.nc + there[1]))
            got.append(lax.ppermute(piece, ("fsdp", "ctx"), pairs))
        order = (back(0, place, 0)[2] - jnp.arange(self.each)) % self.each
        return pick(jnp.stack(got), order)

    def total(self, mine, right, left):
        own = lax.dynamic_index_in_dim(mine, lax.axis_index("ctx"), 0, keepdims=False)
        return sum(part.astype(jnp.float32) for part in (own, right, left)).astype(mine.dtype)

    def lone(self, name, hosted_steps):
        plan, ins, outs, scratch, aliases = self.guests(hosted_steps, 0, 0)
        return self.call(
            functools.partial(lone_kernel, self.nf, self.nc, plan),
            name,
            tuple(outs),
            ins,
            self.specs(hosted_steps),
            [in_place()] * len(outs),
            scratch,
            aliases,
        )

    def specs(self, hosted_steps):
        made = []
        for kind, _, arrays in hosted_steps:
            made += [in_vmem() if kind.VMEM_IN else in_place()] * len(arrays)
        return made

    def startup(self, pieces, block_rows, whole_rows, blocks, spans, rows):
        nf, nc = self.nf, self.nc
        first = (block_rows, pieces.shape[2])
        arrays = [pieces] + list(blocks) + list(rows)
        outs = [jax.ShapeDtypeStruct((whole_rows, pieces.shape[2]), pieces.dtype)]
        outs += [jax.ShapeDtypeStruct((nc,) + a.shape, a.dtype) for a in blocks]
        outs += [jax.ShapeDtypeStruct((nf,) + a.shape, a.dtype) for a in rows]
        scratch = [pltpu.SemaphoreType.DMA((5, nc // 2, nf + 1)) for _ in range(1 + len(blocks))]
        scratch += [pltpu.SemaphoreType.DMA(FsdpGather.SEMS) for _ in rows]
        scratch += [pltpu.VMEM(first, pieces.dtype)] + [pltpu.SemaphoreType.DMA((3, nf))] * 2
        count = len(arrays)
        return self.call(
            functools.partial(startup_kernel, nf, nc, tuple(spans), len(rows)),
            "startup", tuple(outs), arrays, [in_vmem()] * count, [in_place()] * count, scratch,
        )

    def guests(self, hosted_steps, first_in, first_out):
        plan, ins, outs, scratch, aliases = [], [], [], [], {}
        for kind, step, arrays in hosted_steps:
            shapes, boxes, alias = kind.shapes(self.nf, self.nc, step, arrays)
            if alias:
                aliases[first_in + len(ins)] = first_out + len(outs)
            plan.append((kind, step, len(arrays), len(shapes), len(boxes)))
            ins += list(arrays)
            outs += shapes
            scratch += boxes
        return tuple(plan), ins, outs, scratch, aliases

    def gather_fsdp(self, name, rows, hosted_steps=()):
        plan, ins, outs, scratch, aliases = self.guests(hosted_steps, 1, 1)
        got = self.call(
            functools.partial(gather_fsdp_kernel, self.nf, self.nc, plan),
            name,
            (jax.ShapeDtypeStruct((self.nf,) + rows.shape, rows.dtype),) + tuple(outs),
            [rows] + ins,
            [in_vmem()] + self.specs(hosted_steps),
            [in_place()] * (1 + len(outs)),
            [pltpu.SemaphoreType.DMA(FsdpGather.SEMS)] + scratch,
            aliases,
        )
        return got[0].reshape((-1,) + rows.shape[1:]), got[1:]

    def scatter_fsdp(self, name, left, right, turned, hosted_steps=(), order=None):
        count = left.shape[0] // self.nf
        own = [left, right]
        if order is not None:
            own = [left.reshape(2 * self.nf, count // 2, left.shape[1]), right, order]
        plan, ins, outs, scratch, aliases = self.guests(hosted_steps, len(own), 1)
        block = (count, right.shape[0] if turned else right.shape[1])
        box = pltpu.VMEM(block, left.dtype)
        got = self.call(
            functools.partial(
                scatter_fsdp_kernel, self.nf, self.nc, plan, turned, order is not None
            ),
            name,
            (jax.ShapeDtypeStruct(block, jnp.float32),) + tuple(outs),
            own + ins,
            [in_vmem(), in_vmem(), in_smem()][: len(own)] + self.specs(hosted_steps),
            [in_vmem()] + [in_place()] * len(outs),
            [pltpu.VMEM((self.nf,) + block, left.dtype), box, box, box, box]
            + [pltpu.SemaphoreType.DMA((6, 4))]
            + scratch,
            aliases,
        )
        return got[0], got[1:]

    def attend_forward(self, segs, qkv, heads, hosted_steps):
        rows, wide = qkv.shape
        slots = wide // 3
        pairs = slots // LANES
        plan, ins, outs, scratch, aliases = self.guests(hosted_steps, 3, 3)
        low = jnp.bfloat16
        got = self.call(
            functools.partial(attend_forward_kernel, self.nf, self.nc, heads, plan),
            "attend_forward",
            (
                jax.ShapeDtypeStruct((rows, slots), low),
                jax.ShapeDtypeStruct((pairs, LANES, rows), jnp.float32),
                jax.ShapeDtypeStruct((pairs, 2, rows), jnp.float32),
            )
            + tuple(outs),
            [segs.reshape(1, rows), segs.reshape(rows, 1), qkv] + ins,
            [in_vmem()] * 3 + self.specs(hosted_steps),
            [in_vmem()] * 3 + [in_place()] * len(outs),
            [
                pltpu.VMEM((rows, LANES), low),
                pltpu.VMEM((rows, LANES), low),
                pltpu.VMEM((rows, LANES), low),
                pltpu.VMEM((LANES, rows), low),
                pltpu.VMEM((LANES, TILE), jnp.float32),
                pltpu.VMEM((2, 1, TILE), jnp.float32),
                pltpu.VMEM((2, 1, TILE), jnp.float32),
            ]
            + scratch,
            aliases,
        )
        return got[:3], got[3:]

    def attend_backward(self, segs, order, qkv, grads, turned, lse, heads, hosted_steps):
        rows, wide = qkv.shape
        plan, ins, outs, scratch, aliases = self.guests(hosted_steps, 7, 1)
        low = jnp.bfloat16
        got = self.call(
            functools.partial(attend_backward_kernel, self.nf, self.nc, heads, plan),
            "attend_backward",
            (jax.ShapeDtypeStruct((rows, wide), low),) + tuple(outs),
            [segs.reshape(1, rows), segs.reshape(rows, 1), qkv, grads, turned, lse, order] + ins,
            [in_vmem()] * 6 + [in_smem()] + self.specs(hosted_steps),
            [in_vmem()] + [in_place()] * len(outs),
            [
                pltpu.VMEM((rows, LANES), low),
                pltpu.VMEM((rows, LANES), low),
                pltpu.VMEM((rows, LANES), low),
                pltpu.VMEM((LANES, rows), low),
                pltpu.VMEM((rows, LANES), low),
                pltpu.VMEM((rows, LANES), low),
                pltpu.VMEM((rows, LANES), low),
                pltpu.VMEM((LANES, TILE), jnp.float32),
                pltpu.VMEM((rows, LANES), jnp.float32),
                pltpu.VMEM((rows, LANES), jnp.float32),
                pltpu.VMEM((2, 1, rows), jnp.float32),
            ]
            + scratch,
            aliases,
        )
        return got[0], got[1:]


def local_fast(
    net,
    inputs,
    cotangent,
    segments,
    stretch_order,
    prenorm_gain,
    prenorm_shift,
    joint_weight,
    query_bias,
    value_bias,
    mixer_weight,
    mixer_bias,
    midnorm_gain,
    midnorm_shift,
    expand_weight,
    expand_bias,
    shrink_weight,
    shrink_bias,
):
    nf, nc, each = net.nf, net.nc, net.each
    low, wide = jnp.bfloat16, jnp.float32
    _, stretch_len, width = inputs.shape
    heads_each = -(-(width // HEAD) // nf)
    span = heads_each * HEAD
    slots = slot_width(heads_each)
    rows_all = nc * stretch_len
    rows_own = each * stretch_len
    shard = lax.axis_index("fsdp")
    positions = stretch_order.reshape(each, nf).T.reshape(nc)
    inverse = jnp.sum(
        jnp.where(
            positions[None, :] == jnp.arange(nc, dtype=jnp.int32)[:, None],
            jnp.arange(nc, dtype=jnp.int32)[None, :],
            0,
        ),
        axis=1,
    ).astype(jnp.int32)

    narrow = prenorm_gain.shape[0]
    unit_each = expand_bias.shape[0] // nf

    depth = joint_weight.shape[0]
    thin = depth // (8 * nc) * 8
    rest = (depth - nc * thin) // each
    out_each = shrink_weight.shape[1]
    small_parts = (
        prenorm_gain, prenorm_shift, query_bias, value_bias, mixer_bias,
        midnorm_gain, midnorm_shift, shrink_bias, expand_bias,
    )
    small_count = len(small_parts) - 1 + nf
    small_rows = small_count + -small_count % 16
    last_rows = ((len(small_parts) - 1, small_rows - small_count), (0, 0))
    small_own = rows_of(small_parts[:-1], small_rows) + jnp.pad(
        expand_bias.reshape(nf, narrow), last_rows
    )
    small_own = widen(small_own)
    step = span - mixer_weight.shape[0]
    most = step * (nf - 1)
    columns = joint_weight.shape[1]
    joint_tall = jnp.concatenate(
        [
            joint_weight[: nc * thin].reshape(nc, thin, columns),
            jnp.tile(joint_weight[nc * thin :].reshape(each, rest, columns), (nf, 1, 1)),
        ],
        axis=1,
    )
    seg_own = jnp.broadcast_to(segments.astype(low)[:, None], (each, 16, stretch_len))
    joint_pieces, small_all, own_tokens, seg_own, above, expand_pieces, shrink_pieces = (
        net.lone(
            "first",
            [
                (TradeGuest, ("ctx", None), [widen(joint_tall)]),
                (TradeGuest, ("ctx", None), [small_own]),
                (SwapGuest, "column", [inputs]),
                (SwapGuest, "column", [seg_own]),
                (TradeGuest, ("fsdp", (nf - 1,)), [widen(mixer_weight[:most])]),
                (
                    TradeGuest,
                    ("fsdp", None),
                    [widen(expand_weight.T.reshape(nf, unit_each, depth))],
                ),
                (
                    TradeGuest,
                    ("fsdp", None),
                    [
                        widen(
                            shrink_weight.reshape(each, nf, unit_each, out_each)
                            .transpose(1, 0, 2, 3)
                            .reshape(nf, each * unit_each, out_each)
                        )
                    ],
                ),
            ],
        )
    )
    own_tokens = own_tokens.reshape(rows_own, width)
    joint_pieces = joint_pieces[..., :columns].transpose(1, 0, 2)
    joint_pieces = joint_split(joint_pieces.reshape(thin + rest, 3, width), nf, heads_each)
    expand_pieces = (
        expand_pieces[..., :depth].transpose(1, 0, 2).reshape(unit_each, width)
    )
    shrink_pieces = shrink_pieces[..., :out_each].reshape(nc * unit_each, out_each).T

    above = lax.dynamic_index_in_dim(above, (shard + 1) % nf, 0, keepdims=False)
    above = above[:, : mixer_weight.shape[1]]
    tall = jnp.concatenate([mixer_weight, above, jnp.zeros_like(above)])
    mixer_rows = lax.dynamic_slice_in_dim(tall, step * shard, span, 0)
    kept = shard * span + jnp.arange(span, dtype=jnp.int32) < width
    mixer_rows = jnp.where(kept[:, None], mixer_rows, jnp.zeros_like(mixer_rows))
    mixer_pieces = jnp.pad(mixer_rows.T, ((0, 0), (0, slots - span)))

    joint, mixer, expand, shrink, tokens, seg_blocks = net.startup(
        joint_pieces,
        nf * thin + rest,
        width,
        [mixer_pieces, expand_pieces, shrink_pieces],
        [nc // 2, nc // 2, 1, 1],
        [own_tokens, seg_own.reshape(each * 16, stretch_len)],
    )
    mixer = mixer.reshape(width, slots)
    tokens = tokens.reshape(rows_all, width)
    cotangent, tokens = lax.optimization_barrier((cotangent, tokens))
    own_tangent = net.swap(cotangent, to_column, to_origin).reshape(rows_own, width)
    segs = pick(seg_blocks.reshape(nc, 16, stretch_len)[:, 0], inverse)
    segs = segs.astype(jnp.int32)
    small_all = small_all[:, :small_count, :narrow].transpose(1, 0, 2).astype(wide)
    gain_one, shift_one, qbias, vbias, mbias, gain_two, shift_two, sbias = (
        small_all[: small_count - nf].reshape(small_count - nf, width)
    )
    ebias = small_all[small_count - nf :].reshape(nf, nc, unit_each)
    ebias = all_units(ebias, nc, nf, unit_each, shard)
    joint_bias = lax.dynamic_index_in_dim(
        joint_split(
            jnp.stack([qbias, jnp.zeros_like(qbias), vbias])[None], nf, heads_each
        ),
        shard, 0, keepdims=False,
    )

    tokens = pick(tokens.reshape(nc, stretch_len, width), inverse)
    token_values = tokens.reshape(rows_all, width).astype(wide)
    unit_one, _ = normalize(token_values)
    normed = lax.optimization_barrier((unit_one * gain_one + shift_one).astype(low))
    qkv = (
        jnp.dot(normed, joint, preferred_element_type=wide) + joint_bias
    ).astype(low)
    (attended, turned, lse), (expand, shrink, tangent) = net.attend_forward(
        segs,
        qkv,
        heads_each,
        [
            (GatherStep, 2, [expand]),
            (GatherStep, 2, [shrink]),
            (SideGather, 0, [own_tangent]),
        ],
    )
    attended = pick(attended.reshape(nc, stretch_len, slots), positions)
    attended = attended.reshape(rows_all, slots)
    branch, (expand, shrink) = net.scatter_fsdp(
        "scatter_branch",
        attended,
        mixer,
        True,
        [
            (GatherStep, 3, [expand]),
            (GatherStep, 3, [shrink]),
        ],
    )
    tangent = tangent.reshape(rows_all, width)
    middle = own_tokens.astype(wide) + branch + mbias
    unit_two, inverse_two = normalize(middle)
    second_own = (unit_two * gain_two + shift_two).astype(low)
    second, (expand, shrink) = net.gather_fsdp(
        "gather_second", second_own, [(GatherStep, 4, [expand]), (GatherStep, 4, [shrink])]
    )
    expand = expand.reshape(nc * unit_each, width)
    shrink = shrink.reshape(width, nc * unit_each)
    expanded = times_transposed(second, expand) + ebias
    active, slope = gelu_parts(expanded)
    active = active.astype(low)

    shrink_rows = outer_sum(tangent, active).astype(low).reshape(nc, out_each, nc * unit_each)
    active_grad = jnp.dot(tangent, shrink, preferred_element_type=wide)
    expand_delta = (active_grad * slope).astype(low)
    expand_rows = outer_sum(expand_delta, second).astype(low).reshape(nc, unit_each, width)
    second_grad, boxes = net.scatter_fsdp(
        "scatter_second",
        expand_delta,
        expand,
        False,
        [(ScatterStep, 1, [expand_rows]), (ScatterStep, 1, [shrink_rows])],
    )
    middle_delta = own_tangent.astype(wide) + normalize_back(
        second_grad, gain_two, unit_two, inverse_two
    )
    branch_own = middle_delta.astype(low)
    branch_delta, boxes = net.gather_fsdp(
        "gather_branch",
        branch_own,
        [(ScatterStep, 2, [expand_rows, *boxes[:2]]), (ScatterStep, 2, [shrink_rows, *boxes[2:]])],
    )
    lifted, boxes = net.scatter_fsdp(
        "scatter_lifted",
        active,
        shrink,
        True,
        [(ScatterStep, 3, [expand_rows, *boxes[:2]]), (ScatterStep, 3, [shrink_rows, *boxes[2:]])],
    )
    out_rows = (middle + lifted + sbias).astype(low)
    block_output = net.swap(out_rows.reshape(each, stretch_len, width), to_origin, to_column)
    attended_delta = jnp.dot(branch_delta, mixer, preferred_element_type=wide).astype(low)
    mixer_rows = outer_sum(branch_delta, attended).astype(low).reshape(nc, out_each, slots)
    attended_delta = attended_delta.reshape(nc, stretch_len, slots)
    joint_delta, boxes = net.attend_backward(
        segs,
        inverse,
        qkv,
        attended_delta,
        turned,
        lse,
        heads_each,
        [(ScatterStep, 4, [expand_rows, *boxes[:2]]), (ScatterStep, 4, [shrink_rows, *boxes[2:]])],
    )
    expand_grad = widen(net.total(expand_rows, *boxes[:2]))
    shrink_grad = widen(net.total(shrink_rows, *boxes[2:]))
    joint_rows = outer_sum(normed, joint_delta).astype(low)
    normed_grad, (joint_grad, mixer_grad, expand_pieces, shrink_pieces) = (
        net.scatter_fsdp(
            "scatter_normed",
            joint_delta,
            joint,
            True,
            [
                (ScatterRing, nf * thin + rest, [joint_rows]),
                (ScatterRing, 0, [mixer_rows]),
                (WindowTrade, width, [expand_grad]),
                (WindowTrade, nc * unit_each, [shrink_grad]),
            ],
            positions,
        )
    )
    unit_own, inverse_own = normalize(own_tokens.astype(wide))
    input_rows = middle_delta + normalize_back(normed_grad, gain_one, unit_own, inverse_own)
    mine = jnp.arange(nf, dtype=jnp.int32) == shard
    sums = jnp.sum(joint_delta.astype(wide), axis=0).reshape(3, slots)[:, :span]
    spread = jnp.where(mine[None, :, None], sums[:, None, :], 0.0).reshape(3, nf * span)
    unit_sums = jnp.sum(expand_delta.astype(wide), axis=0).reshape(nc, 1, unit_each)
    unit_sums = jnp.where(mine[None, :, None], unit_sums, 0.0).reshape(nc, nf * unit_each)
    vectors = (
        jnp.sum(normed_grad * unit_own, axis=0),
        jnp.sum(normed_grad, axis=0),
        spread[0, :width],
        spread[2, :width],
        jnp.sum(branch_own.astype(wide), axis=0),
        jnp.sum(second_grad * unit_two, axis=0),
        jnp.sum(second_grad, axis=0),
        jnp.sum(own_tangent.astype(wide), axis=0),
    )
    stacked = rows_of(vectors, len(vectors)).reshape(len(vectors), nc, narrow)
    unit_sums = unit_sums.reshape(nc, nf, narrow).transpose(1, 0, 2)
    small_blocks = jnp.concatenate(
        [stacked, unit_sums, jnp.zeros((small_rows - small_count, nc, narrow), wide)]
    )
    small_blocks = widen(small_blocks.astype(low)).transpose(1, 0, 2)
    small_lanes = small_blocks.shape[2]

    joint_pieces, joint_last, mixer_pieces, small_pieces, input_gradient = net.lone(
        "second",
        [
            (
                TradeGuest,
                ("fsdp", None),
                [joint_grad[: nf * thin].reshape(nf, thin, 3 * slots)],
            ),
            (TradeGuest, ("fsdp", None), [joint_grad[nf * thin :]]),
            (TradeGuest, ("fsdp", (1,)), [mixer_grad]),
            (TradeGuest, ("fsdp", None), [small_blocks.reshape(nc * small_rows, small_lanes)]),
            (SwapGuest, "origin", [input_rows.astype(low).reshape(each, stretch_len, width)]),
        ],
    )
    input_gradient = input_gradient.astype(wide)
    small_blocks = jnp.sum(small_pieces.astype(wide), axis=0).astype(low)
    joint_pieces = jnp.concatenate([joint_pieces, joint_last], axis=1)
    joint_pieces = joint_join(joint_pieces, heads_each, width)
    joint_pieces = joint_pieces.reshape(thin + rest, nc, columns).transpose(1, 0, 2)
    joint_pieces, small_pieces = net.lone(
        "third",
        [
            (TradeGuest, ("ctx", None), [widen(joint_pieces)]),
            (TradeGuest, ("ctx", None), [small_blocks.reshape(nc, small_rows, small_lanes)]),
        ],
    )
    joint_pieces = joint_pieces[..., :columns]
    joint_last = lax.dynamic_slice_in_dim(joint_pieces[:, thin:], each * shard, each, 0)
    joint_gradient = jnp.concatenate(
        [
            joint_pieces[:, :thin].reshape(nc * thin, columns),
            joint_last.reshape(each * rest, columns),
        ]
    ).astype(wide)
    at = shard * depth - window(shard, nf, width)[0]
    expand_pieces = lax.dynamic_slice_in_dim(expand_pieces, at, depth, 2)
    expand_gradient = expand_pieces.reshape(nf * unit_each, depth).T.astype(wide)
    units = each * unit_each
    at = shard * units - window(shard, nf, nf * units)[0]
    shrink_pieces = lax.dynamic_slice_in_dim(shrink_pieces, at, units, 2)
    shrink_pieces = shrink_pieces.reshape(nf, out_each, each, unit_each).transpose(2, 0, 3, 1)
    shrink_gradient = shrink_pieces.reshape(shrink_weight.shape).astype(wide)

    own_rows = lax.dynamic_index_in_dim(mixer_pieces, shard, 0, keepdims=False)[:, :span].T
    before = lax.dynamic_index_in_dim(mixer_pieces, (shard + nf - 1) % nf, 0, keepdims=False)
    below = lax.dynamic_slice_in_dim(
        jnp.pad(before[:, :span].T, ((0, most), (0, 0))),
        mixer_weight.shape[0] - step * ((shard + nf - 1) % nf),
        most,
        0,
    )
    moved = lax.dynamic_slice_in_dim(
        jnp.pad(own_rows, ((most, 0), (0, 0))), most - step * shard, mixer_weight.shape[0], 0
    )
    first_rows = jnp.arange(mixer_weight.shape[0], dtype=jnp.int32)[:, None] < step * shard
    below = jnp.pad(below, ((0, mixer_weight.shape[0] - most), (0, 0)))
    mixer_gradient = jnp.where(first_rows, below, moved).astype(wide)

    small_sum = jnp.sum(small_pieces.astype(wide), axis=0)[:small_count, :narrow]
    outs = [small_sum[k] for k in range(8)]
    return (
        block_output,
        input_gradient,
        outs[0],
        outs[1],
        joint_gradient,
        outs[2],
        outs[3],
        mixer_gradient,
        outs[4],
        outs[5],
        outs[6],
        expand_gradient,
        small_sum[8:].reshape(expand_bias.shape),
        shrink_gradient,
        outs[7],
    )


def solution(mesh):
    in_specs = (
        P("fsdp", "ctx", None),
        P("fsdp", "ctx", None),
        P("fsdp", "ctx"),
        P(),
        P("ctx"),
        P("ctx"),
        P("fsdp", "ctx"),
        P("ctx"),
        P("ctx"),
        P("fsdp", "ctx"),
        P("ctx"),
        P("ctx"),
        P("ctx"),
        P("fsdp", "ctx"),
        P("ctx"),
        P("fsdp", "ctx"),
        P("ctx"),
    )
    out_specs = (
        P("fsdp", "ctx", None),
        P("fsdp", "ctx", None),
        P("ctx"),
        P("ctx"),
        P("fsdp", "ctx"),
        P("ctx"),
        P("ctx"),
        P("fsdp", "ctx"),
        P("ctx"),
        P("ctx"),
        P("ctx"),
        P("fsdp", "ctx"),
        P("ctx"),
        P("fsdp", "ctx"),
        P("ctx"),
    )

    def run(*arrays):
        nf, nc = mesh.shape["fsdp"], mesh.shape["ctx"]
        whole_each = arrays[0].shape[0] == nc and (nf, nc) == (4, 8)
        if whole_each and arrays[0].shape[1] == nc * STRETCH:
            body = functools.partial(local_fast, Net(nf, nc))
        else:
            body = local
        return jax.shard_map(
            body, mesh=mesh, in_specs=in_specs, out_specs=out_specs, check_vma=False
        )(*arrays)

    return run
```
